32 devices in a mesh: dp: 8 (over z, y), tensor: 4 (over x, core).
Axes of the slice: x: 2, y: 2, z: 4, core: 2. Of those that a mesh axis runs over, the one named last changes fastest.
Arguments:
- resid_in: float32 [8, 2048, 1536], P('dp', 'tensor'), may hold values from -32 to 32
- norm_gain: float32 [1536], P(('dp', 'tensor')), may hold values from 0.5 to 1.5
- proj_zx: bfloat16 [1536, 2, 3072], P('dp', None, 'tensor'), may hold values from -0.15625 to 0.15625
- proj_dt: bfloat16 [1536, 48], P('dp', 'tensor'), may hold values from -0.15625 to 0.15625
- proj_bc: bfloat16 [1536, 256], P(('dp', 'tensor')), may hold values from -0.15625 to 0.15625
- conv_x_weight: float32 [4, 3072], P(None, 'tensor'), may hold values from -0.5 to 0.5
- conv_x_bias: float32 [3072], P('tensor'), may hold values from -0.5 to 0.5
- conv_bc_weight: float32 [4, 256], P(None, ('dp', 'tensor')), may hold values from -0.5 to 0.5
- conv_bc_bias: float32 [256], P(('dp', 'tensor')), may hold values from -0.5 to 0.5
- dt_bias: float32 [48], P('tensor'), may hold values from -5 to -2
- a_log: float32 [48], P('tensor'), may hold values from -4.6 to 0.5
- skip_gain: float32 [48], P('tensor'), may hold values from 0.25 to 1.75
- gate_gain: float32 [3072], P('tensor'), may hold values from 0.5 to 1.5
- proj_out: bfloat16 [3072, 1536], P('tensor', 'dp'), may hold values from -0.109375 to 0.109375
- cotangent: float32 [8, 2048, 1536], P('dp', 'tensor'), may hold values from -23 to 23
Outputs:
- block_out: float32 [8, 2048, 1536], P('dp', 'tensor')
- grad_resid_in: float32 [8, 2048, 1536], P('dp', 'tensor')
- grad_norm_gain: float32 [1536], P(('dp', 'tensor'))
- grad_proj_zx: float32 [1536, 2, 3072], P('dp', None, 'tensor')
- grad_proj_dt: float32 [1536, 48], P('dp', 'tensor')
- grad_proj_bc: float32 [1536, 256], P(('dp', 'tensor'))
- grad_conv_x_weight: float32 [4, 3072], P(None, 'tensor')
- grad_conv_x_bias: float32 [3072], P('tensor')
- grad_conv_bc_weight: float32 [4, 256], P(None, ('dp', 'tensor'))
- grad_conv_bc_bias: float32 [256], P(('dp', 'tensor'))
- grad_dt_bias: float32 [48], P('tensor')
- grad_a_log: float32 [48], P('tensor')
- grad_skip_gain: float32 [48], P('tensor')
- grad_gate_gain: float32 [3072], P('tensor')
- grad_proj_out: float32 [3072, 1536], P('tensor', 'dp')
The draws below stay inside these ranges and needn't reach their ends.
All inputs are finite; a program needn't handle non-finite values.
Results may differ from the reference program's by a relative error of at most 0.012.
The reference program's roundings to bfloat16 on the way count: a program that leaves them out, or rounds other values in their place, can miss the bound.
Values may be sent and summed in bfloat16 or wider, within the bound.
A program may use at most 320 MiB of HBM per device.

```python
import jax
import jax.numpy as jnp
from jax import lax

D = 1536
H = 48
N = 128
K = 4
BLK = 256
LEN = 2048
DI = 3072
SEQS = 8


def draw_resid_in(key, part):
    key_base, key_rows, key_cols = jax.random.split(jax.random.fold_in(key, 11), 3)
    base = jnp.clip(jax.random.normal(key_base, (SEQS, LEN, D), jnp.float32), -5.0, 5.0)
    row_scale = jnp.exp(jax.random.uniform(key_rows, (SEQS, LEN, 1), jnp.float32, -1.15, 1.15))
    col_scale = jnp.exp(jax.random.uniform(key_cols, (1, 1, D), jnp.float32, -0.69, 0.69))
    return base * row_scale * col_scale


def draw_cotangent(key, part):
    key_base = jax.random.fold_in(key, 23)
    base = jnp.clip(jax.random.normal(key_base, (SEQS, LEN, D), jnp.float32), -5.0, 5.0)
    seq_pos = jnp.arange(SEQS, dtype=jnp.float32)[:, None, None] / (SEQS - 1)
    tok_pos = jnp.arange(LEN, dtype=jnp.float32)[None, :, None] / (LEN - 1)
    scale = 0.5 * jnp.exp(jnp.log(3.0) * (seq_pos + tok_pos))
    return base * scale


def level_of(key, dims, cuts, low, high):
    def one(dim, parts):
        steps = jax.random.uniform(jax.random.fold_in(jax.random.fold_in(key, 6), dim), (parts,), jnp.float32, low / len(cuts), high / len(cuts))
        return jnp.repeat(jnp.exp(steps), dims[dim] // parts).reshape((-1,) + (1,) * (len(dims) - dim - 1))

    level = one(*cuts[0])
    for cut in cuts[1:]:
        level = level * one(*cut)
    return level


def centred(stream_key, extent, width, limit, cuts=(), held_as=jnp.bfloat16):
    loudness = level_of(stream_key, extent, cuts, -0.22, 0.18) if cuts else 1.0
    values = jax.random.normal(stream_key, extent, jnp.float32) * width * loudness
    return jnp.minimum(jnp.maximum(values, -limit), limit).astype(held_as)


def setup_inputs(seed: int = 0) -> dict:
    splits = jax.random.split(jax.random.key(seed), 16)
    resid_in = draw_resid_in(jax.random.fold_in(splits[15], 71), 0)
    norm_gain = jnp.clip(0.5 + 1.0 * jax.random.uniform(splits[1], (D,), jnp.float32) ** level_of(splits[1], (D,), ((0, 32),), -0.2, 0.2), 0.5, 1.5)
    proj_zx = centred(splits[2], (D, 2, DI), D ** -0.5, 0.15625, ((0, 8), (2, 4)))
    proj_dt = centred(splits[3], (D, H), D ** -0.5, 0.15625, ((0, 8), (1, 4)))
    proj_bc = centred(splits[4], (D, 2 * N), D ** -0.5, 0.15625, ((0, 32),))
    conv_x_weight = jnp.clip(jax.random.uniform(splits[5], (K, DI), jnp.float32, -0.5, 0.5) * level_of(splits[5], (K, DI), ((1, 4),), -0.4, 0.0), -0.5, 0.5)
    conv_x_bias = jnp.clip(jax.random.uniform(splits[6], (DI,), jnp.float32, -0.5, 0.5) * level_of(splits[6], (DI,), ((0, 4),), -0.4, 0.0), -0.5, 0.5)
    conv_bc_weight = jnp.clip(jax.random.uniform(splits[7], (K, 2 * N), jnp.float32, -0.5, 0.5) * level_of(splits[7], (K, 2 * N), ((1, 32),), -0.4, 0.0), -0.5, 0.5)
    conv_bc_bias = jnp.clip(jax.random.uniform(splits[8], (2 * N,), jnp.float32, -0.5, 0.5) * level_of(splits[8], (2 * N,), ((0, 32),), -0.4, 0.0), -0.5, 0.5)
    dt_bias = jnp.clip(-5.0 + 3.0 * jax.random.uniform(splits[9], (H,), jnp.float32) ** level_of(splits[9], (H,), ((0, 4),), -0.2, 0.2), -5.0, -2.0)
    a_log = jnp.clip(-4.6 + 5.1 * jax.random.uniform(splits[10], (H,), jnp.float32) ** level_of(splits[10], (H,), ((0, 4),), -0.2, 0.2), -4.6, 0.5)
    skip_gain = jnp.clip(0.25 + 1.5 * jax.random.uniform(splits[11], (H,), jnp.float32) ** level_of(splits[11], (H,), ((0, 4),), -0.2, 0.2), 0.25, 1.75)
    gate_gain = jnp.clip(0.5 + 1.0 * jax.random.uniform(splits[12], (DI,), jnp.float32) ** level_of(splits[12], (DI,), ((0, 4),), -0.2, 0.2), 0.5, 1.5)
    proj_out = centred(splits[13], (DI, D), DI ** -0.5, 0.109375, ((0, 4), (1, 8)))
    cotangent = draw_cotangent(jax.random.fold_in(splits[15], 71), 0)
    return dict(resid_in=resid_in, norm_gain=norm_gain, proj_zx=proj_zx, proj_dt=proj_dt, proj_bc=proj_bc, conv_x_weight=conv_x_weight, conv_x_bias=conv_x_bias, conv_bc_weight=conv_bc_weight, conv_bc_bias=conv_bc_bias, dt_bias=dt_bias, a_log=a_log, skip_gain=skip_gain, gate_gain=gate_gain, proj_out=proj_out, cotangent=cotangent)


EPSILON = 1e-05

def causal_conv(values, weight, offset_bias):
    length = values.shape[0]
    padded = jnp.pad(values, ((K - 1, 0), (0, 0)))
    summed = jnp.zeros(values.shape, jnp.float32) + offset_bias[None, :]
    for offset in range(K):
        summed = summed + weight[offset][None, :] * padded[offset:offset + length]
    return summed

def state_space(x_act, bc_act, dt_raw, dt_bias, a_log, skip_gain):
    maximum_precision = lax.Precision.HIGHEST
    length = x_act.shape[0]
    head_count = a_log.shape[0]
    head_width = x_act.shape[1] // head_count
    state_size = bc_act.shape[1] // 2
    blocks = length // BLK
    step_sizes = jax.nn.softplus(dt_raw + dt_bias[None, :])
    log_rates = step_sizes * (-jnp.exp(a_log))[None, :]
    x_blocks = x_act.reshape(blocks, BLK, head_count, head_width)
    dt_blocks = step_sizes.reshape(blocks, BLK, head_count)
    log_cum = jnp.cumsum(log_rates.reshape(blocks, BLK, head_count), axis=1)
    b_in = bc_act[:, :state_size].reshape(blocks, BLK, state_size)
    c_out = bc_act[:, state_size:].reshape(blocks, BLK, state_size)
    scores = jnp.einsum('bin,bjn->bij', c_out, b_in, precision=maximum_precision)
    log_gaps = log_cum[:, :, None, :] - log_cum[:, None, :, :]
    position = jnp.arange(BLK, dtype=jnp.int32)
    causal = position[:, None] >= position[None, :]
    kernel = jnp.exp(jnp.where(causal[None, :, :, None], log_gaps, -jnp.inf))
    kernel = kernel * scores[..., None] * dt_blocks[:, None, :, :]
    inner_out = jnp.einsum('bijh,bjhp->bihp', kernel, x_blocks, precision=maximum_precision)
    tail_weight = jnp.exp(log_cum[:, -1:, :] - log_cum) * dt_blocks
    states = jnp.einsum('bjn,bjh,bjhp->bhnp', b_in, tail_weight, x_blocks, precision=maximum_precision)
    block_decay = jnp.exp(log_cum[:, -1, :])

    def carry_state(entering, inputs):
        block_factor, block_state = inputs
        return (block_factor[:, None, None] * entering + block_state, entering)
    start_state = jnp.zeros((head_count, state_size, head_width), jnp.float32)
    unused, entering = lax.scan(carry_state, start_state, (block_decay, states))
    outer_out = jnp.einsum('bin,bhnp->bihp', c_out, entering, precision=maximum_precision) * jnp.exp(log_cum)[..., None]
    result = inner_out + outer_out + skip_gain[None, None, :, None] * x_blocks
    return result.reshape(length, head_count * head_width)

def scan_core(x_in, bc_in, dt_raw, conv_x_weight, conv_x_bias, conv_bc_weight, conv_bc_bias, dt_bias, a_log, skip_gain):
    x_act = jax.nn.silu(causal_conv(x_in, conv_x_weight, conv_x_bias))
    bc_act = jax.nn.silu(causal_conv(bc_in, conv_bc_weight, conv_bc_bias))
    return state_space(x_act, bc_act, dt_raw, dt_bias, a_log, skip_gain)

def pre_norm(seq_rows, gain):
    return seq_rows * lax.rsqrt(lax.optimization_barrier(jnp.mean(seq_rows * seq_rows, axis=-1, keepdims=True)) + EPSILON) * gain

def gated_norm(y_vals, gate_vals, gain):
    product = y_vals * jax.nn.silu(gate_vals)
    return product * lax.rsqrt(lax.optimization_barrier(jnp.mean(product * product, axis=-1, keepdims=True)) + EPSILON) * gain

def contract_first(left, right):
    return lax.dot_general(left, right, (((0,), (0,)), ((), ())), preferred_element_type=jnp.float32)

def contract_last(left, right):
    return lax.dot_general(left, right, (((1,), (1,)), ((), ())), preferred_element_type=jnp.float32)

def reference(resid_in, norm_gain, proj_zx, proj_dt, proj_bc, conv_x_weight, conv_x_bias, conv_bc_weight, conv_bc_bias, dt_bias, a_log, skip_gain, gate_gain, proj_out, cotangent):
    maximum_precision = lax.Precision.HIGHEST
    zx_flat = proj_zx.reshape(D, 2 * DI)
    key_query_wide = proj_bc.astype(jnp.float32)
    params = (norm_gain, proj_zx, proj_dt, proj_bc, conv_x_weight, conv_x_bias, conv_bc_weight, conv_bc_bias, dt_bias, a_log, skip_gain, gate_gain, proj_out)

    def one_sequence(totals, inputs):
        seq_rows, seq_cot = inputs
        normed, norm_back = jax.vjp(pre_norm, seq_rows, norm_gain)
        normed_half = normed.astype(jnp.bfloat16)
        zx_all = jnp.dot(normed_half, zx_flat, preferred_element_type=jnp.float32)
        gate_pre = zx_all[:, :DI]
        x_in = zx_all[:, DI:]
        dt_raw = jnp.dot(normed_half, proj_dt, preferred_element_type=jnp.float32)
        bc_in = jnp.dot(normed_half, proj_bc, preferred_element_type=jnp.float32)
        y_vals, core_back = jax.vjp(scan_core, x_in, bc_in, dt_raw, conv_x_weight, conv_x_bias, conv_bc_weight, conv_bc_bias, dt_bias, a_log, skip_gain)
        gnorm, gate_back = jax.vjp(gated_norm, y_vals, gate_pre, gate_gain)
        gated_values = gnorm.astype(jnp.bfloat16)
        block_out = seq_rows + jnp.dot(gated_values, proj_out, preferred_element_type=jnp.float32)
        cot_half = seq_cot.astype(jnp.bfloat16)
        gated_output_gradient = contract_last(cot_half, proj_out)
        output_weight_gradient = contract_first(gated_values, cot_half)
        d_y, d_gate, grad_gate = gate_back(gated_output_gradient)
        core_grads = core_back(d_y)
        d_x_in = core_grads[0]
        key_query_input_gradient = core_grads[1]
        d_dt_raw = core_grads[2]
        gate_input_gradient = jnp.concatenate([d_gate, d_x_in], axis=1).astype(jnp.bfloat16)
        step_size_gradient = d_dt_raw.astype(jnp.bfloat16)
        normalized_gradient = contract_last(gate_input_gradient, zx_flat) + contract_last(step_size_gradient, proj_dt)
        normalized_gradient = normalized_gradient + lax.dot_general(key_query_input_gradient, key_query_wide, (((1,), (1,)), ((), ())), precision=maximum_precision)
        d_rows, grad_gain = norm_back(normalized_gradient)
        gate_input_weight_gradient = contract_first(normed_half, gate_input_gradient).reshape(D, 2, DI)
        step_weight_gradient = contract_first(normed_half, step_size_gradient)
        key_query_weight_gradient = lax.dot_general(normed_half.astype(jnp.float32), key_query_input_gradient, (((0,), (0,)), ((), ())), precision=maximum_precision)
        fresh = (grad_gain, gate_input_weight_gradient, step_weight_gradient, key_query_weight_gradient) + tuple(core_grads[3:]) + (grad_gate, output_weight_gradient)
        totals = jax.tree.map(lambda held, new_term: held + new_term, totals, fresh)
        return (totals, (block_out, d_rows + seq_cot))
    start = jax.tree.map(lambda item: jnp.zeros(item.shape, jnp.float32), params)
    totals, outputs = lax.scan(one_sequence, start, (resid_in, cotangent))
    return (outputs[0], outputs[1]) + tuple(totals)
```

```python
import functools, math
import jax, jax.numpy as jnp
from jax import lax
from jax.experimental import pallas as pl
from jax.experimental.pallas import tpu as pltpu
from jax.sharding import PartitionSpec as P

EPSILON = 1e-05
CHUNK = 128
LANES = 128
TAPS = 4
LOG2E = 1.4426950408889634
BF = jnp.bfloat16
F32 = jnp.float32


MESH = pl.DeviceIdType.MESH
PARTS = 4
ROW_PARTS = 6


def _place():
    d, t = lax.axis_index("dp"), lax.axis_index("tensor")
    return d // 2, d % 2, t // 2, t % 2


def _peer(outer, inner, far, near):
    return (outer * 2 + inner, far * 2 + near)


def _greet(outer_n):
    z, y, x, c = _place()
    barrier = pltpu.get_barrier_semaphore()
    peers = []
    for k in range(outer_n):
        for j in (0, 1):
            if k or j:
                peers.append(_peer((z + k) % outer_n, (y + j) % 2, x, c))
    for k in (0, 1):
        for j in (0, 1):
            if k or j:
                peers.append(_peer(z, y, (x + k) % 2, (c + j) % 2))
    for peer in peers:
        pl.semaphore_signal(barrier, inc=1, device_id=peer, device_id_type=MESH)
    pl.semaphore_wait(barrier, len(peers))


def _parts(rows):
    return max(p for p in range(1, ROW_PARTS + 1) if rows % (16 * p) == 0)


def _remote(src, dst, send, recv, peer):
    return pltpu.make_async_remote_copy(
        src_ref=src, dst_ref=dst, send_sem=send, recv_sem=recv, device_id=peer, device_id_type=MESH)


def _rows(start, size):
    return pl.ds(pl.multiple_of(start, 16), size)


class _Reduction:
    def __init__(self, outer_n, partial, grads, block_sum, owned, own_tokens, near_buf, far_src, far_buf,
                 own_grads, in_buf, out_src, out_buf, near_sem, far_sem, in_sem, out_sem, local_sem):
        self.__dict__.update(locals())
        self.z, self.y, self.x, self.c = _place()
        self.me = _peer(self.z, self.y, self.x, self.c)
        self.own_rows = block_sum.shape[0]
        self.block = owned.shape[0]
        self.wparts = _parts(self.block)
        self.late = -(-self.wparts // 6)
        self.size = self.own_rows // PARTS
        self.bsize = self.block // self.wparts
        order = list(range(1, outer_n))
        order.sort(key=lambda k: -min(k, outer_n - k))
        self.order = order + [0]

    def token_rows(self, far, near, part):
        return _rows((far * 2 + near) * self.own_rows + part * self.size, self.size)

    def grad_rows(self, outer, inner, part):
        return _rows((outer * 2 + inner) * self.block + part * self.bsize, self.bsize)

    def near_copy(self, i, part):
        far = (1 - self.x, self.x)[i]
        at = pl.ds(part * self.size, self.size)
        return _remote(self.partial.at[self.token_rows(far, 1 - self.c, part), :], self.near_buf.at[i, at, :],
                       self.near_sem.at[0, i, part], self.near_sem.at[1, i, part],
                       _peer(self.z, self.y, self.x, 1 - self.c))

    def far_copy(self, part):
        at = pl.ds(part * self.size, self.size)
        return _remote(self.far_src.at[at, :], self.far_buf.at[at, :], self.far_sem.at[0, part],
                       self.far_sem.at[1, part], _peer(self.z, self.y, 1 - self.x, self.c))

    def in_copy(self, k, part):
        at = pl.ds(part * self.bsize, self.bsize)
        rows = self.grad_rows((self.z + k) % self.outer_n, 1 - self.y, part)
        return _remote(self.grads.at[rows, :], self.in_buf.at[k, at, :], self.in_sem.at[0, k, part],
                       self.in_sem.at[1, k, part], _peer(self.z, 1 - self.y, self.x, self.c))

    def out_copy(self, k, part):
        at = pl.ds(part * self.bsize, self.bsize)
        return _remote(self.out_src.at[k - 1, at, :], self.out_buf.at[k - 1, at, :], self.out_sem.at[0, k - 1, part],
                       self.out_sem.at[1, k - 1, part], _peer((self.z + k) % self.outer_n, self.y, self.x, self.c))

    def local_copies(self):
        copies = []
        for i, far in enumerate((1 - self.x, self.x)):
            rows = _rows((far * 2 + self.c) * self.own_rows, self.own_rows)
            copies.append(pltpu.make_async_copy(self.partial.at[rows, :], self.own_tokens.at[i], self.local_sem.at[i]))
        for k in range(self.outer_n):
            rows = _rows((((self.z + k) % self.outer_n) * 2 + self.y) * self.block, self.block)
            copies.append(pltpu.make_async_copy(self.grads.at[rows, :], self.own_grads.at[k], self.local_sem.at[2 + k]))
        return copies

    def begin(self):
        _greet(self.outer_n)
        for part in range(PARTS):
            self.near_copy(0, part).start()
        for part in range(self.wparts):
            for k in self.order:
                self.in_copy(k, part).start()
        for part in range(PARTS):
            self.near_copy(1, part).start()
        for copy in self.local_copies():
            copy.start()

    def ready(self):
        for copy in self.local_copies():
            copy.wait()

    def token_step(self, part):
        at = pl.ds(part * self.size, self.size)
        self.near_copy(0, part).wait_recv()
        self.far_src[at, :] = (self.own_tokens[0, at, :].astype(F32) + self.near_buf[0, at, :].astype(F32)).astype(BF)
        self.far_copy(part).start()

    def grad_step(self, part):
        at = pl.ds(part * self.bsize, self.bsize)
        for k in self.order:
            self.in_copy(k, part).wait_recv()
            both = self.own_grads[k, at, :].astype(F32) + self.in_buf[k, at, :].astype(F32)
            if k:
                self.out_src[k - 1, at, :] = both.astype(BF)
                self.out_copy(k, part).start()
            else:
                self.owned[at, :] = both

    def plan(self, steps):
        pieces = [(1, self.ready)]
        for part in range(PARTS):
            pieces.append((min(1 + part, steps - 1), functools.partial(self.token_step, part)))
        for part in range(self.wparts - self.late):
            pieces.append((min(2 + part * (steps - 2) // self.wparts, steps - 1),
                           functools.partial(self.grad_step, part)))
        return pieces

    def end(self):
        for part in range(self.wparts - self.late, self.wparts):
            self.grad_step(part)
        for part in range(PARTS):
            at = pl.ds(part * self.size, self.size)
            self.near_copy(1, part).wait_recv()
            self.far_copy(part).wait_recv()
            self.block_sum[at, :] = (self.own_tokens[1, at, :].astype(F32) + self.near_buf[1, at, :].astype(F32)
                                     + self.far_buf[at, :].astype(F32))
        for part in range(self.wparts):
            at = pl.ds(part * self.bsize, self.bsize)
            total = self.owned[at, :]
            for k in self.order[:-1]:
                self.out_copy(k, part).wait_recv()
                total = total + self.out_buf[k - 1, at, :].astype(F32)
            self.owned[at, :] = total
        for part in range(PARTS):
            self.near_copy(0, part).wait_send()
            self.near_copy(1, part).wait_send()
            self.far_copy(part).wait_send()
        for part in range(self.wparts):
            for k in self.order:
                self.in_copy(k, part).wait_send()
                if k:
                    self.out_copy(k, part).wait_send()


def reduction_scratch(outer_n, tokens, grads):
    dma = pltpu.SemaphoreType.DMA
    parts = _parts(grads[0])
    return [pltpu.VMEM((2,) + tokens, BF), pltpu.VMEM((2,) + tokens, BF), pltpu.VMEM(tokens, BF),
            pltpu.VMEM(tokens, BF), pltpu.VMEM((outer_n,) + grads, BF), pltpu.VMEM((outer_n,) + grads, BF),
            pltpu.VMEM((outer_n - 1,) + grads, BF), pltpu.VMEM((outer_n - 1,) + grads, BF),
            dma((2, 2, PARTS)), dma((2, PARTS)), dma((2, outer_n, parts)), dma((2, outer_n - 1, parts)),
            dma((2 + outer_n,))]


def _sigmoid(v):
    return 1.0 / (1.0 + jnp.exp(-v))


def _softplus(t):
    return jnp.maximum(t, 0.0) + jnp.log1p(jnp.exp(-jnp.abs(t)))


def _dot_last(a, b):
    return lax.dot_general(a, b, (((1,), (1,)), ((), ())), preferred_element_type=F32)


def _dot_exact(a, b):
    return jnp.dot(a, b, precision=lax.Precision.HIGHEST, preferred_element_type=F32)


def _halves(v):
    high = v.astype(BF)
    return high, (v - high.astype(F32)).astype(BF)


def _dot_three(a, b):
    a_high, a_low = _halves(a)
    b_high, b_low = _halves(b)
    return _dot_last(jnp.concatenate([a_high, a_low, a_high], axis=1),
                     jnp.concatenate([b_high, b_high, b_low], axis=1))


def _rows_sum(v):
    return v.reshape(v.shape[0] // 8, 8, v.shape[1]).sum(axis=0)


def _split(lo, v):
    zero = jnp.zeros_like(v)
    return [jnp.where(lo, v, zero), jnp.where(lo, zero, v)]


def _times(dt_raw, head, rows, cols):
    t = dt_raw + head[0:1, :]
    delta = _softplus(t)
    rate = -jnp.exp(head[1:2, :])
    tri = (rows >= cols).astype(F32)
    cum = _dot_exact(tri, delta * (rate * LOG2E))
    return t, delta, rate, cum


def _pair_cols(lo, v, q):
    return jnp.where(lo, v[:, 2 * q : 2 * q + 1], v[:, 2 * q + 1 : 2 * q + 2])


def _conv(buf, start, cols, w, length):
    shifted = [buf[start + k : start + k + length, cols] for k in range(TAPS)]
    v = w[TAPS : TAPS + 1, :] + w[0:1, :] * shifted[0]
    for k in range(1, TAPS):
        v = v + w[k : k + 1, :] * shifted[k]
    return v, shifted


def forward_kernel(width, p_ref, dg_ref, convx_ref, convbc_ref, head_ref, lane_ref,
                   y_ref, h_ref, s_ref, state, xbuf, bcbuf, sums, sum_sem):
    tokens = p_ref.shape[0]
    pairs = width // LANES
    step = pl.program_id(0)
    z, y_at, x, c = _place()
    me = x * 2 + c
    half = sums.shape[1] // 2
    tensor_peers = [_peer(z, y_at, (x + k) % 2, (c + j) % 2) for k in (0, 1) for j in (0, 1) if k or j]

    @pl.when(step == 0)
    def _():
        barrier = pltpu.get_barrier_semaphore()
        for peer in tensor_peers:
            pl.semaphore_signal(barrier, inc=1, device_id=peer, device_id_type=MESH)
        pl.semaphore_wait(barrier, len(tensor_peers))
        state[...] = jnp.zeros_like(state)
        xbuf[0:8, :] = jnp.zeros((8, width), F32)
        bcbuf[0:8, :] = jnp.zeros((8, 2 * LANES), F32)

    @pl.when(step > 0)
    def _():
        xbuf[0:8, :] = xbuf[tokens : tokens + 8, :]
        bcbuf[0:8, :] = bcbuf[tokens : tokens + 8, :]

    xbuf[8 : 8 + tokens, :] = p_ref[:, width : 2 * width]
    bcbuf[8 : 8 + tokens, :] = p_ref[:, 2 * width : 2 * width + 2 * LANES]
    rows = lax.broadcasted_iota(jnp.int32, (CHUNK, CHUNK), 0)
    cols = lax.broadcasted_iota(jnp.int32, (CHUNK, CHUNK), 1)
    lo = cols < LANES // 2
    head = head_ref[...]
    ones = jnp.ones((8, LANES), F32)
    for sub in range(tokens // CHUNK):
        base = sub * CHUNK
        span = slice(base, base + CHUNK)
        vbc, _ = _conv(bcbuf, base + 5, slice(0, 2 * LANES), convbc_ref[...], CHUNK)
        bc = vbc * _sigmoid(vbc)
        b_in, c_out = bc[:, :LANES], bc[:, LANES:]
        c_high, c_low = _halves(c_out)
        c_wide = jnp.concatenate([c_high, c_low, c_high], axis=1)
        _, delta, _, cum = _times(p_ref[span, 2 * width + 2 * LANES :], head, rows, cols)
        cum_t = cum.T
        scores = jnp.where(rows >= cols, _dot_three(c_out, b_in), 0.0)
        last = cum[CHUNK - 1 : CHUNK, :]
        tail = jnp.exp2(last - cum)
        grow = jnp.exp2(cum)
        decay = jnp.exp2(last)
        b_t = b_in.T.astype(BF)
        squares = jnp.zeros((CHUNK, LANES), F32)
        inner = jnp.zeros((CHUNK, LANES), F32)
        h_ref[sub] = state[...]
        for q in range(pairs):
            lanes = slice(q * LANES, (q + 1) * LANES)
            v, _ = _conv(xbuf, base + 5, lanes, convx_ref[:, lanes], CHUNK)
            x_act = v * _sigmoid(v)
            u = x_act * _pair_cols(lo, delta, q)
            left = []
            for h in (2 * q, 2 * q + 1):
                e = jnp.exp2(jnp.minimum(cum[:, h : h + 1] - cum_t[h : h + 1, :], 0.0))
                left.append((e * scores).astype(BF))
            held = state[:, lanes]
            held_high, held_low = _halves(held)
            y = jnp.dot(jnp.concatenate(left, axis=1), jnp.concatenate(_split(lo, u.astype(BF)), axis=0),
                        preferred_element_type=F32)
            outer = jnp.dot(c_wide, jnp.concatenate([held_high, held_high, held_low], axis=0),
                            preferred_element_type=F32)
            y = y + outer * _pair_cols(lo, grow, q) + lane_ref[0:1, lanes] * x_act
            y_ref[span, lanes] = y
            uw = (u * _pair_cols(lo, tail, q)).astype(BF)
            factor = _pair_cols(lo[0:1, :], decay, q)
            state[:, lanes] = held * factor + jnp.dot(b_t, uw, preferred_element_type=F32)
            z = p_ref[span, lanes]
            product = y * (z * _sigmoid(z))
            squares = squares + product * product
            inner = inner + dg_ref[span, lanes].astype(F32) * lane_ref[1:2, lanes] * product
        row_sq = lax.dot_general(ones, squares, (((1,), (1,)), ((), ())),
                                 precision=lax.Precision.HIGHEST, preferred_element_type=F32)
        row_in = lax.dot_general(ones, inner, (((1,), (1,)), ((), ())),
                                 precision=lax.Precision.HIGHEST, preferred_element_type=F32)
        at = step * (tokens // CHUNK) + sub
        sums[me, pl.ds(at, 1), :] = row_sq[0:1, :]
        sums[me, pl.ds(half + at, 1), :] = row_in[0:1, :]

    @pl.when(step == pl.num_programs(0) - 1)
    def _():
        copies = [_remote(sums.at[me], sums.at[me], sum_sem.at[0, i], sum_sem.at[1, i], peer)
                  for i, peer in enumerate(tensor_peers)]
        for copy in copies:
            copy.start()
        for copy in copies:
            copy.wait_recv()
        s_ref[...] = (sums[0] + sums[1]) + (sums[2] + sums[3])
        for copy in copies:
            copy.wait_send()


def backward_kernel(width, outer_n, p_ref, prev_ref, y_ref, dy_ref, h_ref,
                    convx_ref, convbc_ref, head_ref, lane_ref, partial, grads,
                    dp_ref, gx_ref, gbc_ref, gh_ref, block_sum, owned,
                    grad_state, carry_hg, xbuf, bcbuf, dvx, dvbc, *comm):
    tokens = p_ref.shape[0]
    pairs = width // LANES
    step = pl.program_id(0)
    is_first_block = step == pl.num_programs(0) - 1
    length = partial.shape[0]
    reduction = _Reduction(outer_n, partial, grads, block_sum, owned, *comm)

    @pl.when(step == 0)
    def _():
        reduction.begin()

    for at, piece in reduction.plan(length // tokens):
        @pl.when(step == at)
        def _(piece=piece):
            piece()

    @pl.when(step == 0)
    def _():
        grad_state[...] = jnp.zeros_like(grad_state)
        carry_hg[...] = jnp.zeros_like(carry_hg)
        dvx[0:8, :] = jnp.zeros((8, width), F32)
        dvbc[0:8, :] = jnp.zeros((8, 2 * LANES), F32)
        gx_ref[...] = jnp.zeros_like(gx_ref)
        gbc_ref[...] = jnp.zeros_like(gbc_ref)
        gh_ref[...] = jnp.zeros_like(gh_ref)

    keep = jnp.where(is_first_block, 0.0, 1.0)
    xbuf[0:8, :] = prev_ref[:, width : 2 * width] * keep
    bcbuf[0:8, :] = prev_ref[:, 2 * width : 2 * width + 2 * LANES] * keep
    xbuf[8 : 8 + tokens, :] = p_ref[:, width : 2 * width]
    bcbuf[8 : 8 + tokens, :] = p_ref[:, 2 * width : 2 * width + 2 * LANES]
    rows = lax.broadcasted_iota(jnp.int32, (CHUNK, CHUNK), 0)
    cols = lax.broadcasted_iota(jnp.int32, (CHUNK, CHUNK), 1)
    lo = cols < LANES // 2
    head = head_ref[...]
    for sub in reversed(range(tokens // CHUNK)):
        base = sub * CHUNK
        span = slice(base, base + CHUNK)
        vbc, shifted_bc = _conv(bcbuf, base + 5, slice(0, 2 * LANES), convbc_ref[...], CHUNK)
        sbc = _sigmoid(vbc)
        bc = vbc * sbc
        b_in, c_out = bc[:, :LANES], bc[:, LANES:]
        b_half, c_half = b_in.astype(BF), c_out.astype(BF)
        t, delta, rate, cum = _times(p_ref[span, 2 * width + 2 * LANES :], head, rows, cols)
        cum_t = cum.T
        causal_t = cols >= rows
        scores_t = jnp.where(causal_t, _dot_three(b_in, c_out), 0.0)
        last = cum[CHUNK - 1 : CHUNK, :]
        tail = jnp.exp2(last - cum)
        grow = jnp.exp2(cum)
        decay = jnp.exp2(last)
        c_t = c_out.T.astype(BF)
        d_scores = jnp.zeros((CHUNK, CHUNK), F32)
        d_b = jnp.zeros((CHUNK, LANES), F32)
        d_c = jnp.zeros((CHUNK, LANES), F32)
        per_head = jnp.zeros((CHUNK, LANES), F32)
        hg_heads = jnp.zeros((8, LANES), F32)
        dvx[CHUNK : CHUNK + 8, :] = dvx[0:8, :]
        dvbc[CHUNK : CHUNK + 8, :] = dvbc[0:8, :]
        for q in range(pairs):
            lanes = slice(q * LANES, (q + 1) * LANES)
            wide = _pair_cols(lo, delta, q)
            skip = lane_ref[0:1, lanes]
            v, shifted = _conv(xbuf, base + 5, lanes, convx_ref[:, lanes], CHUNK)
            sv = _sigmoid(v)
            x_act = v * sv
            u = x_act * wide
            u_half = u.astype(BF)
            y = y_ref[span, lanes]
            dy_half = dy_ref[span, lanes]
            dy = dy_half.astype(F32)
            dy_block = jnp.concatenate(_split(lo, dy_half), axis=0)
            d_m = _dot_last(u_half, dy_block)
            left, left_b = [], []
            for a in (0, 1):
                h = 2 * q + a
                e = jnp.exp2(jnp.minimum(cum_t[h : h + 1, :] - cum[:, h : h + 1], 0.0))
                left.append((e * scores_t).astype(BF))
                d_scores = d_scores + e * d_m[:, a * CHUNK : (a + 1) * CHUNK]
                left_b.append((b_in * tail[:, h : h + 1]).astype(BF))
            g_held = grad_state[:, lanes]
            g_half, g_low = _halves(g_held)
            h_held = h_ref[sub, :, lanes]
            h_half, h_low = _halves(h_held)
            right = jnp.concatenate([dy_block] + _split(lo, g_half), axis=0)
            du = jnp.dot(jnp.concatenate(left + left_b, axis=1), right, preferred_element_type=F32)
            dx = du * wide + skip * dy
            dv = dx * (sv * (1.0 + v * (1.0 - sv)))
            dvx[0:CHUNK, lanes] = dv
            w = convx_ref[:, lanes]
            d_in = w[TAPS - 1 : TAPS, :] * dv
            for k in range(TAPS - 1):
                ahead = TAPS - 1 - k
                d_in = d_in + w[k : k + 1, :] * dvx[ahead : ahead + CHUNK, lanes]
            dp_ref[span, lanes] = d_in.astype(BF)
            for k in range(TAPS):
                gx_ref[k, :, lanes] += _rows_sum(dv * shifted[k])
            gx_ref[4, :, lanes] += _rows_sum(dv)
            gx_ref[5, :, lanes] += _rows_sum(dy * x_act)
            edy = (dy * _pair_cols(lo, grow, q)).astype(BF)
            uw = (u * _pair_cols(lo, tail, q)).astype(BF)
            d_c = d_c + _dot_last(jnp.concatenate([edy, edy], axis=1), jnp.concatenate([h_half, h_low], axis=1))
            d_b = d_b + _dot_last(jnp.concatenate([uw, uw], axis=1), jnp.concatenate([g_half, g_low], axis=1))
            g_new = g_held * _pair_cols(lo[0:1, :], decay, q) + jnp.dot(
                c_t, edy, preferred_element_type=F32)
            grad_state[:, lanes] = g_new
            r1 = x_act * du
            r2 = dy * (y - skip * x_act)
            sel1 = (cols == 2 * q + (rows >= LANES // 2).astype(jnp.int32)).astype(BF)
            sel2 = (cols == LANES // 2 + 2 * q + (rows >= LANES // 2).astype(jnp.int32)).astype(BF)
            r1h = r1.astype(BF)
            r1l = (r1 - r1h.astype(F32)).astype(BF)
            r2h = r2.astype(BF)
            r2l = (r2 - r2h.astype(F32)).astype(BF)
            per_head = per_head + jnp.dot(
                jnp.concatenate([r1h, r1l, r2h, r2l], axis=1),
                jnp.concatenate([sel1, sel1, sel2, sel2], axis=0), preferred_element_type=F32)
            hg_heads = hg_heads + _dot_exact(carry_hg[:, lanes], sel1.astype(F32))
            carry_hg[:, lanes] = _rows_sum(g_new * h_held)
        d_scores = jnp.where(causal_t, d_scores, 0.0)
        ds_half = d_scores.astype(BF)
        d_b = d_b + jnp.dot(ds_half, c_half, preferred_element_type=F32)
        d_c = d_c + jnp.dot(d_scores.T.astype(BF), b_half, preferred_element_type=F32)
        dvb = jnp.concatenate([d_b, d_c], axis=1) * (sbc * (1.0 + vbc * (1.0 - sbc)))
        dvbc[0:CHUNK, :] = dvb
        wbc = convbc_ref[...]
        d_bc = wbc[TAPS - 1 : TAPS, :] * dvb
        for k in range(TAPS - 1):
            ahead = TAPS - 1 - k
            d_bc = d_bc + wbc[k : k + 1, :] * dvbc[ahead : ahead + CHUNK, :]
        dp_ref[span, width : width + 2 * LANES] = d_bc.astype(BF)
        for k in range(TAPS):
            gbc_ref[k] += _rows_sum(dvb * shifted_bc[k])
        gbc_ref[4] += _rows_sum(dvb)
        direct = per_head
        through = pltpu.roll(per_head, LANES // 2, 1)
        d_cum = through - delta * direct
        suffix = _dot_exact((cols >= rows).astype(F32), d_cum)
        d_log = suffix + jnp.sum(hg_heads, axis=0, keepdims=True)
        valid = cols < 2 * pairs
        d_delta = direct + rate * d_log
        d_dt = jnp.where(valid, d_delta * _sigmoid(t), 0.0)
        dp_ref[span, width + 2 * LANES :] = d_dt.astype(BF)
        gh_ref[0] += _rows_sum(d_dt)
        gh_ref[1] += _rows_sum(jnp.where(valid, delta * d_log, 0.0)) * rate

    @pl.when(is_first_block)
    def _():
        reduction.end()


def ssd_forward(proj, dg, convx, convbc, head, lane, tokens=256):
    length, total = proj.shape
    width = convx.shape[1]
    subs = tokens // CHUNK
    whole = lambda a: pl.BlockSpec(a.shape, lambda i: (0,) * a.ndim)
    return pl.pallas_call(
        functools.partial(forward_kernel, width),
        grid=(length // tokens,),
        in_specs=[pl.BlockSpec((tokens, total), lambda i: (i, 0)),
                  pl.BlockSpec((tokens, width), lambda i: (i, 0)),
                  whole(convx), whole(convbc), whole(head), whole(lane)],
        out_specs=[pl.BlockSpec((tokens, width), lambda i: (i, 0)),
                   pl.BlockSpec((subs, LANES, width), lambda i: (i, 0, 0)),
                   pl.BlockSpec((2 * length // CHUNK, CHUNK), lambda i: (0, 0))],
        out_shape=[jax.ShapeDtypeStruct((length, width), F32),
                   jax.ShapeDtypeStruct((length // CHUNK, LANES, width), F32),
                   jax.ShapeDtypeStruct((2 * length // CHUNK, CHUNK), F32)],
        scratch_shapes=[pltpu.VMEM((LANES, width), F32),
                        pltpu.VMEM((tokens + 8, width), F32),
                        pltpu.VMEM((tokens + 8, 2 * LANES), F32),
                        pltpu.VMEM((4, 2 * length // CHUNK, CHUNK), F32),
                        pltpu.SemaphoreType.DMA((2, 3))],
        compiler_params=pltpu.CompilerParams(collective_id=2, has_side_effects=True),
        cost_estimate=pl.CostEstimate(flops=4 * 10**9, bytes_accessed=30 * 2**20, transcendentals=10**7),
        name="scan_forward",
    )(proj, dg, convx, convbc, head, lane)


def ssd_backward(proj, y, dy, states, convx, convbc, head, lane, partial, grads, tokens=256):
    length, total = proj.shape
    width = convx.shape[1]
    subs = tokens // CHUNK
    n = length // tokens
    dp, tp = lax.axis_size("dp"), lax.axis_size("tensor")
    whole = lambda a: pl.BlockSpec(a.shape, lambda i: (0,) * a.ndim)
    rev = lambda i: (n - 1 - i, 0)
    own = lambda shape: pl.BlockSpec(shape, lambda i: (0, 0))
    hbm = pl.BlockSpec(memory_space=pl.ANY)
    block_shape = (length // tp, partial.shape[1])
    owned_shape = (grads.shape[0] // dp, grads.shape[1])
    return pl.pallas_call(
        functools.partial(backward_kernel, width, dp // 2),
        grid=(n,),
        in_specs=[pl.BlockSpec((tokens, total), rev),
                  pl.BlockSpec((8, total), lambda i: (jnp.maximum((n - 1 - i) * (tokens // 8) - 1, 0), 0)),
                  pl.BlockSpec((tokens, width), rev),
                  pl.BlockSpec((tokens, width), rev),
                  pl.BlockSpec((subs, LANES, width), lambda i: (n - 1 - i, 0, 0)),
                  whole(convx), whole(convbc), whole(head), whole(lane), hbm, hbm],
        out_specs=[pl.BlockSpec((tokens, total - width), rev),
                   pl.BlockSpec((6, 8, width), lambda i: (0, 0, 0)),
                   pl.BlockSpec((5, 8, 2 * LANES), lambda i: (0, 0, 0)),
                   pl.BlockSpec((2, 8, LANES), lambda i: (0, 0, 0)),
                   own(block_shape), own(owned_shape)],
        out_shape=[jax.ShapeDtypeStruct((length, total - width), BF),
                   jax.ShapeDtypeStruct((6, 8, width), F32),
                   jax.ShapeDtypeStruct((5, 8, 2 * LANES), F32),
                   jax.ShapeDtypeStruct((2, 8, LANES), F32),
                   jax.ShapeDtypeStruct(block_shape, F32),
                   jax.ShapeDtypeStruct(owned_shape, F32)],
        scratch_shapes=[pltpu.VMEM((LANES, width), F32),
                        pltpu.VMEM((8, width), F32),
                        pltpu.VMEM((tokens + 8, width), F32),
                        pltpu.VMEM((tokens + 8, 2 * LANES), F32),
                        pltpu.VMEM((CHUNK + 8, width), F32),
                        pltpu.VMEM((CHUNK + 8, 2 * LANES), F32)] + reduction_scratch(dp // 2, block_shape, owned_shape),
        compiler_params=pltpu.CompilerParams(collective_id=3, has_side_effects=True, vmem_limit_bytes=62 * 2**20),
        cost_estimate=pl.CostEstimate(flops=12 * 10**9, bytes_accessed=50 * 2**20, transcendentals=10**7),
        name="scan_backward",
    )(proj, proj, y, dy, states, convx, convbc, head, lane, partial, grads)


def middle_kernel(width, inner_channels, z_ref, y_ref, dg_ref, s_ref, lane_ref, normed, cot, out_t,
                  dy_ref, dz_ref, out_ref, grads_ref, gg_ref, gated, acc_z, acc_o):
    tokens = z_ref.shape[0]
    step = pl.program_id(0)
    half = s_ref.shape[0] // 2

    @pl.when(step == 0)
    def _():
        gg_ref[...] = jnp.zeros_like(gg_ref)
        acc_z[...] = jnp.zeros_like(acc_z)
        acc_o[...] = jnp.zeros_like(acc_o)

    for sub in range(tokens // CHUNK):
        span = slice(sub * CHUNK, (sub + 1) * CHUNK)
        at = step * (tokens // CHUNK) + sub
        wide = lambda row: jnp.broadcast_to(row, (8, CHUNK)).T[:, 0:1]
        squares, dots = wide(s_ref[pl.ds(at, 1), :]), wide(s_ref[pl.ds(half + at, 1), :])
        inv = lax.rsqrt(squares / inner_channels + EPSILON)
        mean = inv * dots / inner_channels
        for q in range(width // LANES):
            lanes = slice(q * LANES, (q + 1) * LANES)
            gain = lane_ref[1:2, lanes]
            y, z, dg = y_ref[span, lanes], z_ref[span, lanes], dg_ref[span, lanes]
            sz = _sigmoid(z)
            act = z * sz
            quot = y * act * inv
            gg_ref[:, lanes] += _rows_sum(dg * quot)
            gated[span, lanes] = (quot * gain).astype(BF)
            d_prod = inv * (dg * gain - quot * mean)
            dy_ref[span, lanes] = (d_prod * act).astype(BF)
            dz_ref[span, lanes] = (d_prod * y * sz * (1.0 + z * (1.0 - sz))).astype(BF)
    out_ref[...] = _dot_last(gated[...], out_t[...]).astype(BF)
    first = lambda a, b: lax.dot_general(a, b, (((0,), (0,)), ((), ())), preferred_element_type=F32)
    acc_z[...] += first(normed[...], dz_ref[...])
    acc_o[...] += first(cot[...], gated[...])

    @pl.when(step == pl.num_programs(0) - 1)
    def _():
        grads_ref[:, :width] = acc_z[...].astype(BF)
        grads_ref[:, width:] = acc_o[...].astype(BF)


def middle(proj, y, dg, sums, lane, normed, cot, out_t, inner_channels, tokens=512):
    length, model = normed.shape
    width = y.shape[1]
    at = lambda cols: pl.BlockSpec((tokens, cols), lambda i: (i, 0))
    once = lambda shape: pl.BlockSpec(shape, lambda i: (0, 0), pipeline_mode=pl.Buffered(1))
    return pl.pallas_call(
        functools.partial(middle_kernel, width, inner_channels),
        grid=(length // tokens,),
        in_specs=[at(width), at(width), at(width), once(sums.shape), once(lane.shape), at(model), at(model),
                  once(out_t.shape)],
        out_specs=[at(width), at(width), at(model), once((model, 2 * width)), once((8, width))],
        out_shape=[jax.ShapeDtypeStruct((length, width), BF),
                   jax.ShapeDtypeStruct((length, width), BF),
                   jax.ShapeDtypeStruct((length, model), BF),
                   jax.ShapeDtypeStruct((model, 2 * width), BF),
                   jax.ShapeDtypeStruct((8, width), F32)],
        scratch_shapes=[pltpu.VMEM((tokens, width), BF),
                        pltpu.VMEM((model, width), F32),
                        pltpu.VMEM((model, width), F32)],
        cost_estimate=pl.CostEstimate(flops=15 * 10**9, bytes_accessed=50 * 2**20, transcendentals=10**6),
        name="middle",
    )(proj, y, dg, sums, lane, normed, cot, out_t)


def pad_rows(a, rows):
    return jnp.pad(a, ((0, rows - a.shape[0]), (0, 0)))


def pack_params(conv_x_weight, conv_x_bias, conv_bc_weight, conv_bc_bias, dt_bias, a_log, skip_gain, gate_gain):
    width = conv_x_weight.shape[1]
    convx = pad_rows(jnp.concatenate([conv_x_weight, conv_x_bias[None]], 0), 8)
    convbc = pad_rows(jnp.concatenate([conv_bc_weight, conv_bc_bias[None]], 0), 8)
    heads = dt_bias.shape[0]
    head = jnp.pad(jnp.stack([dt_bias, a_log]), ((0, 6), (0, LANES - heads)))
    lane = pad_rows(jnp.stack([jnp.repeat(skip_gain, width // heads), gate_gain]), 8)
    return convx, convbc, head, lane
def gather_kernel(outer_n, small, resid, cot, wzx, wdt, wbc, wout,
                  small_all, normed_all, cot_all, weight, weight_out,
                  small_t, small_d, normed_own, cot_own, bc_slots, bc_rows,
                  small_sem_t, small_sem_d, bc_sem, norm_sem, cot_sem, zx_sem, bd_sem, wo_sem, local_sem):
    z, y, x, c = _place()
    t = x * 2 + c
    d = z * 2 + y
    block = wzx.shape[0]
    zx_cols = wzx.shape[1]
    bc_cols = wbc.shape[1]
    wparts = _parts(block)
    own_rows = resid.shape[0]
    model = resid.shape[1]
    cot_own[...] = cot[...].astype(BF)
    _greet(outer_n)
    started = []

    def go(copy):
        copy.start()
        started.append(copy)
        return copy

    dp_peers = [(k, j) for k in range(outer_n) for j in (0, 1) if k or j]
    tensor_peers = [(k, j) for k in (0, 1) for j in (0, 1) if k or j]
    small_first, bc_first = [], []
    for i, (k, j) in enumerate(dp_peers):
        peer = _peer((z + k) % outer_n, (y + j) % 2, x, c)
        small_first.append(go(_remote(small, small_d.at[i], small_sem_d.at[0, i], small_sem_d.at[1, i], peer)))
    for i, (k, j) in enumerate(tensor_peers):
        peer = _peer(z, y, (x + k) % 2, (c + j) % 2)
        bc_first.append(go(_remote(wbc, bc_slots.at[t], bc_sem.at[0, i], bc_sem.at[1, i], peer)))
    bc_slots[t] = wbc[...]

    order = [k for k in range(1, outer_n)]
    order.sort(key=lambda k: -min(k, outer_n - k))

    def block_rows(outer, inner, part):
        size = block // wparts
        return _rows((outer * 2 + inner) * block + part * size, size)

    def send_out(src, dst, cols, sem, part):
        size = block // wparts
        rows = block_rows(z, y, part)
        piece = src.at[part * size : (part + 1) * size, :]
        for k in order:
            go(_remote(piece, dst.at[rows, cols], sem.at[0, k, part], sem.at[1, k, part],
                       _peer((z + k) % outer_n, y, x, c)))
        go(_remote(piece, dst.at[rows, cols], sem.at[2, 0, part], sem.at[3, 0, part],
                   _peer(z, 1 - y, x, c)))

    def pass_on(dst, cols, sem, part):
        for k in order:
            rows = block_rows((z - k) % outer_n, y, part)
            view = dst.at[rows, cols]
            _remote(view, view, sem.at[0, k, part], sem.at[1, k, part], _peer(z, y, x, c)).wait_recv()
            go(_remote(view, view, sem.at[2, k, part], sem.at[3, k, part], _peer(z, 1 - y, x, c)))

    def finish(dst, cols, sem, part):
        for k in range(outer_n):
            view = dst.at[block_rows((z - k) % outer_n, 1 - y, part), cols]
            _remote(view, view, sem.at[2, k, part], sem.at[3, k, part], _peer(z, y, x, c)).wait_recv()

    zx_at = slice(0, zx_cols)
    bc_at = slice(zx_cols, zx_cols + bc_cols)
    dt_at = slice(zx_cols + bc_cols, weight.shape[1])
    all_cols = slice(0, wout.shape[1])
    for part in range(wparts):
        send_out(wzx, weight, zx_at, zx_sem, part)

    for copy in small_first:
        copy.wait_recv()
    total = small[...]
    for i in range(len(dp_peers)):
        total = total + small_d[i]
    small_t[3] = total
    second = []
    for i, (k, j) in enumerate(tensor_peers):
        peer = _peer(z, y, (x + k) % 2, (c + j) % 2)
        second.append(go(_remote(small_t.at[3], small_t.at[i], small_sem_t.at[0, i], small_sem_t.at[1, i], peer)))

    values = resid[...]
    inv = lax.rsqrt(jnp.mean(values * values, axis=-1, keepdims=True) + EPSILON)
    for copy in second:
        copy.wait_recv()
    total = small_t[3]
    for i in range(len(second)):
        total = total + small_t[i]
    small_all[...] = total
    for j in range(model // LANES):
        lanes = slice(j * LANES, (j + 1) * LANES)
        normed_own[:, lanes] = (resid[:, lanes] * inv * total[j : j + 1, :]).astype(BF)

    def token_rows(far, near, part):
        size = own_rows // PARTS
        return _rows((far * 2 + near) * own_rows + part * size, size)

    def send_tokens(src, dst, sem, part):
        size = own_rows // PARTS
        piece = src.at[part * size : (part + 1) * size, :]
        view = dst.at[token_rows(x, c, part), :]
        go(_remote(piece, view, sem.at[0, 0, part], sem.at[1, 0, part], _peer(z, y, 1 - x, c)))
        go(_remote(piece, view, sem.at[0, 1, part], sem.at[1, 1, part], _peer(z, y, x, 1 - c)))

    def pass_tokens(dst, sem, part):
        view = dst.at[token_rows(1 - x, c, part), :]
        _remote(view, view, sem.at[0, 0, part], sem.at[1, 0, part], _peer(z, y, x, c)).wait_recv()
        go(_remote(view, view, sem.at[0, 2, part], sem.at[1, 2, part], _peer(z, y, x, 1 - c)))

    def finish_tokens(dst, sem, part):
        for i, far in ((1, x), (2, 1 - x)):
            view = dst.at[token_rows(far, 1 - c, part), :]
            _remote(view, view, sem.at[0, i, part], sem.at[1, i, part], _peer(z, y, x, c)).wait_recv()

    for part in range(PARTS):
        send_tokens(normed_own, normed_all, norm_sem, part)
    for part in range(PARTS):
        send_tokens(cot_own, cot_all, cot_sem, part)
    for copy in bc_first:
        copy.wait_recv()
    for i in range(4):
        bc_rows[i * wbc.shape[0] : (i + 1) * wbc.shape[0], :] = bc_slots[i]
    for part in range(wparts):
        send_out(bc_rows, weight, bc_at, bd_sem.at[0], part)
        send_out(wdt, weight, dt_at, bd_sem.at[1], part)
        send_out(wout, weight_out, all_cols, wo_sem, part)
    mine = _rows(d * block, block)
    tokens = _rows(t * own_rows, own_rows)
    local = [
        pltpu.make_async_copy(wzx, weight.at[mine, zx_at], local_sem.at[0]),
        pltpu.make_async_copy(bc_rows, weight.at[mine, bc_at], local_sem.at[1]),
        pltpu.make_async_copy(wdt, weight.at[mine, dt_at], local_sem.at[2]),
        pltpu.make_async_copy(wout, weight_out.at[mine, :], local_sem.at[3]),
        pltpu.make_async_copy(normed_own, normed_all.at[tokens, :], local_sem.at[4]),
        pltpu.make_async_copy(cot_own, cot_all.at[tokens, :], local_sem.at[5]),
    ]
    for copy in local:
        copy.start()
    for part in range(max(PARTS, wparts)):
        if part < wparts:
            pass_on(weight, zx_at, zx_sem, part)
        if part < PARTS:
            pass_tokens(normed_all, norm_sem, part)
    for part in range(max(PARTS, wparts)):
        if part < wparts:
            pass_on(weight, bc_at, bd_sem.at[0], part)
            pass_on(weight, dt_at, bd_sem.at[1], part)
            pass_on(weight_out, all_cols, wo_sem, part)
        if part < PARTS:
            pass_tokens(cot_all, cot_sem, part)
    for part in range(wparts):
        finish(weight, zx_at, zx_sem, part)
        finish(weight, bc_at, bd_sem.at[0], part)
        finish(weight, dt_at, bd_sem.at[1], part)
        finish(weight_out, all_cols, wo_sem, part)
    for part in range(PARTS):
        finish_tokens(normed_all, norm_sem, part)
        finish_tokens(cot_all, cot_sem, part)
    for copy in started:
        copy.wait_send()
    for copy in local:
        copy.wait()


def gather_all(small, resid, cot, wzx, wdt, wbc, wout):
    dp, tp = lax.axis_size("dp"), lax.axis_size("tensor")
    outer_n = dp // 2
    block, zx_cols = wzx.shape
    total = zx_cols + wbc.shape[1] + wdt.shape[1]
    vm = pl.BlockSpec(memory_space=pltpu.VMEM)
    hbm = pl.BlockSpec(memory_space=pl.ANY)
    dma = pltpu.SemaphoreType.DMA
    return pl.pallas_call(
        functools.partial(gather_kernel, outer_n),
        in_specs=[vm] * 7,
        out_specs=[vm, hbm, hbm, hbm, hbm],
        out_shape=[jax.ShapeDtypeStruct(small.shape, F32),
                   jax.ShapeDtypeStruct((resid.shape[0] * tp, resid.shape[1]), BF),
                   jax.ShapeDtypeStruct((resid.shape[0] * tp, resid.shape[1]), BF),
                   jax.ShapeDtypeStruct((block * dp, total), BF),
                   jax.ShapeDtypeStruct((block * dp, wout.shape[1]), BF)],
        scratch_shapes=[pltpu.VMEM((4,) + small.shape, F32),
                        pltpu.VMEM((dp - 1,) + small.shape, F32),
                        pltpu.VMEM(resid.shape, BF),
                        pltpu.VMEM(resid.shape, BF),
                        pltpu.VMEM((4,) + wbc.shape, BF),
                        pltpu.VMEM((block, wbc.shape[1]), BF),
                        dma((2, 3)), dma((2, dp - 1)), dma((2, 3)), dma((2, 3, PARTS)), dma((2, 3, PARTS)),
                        dma((4, outer_n, _parts(block))), dma((2, 4, outer_n, _parts(block))), dma((4, outer_n, _parts(block))),
                        dma((6,))],
        compiler_params=pltpu.CompilerParams(collective_id=0, has_side_effects=True),
        cost_estimate=pl.CostEstimate(flops=10**7, bytes_accessed=40 * 2**20, transcendentals=0),
        name="gather_all",
    )(small, resid, cot, wzx, wdt, wbc, wout)


def reduce_kernel(outer_n, small_rows_both, partial, grads, small, resid, gain,
                  d_local, owned, small_out,
                  near_buf, far_src, far_buf, in_buf, out_src, out_buf, small_d, small_t, gain_acc,
                  near_sem, far_sem, in_sem, out_sem, small_sem_d, small_sem_t):
    z, y, x, c = _place()
    own_rows = resid.shape[0]
    model = resid.shape[1]
    block = owned.shape[0]
    pairs_n = partial.shape[0] // (4 * own_rows)
    _greet(outer_n)
    started = []

    def go(copy):
        copy.start()
        started.append(copy)
        return copy

    me = _peer(z, y, x, c)
    size = own_rows // PARTS
    wparts = _parts(block)
    bsize = block // wparts

    def token_rows(far, near, part):
        return _rows((far * 2 + near) * own_rows + part * size, size)

    for part in range(PARTS):
        for i, far in ((0, 1 - x), (1, x)):
            at = pl.ds(part * size, size)
            go(_remote(partial.at[token_rows(far, 1 - c, part), :], near_buf.at[i, at, :],
                       near_sem.at[0, i, part], near_sem.at[1, i, part], _peer(z, y, x, 1 - c)))
    order = [k for k in range(1, outer_n)]
    order.sort(key=lambda k: -min(k, outer_n - k))
    order = order + [0]

    def grad_rows(outer, inner, part):
        return _rows((outer * 2 + inner) * block + part * bsize, bsize)

    for part in range(wparts):
        for k in order:
            at = pl.ds(part * bsize, bsize)
            go(_remote(grads.at[grad_rows((z + k) % outer_n, 1 - y, part), :], in_buf.at[k, at, :],
                       in_sem.at[0, k, part], in_sem.at[1, k, part], _peer(z, 1 - y, x, c)))

    def token_step(part):
        at = pl.ds(part * size, size)
        view = near_buf.at[0, at, :]
        _remote(view, view, near_sem.at[0, 0, part], near_sem.at[1, 0, part], me).wait_recv()
        far_src[at, :] = (partial[token_rows(1 - x, c, part), :].astype(F32) + view[...].astype(F32)).astype(BF)
        go(_remote(far_src.at[at, :], far_buf.at[at, :], far_sem.at[0, part], far_sem.at[1, part],
                   _peer(z, y, 1 - x, c)))

    def grad_step(part):
        at = pl.ds(part * bsize, bsize)
        for k in order:
            view = in_buf.at[k, at, :]
            _remote(view, view, in_sem.at[0, k, part], in_sem.at[1, k, part], me).wait_recv()
            both = grads[grad_rows((z + k) % outer_n, y, part), :].astype(F32) + view[...].astype(F32)
            if k:
                out_src[k - 1, at, :] = both.astype(BF)
                go(_remote(out_src.at[k - 1, at, :], out_buf.at[k - 1, at, :], out_sem.at[0, k - 1, part],
                           out_sem.at[1, k - 1, part], _peer((z + k) % outer_n, y, x, c)))
            else:
                owned[at, :] = both

    for part in range(max(PARTS, wparts)):
        if part < PARTS:
            token_step(part)
        if part < wparts:
            grad_step(part)

    gain_acc[...] = jnp.zeros_like(gain_acc)
    for part in range(PARTS):
        at = pl.ds(part * size, size)
        view, last = near_buf.at[1, at, :], far_buf.at[at, :]
        _remote(view, view, near_sem.at[0, 1, part], near_sem.at[1, 1, part], me).wait_recv()
        _remote(last, last, far_sem.at[0, part], far_sem.at[1, part], me).wait_recv()
        got = partial[token_rows(x, c, part), :].astype(F32) + view[...].astype(F32) + last[...].astype(F32)
        d_local[at, :] = got
        values = resid[at, :]
        inv = lax.rsqrt(jnp.mean(values * values, axis=-1, keepdims=True) + EPSILON)
        gain_acc[...] += _rows_sum(got * values * inv)

    small_d[0] = small[...]
    for j in range(model // LANES):
        small_d[0, j : j + 1, :] = jnp.sum(gain_acc[:, j * LANES : (j + 1) * LANES], axis=0, keepdims=True)
    first = []
    i = 0
    for k in range(outer_n):
        for j in (0, 1):
            if k or j:
                peer = _peer((z + k) % outer_n, (y + j) % 2, x, c)
                first.append(go(_remote(small_d.at[0], small_d.at[k * 2 + j], small_sem_d.at[0, i],
                                        small_sem_d.at[1, i], peer)))
                i += 1
    for part in range(wparts):
        at = pl.ds(part * bsize, bsize)
        total = owned[at, :]
        for k in order[:-1]:
            view = out_buf.at[k - 1, at, :]
            _remote(view, view, out_sem.at[0, k - 1, part], out_sem.at[1, k - 1, part], me).wait_recv()
            total = total + view[...].astype(F32)
        owned[at, :] = total
    for copy in first:
        copy.wait_recv()
    total = None
    for zz in range(outer_n):
        for yy in (0, 1):
            slot = ((z - zz) % outer_n) * 2 + (y - yy) % 2
            term = small_d[slot]
            total = term if total is None else total + term
    small_out[...] = total
    small_t[0] = total[:small_rows_both, :]
    second = []
    i = 0
    for k in (0, 1):
        for j in (0, 1):
            if k or j:
                peer = _peer(z, y, (x + k) % 2, (c + j) % 2)
                second.append(go(_remote(small_t.at[0], small_t.at[k * 2 + j], small_sem_t.at[0, i],
                                         small_sem_t.at[1, i], peer)))
                i += 1
    for copy in second:
        copy.wait_recv()
    small_out[0:small_rows_both, :] = (small_t[0] + small_t[1]) + (small_t[2] + small_t[3])
    for copy in started:
        copy.wait_send()


def reduce_all(partial, grads, small, resid, gain_rows, both_rows):
    dp, tp = lax.axis_size("dp"), lax.axis_size("tensor")
    outer_n = dp // 2
    own_rows, model = resid.shape
    block, cols = grads.shape[0] // dp, grads.shape[1]
    vm = pl.BlockSpec(memory_space=pltpu.VMEM)
    dma = pltpu.SemaphoreType.DMA
    return pl.pallas_call(
        functools.partial(reduce_kernel, outer_n, both_rows),
        in_specs=[vm] * 5,
        out_specs=[vm] * 3,
        out_shape=[jax.ShapeDtypeStruct((own_rows, model), F32),
                   jax.ShapeDtypeStruct((block, cols), F32),
                   jax.ShapeDtypeStruct(small.shape, F32)],
        scratch_shapes=[pltpu.VMEM((2, own_rows, model), BF),
                        pltpu.VMEM((own_rows, model), BF),
                        pltpu.VMEM((own_rows, model), BF),
                        pltpu.VMEM((outer_n, block, cols), BF),
                        pltpu.VMEM((outer_n - 1, block, cols), BF),
                        pltpu.VMEM((outer_n - 1, block, cols), BF),
                        pltpu.VMEM((dp,) + small.shape, F32),
                        pltpu.VMEM((4, both_rows, LANES), F32),
                        pltpu.VMEM((8, model), F32),
                        dma((2, 2, PARTS)), dma((2, PARTS)), dma((2, outer_n, _parts(block))),
                        dma((2, outer_n - 1, _parts(block))), dma((2, dp - 1)), dma((2, 3))],
        compiler_params=pltpu.CompilerParams(collective_id=1, has_side_effects=True,
                                             vmem_limit_bytes=62 * 2**20),
        cost_estimate=pl.CostEstimate(flops=10**7, bytes_accessed=40 * 2**20, transcendentals=0),
        name="reduce_all",
    )(partial, grads, small, resid, gain_rows)


def _spread(values, index, count):
    size = values.shape[-1]
    full = jnp.zeros(values.shape[:-1] + (size * count,), F32)
    return lax.dynamic_update_slice_in_dim(full, values, index * size, axis=values.ndim - 1)


def _own(values, index, count):
    size = values.shape[-1] // count
    return lax.dynamic_slice_in_dim(values, index * size, size, axis=values.ndim - 1)


def on_device(
    resid_in, norm_gain, proj_zx, proj_dt, proj_bc, conv_x_weight, conv_x_bias, conv_bc_weight,
    conv_bc_bias, dt_bias, a_log, skip_gain, gate_gain, proj_out, cotangent,
):
    dp, tp = lax.axis_size("dp"), lax.axis_size("tensor")
    index = lax.axis_index("dp") * tp + lax.axis_index("tensor")
    count = dp * tp
    model = resid_in.shape[-1]
    width = conv_x_weight.shape[1]
    heads = dt_bias.shape[0]
    inner_channels = width * tp
    states2 = 2 * LANES
    rows = proj_zx.shape[0]
    resid, cot = resid_in[0], cotangent[0]
    small = jnp.concatenate([
        _spread(norm_gain, index, count).reshape(-1, LANES),
        _spread(conv_bc_weight, index, count).reshape(-1, LANES),
        _spread(conv_bc_bias, index, count).reshape(-1, LANES)], axis=0)
    gain_rows = model // LANES
    both_rows = -(-small.shape[0] // 8) * 8
    small = pad_rows(small, both_rows)
    dt_cols = jnp.pad(proj_dt, ((0, 0), (0, LANES - heads)))
    small_all, normed, cot_full, weight, out_t = gather_all(
        small, resid, cot, proj_zx.reshape(rows, 2 * width), dt_cols, proj_bc, proj_out.T)
    full_cbw = small_all[gain_rows : gain_rows + 4 * states2 // LANES].reshape(4, states2)
    full_cbb = small_all[gain_rows + 4 * states2 // LANES : gain_rows + 5 * states2 // LANES].reshape(states2)
    full_gain = small_all[:gain_rows].reshape(model)
    proj = jnp.dot(normed, weight, preferred_element_type=F32)
    d_gated = jnp.dot(cot_full, out_t, preferred_element_type=F32)
    packs = pack_params(conv_x_weight, conv_x_bias, full_cbw, full_cbb, dt_bias, a_log, skip_gain, gate_gain)
    y, states, partial = ssd_forward(proj, d_gated, *packs)
    dy, dz, out_partial, grads_zo, ggain = middle(proj, y, d_gated, partial, packs[3], normed, cot_full, out_t, inner_channels)
    d_rest, gx, gbc, gh, block_sum, owned_zo = ssd_backward(proj, y, dy, states, *packs, out_partial, grads_zo)
    block_out = resid + block_sum
    gx = jnp.concatenate([gx.sum(1), ggain.sum(0)[None]], 0)
    gbc, gh = gbc.sum(1), gh.sum(1)
    d_proj = jnp.concatenate([dz, d_rest], axis=1)
    d_normed = lax.dot_general(d_proj, weight, (((1,), (1,)), ((), ())), preferred_element_type=F32).astype(BF)
    grads = lax.dot_general(normed, d_rest, (((0,), (0,)), ((), ())), preferred_element_type=F32).astype(BF)
    to_sum = jnp.concatenate([
        pad_rows(jnp.concatenate([jnp.zeros((gain_rows, LANES), F32), gbc.reshape(-1, LANES)], 0), both_rows),
        gx.reshape(-1, LANES), gh], axis=0)
    to_sum = pad_rows(to_sum, -(-to_sum.shape[0] // 8) * 8)
    d_local, owned, totals = reduce_all(d_normed, grads, to_sum, resid, small_all, both_rows)
    inv_in = lax.rsqrt(jnp.mean(resid * resid, axis=-1, keepdims=True) + EPSILON)
    scaled = resid * inv_in
    d_scaled = d_local * full_gain
    grad_resid = inv_in * (d_scaled - scaled * jnp.mean(d_scaled * scaled, axis=-1, keepdims=True)) + cot
    grad_zx = jnp.stack([owned_zo[:, :width], owned[:, :width]], axis=1)
    bc_part = owned[:, width : width + states2]
    grad_bc = lax.psum_scatter(bc_part.astype(BF), "tensor", scatter_dimension=0, tiled=True).astype(F32)
    grad_dt = owned[:, width + states2 : width + states2 + heads]
    owned_out = owned_zo[:, width:].T
    owned_gain = _own(totals[:gain_rows].reshape(model), index, count)
    at = gain_rows + 4 * states2 // LANES
    owned_cbw = _own(totals[gain_rows:at].reshape(4, states2), index, count)
    owned_cbb = _own(totals[at : at + states2 // LANES].reshape(states2), index, count)
    gx_all = totals[both_rows : both_rows + 7 * width // LANES].reshape(7, width)
    gh_all = totals[both_rows + 7 * width // LANES :]
    skip = gx_all[5].reshape(heads, -1).sum(1)
    return (
        block_out[None], grad_resid[None], owned_gain, grad_zx, grad_dt, grad_bc, gx_all[:4], gx_all[4],
        owned_cbw, owned_cbb, gh_all[0, :heads], gh_all[1, :heads], skip, gx_all[6], owned_out,
    )


def solution(mesh):
    specs = (
        P("dp", "tensor", None), P(("dp", "tensor")), P("dp", None, "tensor"), P("dp", "tensor"),
        P(("dp", "tensor"), None), P(None, "tensor"), P("tensor"), P(None, ("dp", "tensor")),
        P(("dp", "tensor")), P("tensor"), P("tensor"), P("tensor"), P("tensor"), P("tensor", "dp"),
        P("dp", "tensor", None),
    )
    outs = (specs[0], specs[0]) + specs[1:14]
    return jax.shard_map(on_device, mesh=mesh, in_specs=specs, out_specs=outs, check_vma=False)
```

```python
import functools, math
import jax, jax.numpy as jnp
from jax import lax
from jax.experimental import pallas as pl
from jax.experimental.pallas import tpu as pltpu
from jax.sharding import PartitionSpec as P

EPSILON = 1e-05
CHUNK = 128
LANES = 128
TAPS = 4
LOG2E = 1.4426950408889634
BF = jnp.bfloat16
F32 = jnp.float32


MESH = pl.DeviceIdType.MESH
PARTS = 4
ROW_PARTS = 6


def _place():
    d, t = lax.axis_index("dp"), lax.axis_index("tensor")
    return d // 2, d % 2, t // 2, t % 2


def _peer(outer, inner, far, near):
    return (outer * 2 + inner, far * 2 + near)


def _greet(outer_n):
    z, y, x, c = _place()
    barrier = pltpu.get_barrier_semaphore()
    peers = []
    for k in range(outer_n):
        for j in (0, 1):
            if k or j:
                peers.append(_peer((z + k) % outer_n, (y + j) % 2, x, c))
    for k in (0, 1):
        for j in (0, 1):
            if k or j:
                peers.append(_peer(z, y, (x + k) % 2, (c + j) % 2))
    for peer in peers:
        pl.semaphore_signal(barrier, inc=1, device_id=peer, device_id_type=MESH)
    pl.semaphore_wait(barrier, len(peers))


def _parts(rows):
    return max(p for p in range(1, ROW_PARTS + 1) if rows % (16 * p) == 0)


def _remote(src, dst, send, recv, peer):
    return pltpu.make_async_remote_copy(
        src_ref=src, dst_ref=dst, send_sem=send, recv_sem=recv, device_id=peer, device_id_type=MESH)


def _rows(start, size):
    return pl.ds(pl.multiple_of(start, 16), size)


class _Reduction:
    def __init__(self, outer_n, partial, grads, block_sum, owned, own_tokens, near_buf, far_src, far_buf,
                 own_grads, in_buf, out_src, out_buf, near_sem, far_sem, in_sem, out_sem, local_sem):
        self.__dict__.update(locals())
        self.z, self.y, self.x, self.c = _place()
        self.me = _peer(self.z, self.y, self.x, self.c)
        self.own_rows = block_sum.shape[0]
        self.block = owned.shape[0]
        self.wparts = _parts(self.block)
        self.size = self.own_rows // PARTS
        self.bsize = self.block // self.wparts
        order = list(range(1, outer_n))
        order.sort(key=lambda k: -min(k, outer_n - k))
        self.order = order + [0]

    def token_rows(self, far, near, part):
        return _rows((far * 2 + near) * self.own_rows + part * self.size, self.size)

    def grad_rows(self, outer, inner, part):
        return _rows((outer * 2 + inner) * self.block + part * self.bsize, self.bsize)

    def near_copy(self, i, part):
        far = (1 - self.x, self.x)[i]
        at = pl.ds(part * self.size, self.size)
        return _remote(self.partial.at[self.token_rows(far, 1 - self.c, part), :], self.near_buf.at[i, at, :],
                       self.near_sem.at[0, i, part], self.near_sem.at[1, i, part],
                       _peer(self.z, self.y, self.x, 1 - self.c))

    def far_copy(self, part):
        at = pl.ds(part * self.size, self.size)
        return _remote(self.far_src.at[at, :], self.far_buf.at[at, :], self.far_sem.at[0, part],
                       self.far_sem.at[1, part], _peer(self.z, self.y, 1 - self.x, self.c))

    def in_copy(self, k, part):
        at = pl.ds(part * self.bsize, self.bsize)
        rows = self.grad_rows((self.z + k) % self.outer_n, 1 - self.y, part)
        return _remote(self.grads.at[rows, :], self.in_buf.at[k, at, :], self.in_sem.at[0, k, part],
                       self.in_sem.at[1, k, part], _peer(self.z, 1 - self.y, self.x, self.c))

    def out_copy(self, k, part):
        at = pl.ds(part * self.bsize, self.bsize)
        return _remote(self.out_src.at[k - 1, at, :], self.out_buf.at[k - 1, at, :], self.out_sem.at[0, k - 1, part],
                       self.out_sem.at[1, k - 1, part], _peer((self.z + k) % self.outer_n, self.y, self.x, self.c))

    def local_copies(self):
        copies = []
        for i, far in enumerate((1 - self.x, self.x)):
            rows = _rows((far * 2 + self.c) * self.own_rows, self.own_rows)
            copies.append(pltpu.make_async_copy(self.partial.at[rows, :], self.own_tokens.at[i], self.local_sem.at[i]))
        for k in range(self.outer_n):
            rows = _rows((((self.z + k) % self.outer_n) * 2 + self.y) * self.block, self.block)
            copies.append(pltpu.make_async_copy(self.grads.at[rows, :], self.own_grads.at[k], self.local_sem.at[2 + k]))
        return copies

    def begin(self):
        _greet(self.outer_n)
        for part in range(PARTS):
            self.near_copy(0, part).start()
        for k in self.order:
            for part in range(self.wparts):
                self.in_copy(k, part).start()
        for part in range(PARTS):
            self.near_copy(1, part).start()
        for copy in self.local_copies():
            copy.start()

    def ready(self):
        for copy in self.local_copies():
            copy.wait()

    def token_step(self, part):
        at = pl.ds(part * self.size, self.size)
        self.near_copy(0, part).wait_recv()
        self.far_src[at, :] = (self.own_tokens[0, at, :].astype(F32) + self.near_buf[0, at, :].astype(F32)).astype(BF)
        self.far_copy(part).start()

    def grad_step(self, k, part):
        at = pl.ds(part * self.bsize, self.bsize)
        self.in_copy(k, part).wait_recv()
        both = self.own_grads[k, at, :].astype(F32) + self.in_buf[k, at, :].astype(F32)
        if k:
            self.out_src[k - 1, at, :] = both.astype(BF)
            self.out_copy(k, part).start()
        else:
            self.owned[at, :] = both

    def grad_steps(self):
        return [(k, part) for k in self.order for part in range(self.wparts)]

    def plan(self, steps):
        pieces = [(1, self.ready)]
        for part in range(PARTS):
            pieces.append((min(1 + part, steps - 1), functools.partial(self.token_step, part)))
        todo = self.grad_steps()
        self.late = len(todo) // 8
        for i, (k, part) in enumerate(todo[: len(todo) - self.late]):
            pieces.append((min(1 + (i + 2) * (steps - 1) // len(todo), steps - 1),
                           functools.partial(self.grad_step, k, part)))
        return pieces

    def end(self):
        for k, part in self.grad_steps()[-self.late :]:
            self.grad_step(k, part)
        for part in range(PARTS):
            at = pl.ds(part * self.size, self.size)
            self.near_copy(1, part).wait_recv()
            self.far_copy(part).wait_recv()
            self.block_sum[at, :] = (self.own_tokens[1, at, :].astype(F32) + self.near_buf[1, at, :].astype(F32)
                                     + self.far_buf[at, :].astype(F32))
        for part in range(self.wparts):
            at = pl.ds(part * self.bsize, self.bsize)
            total = self.owned[at, :]
            for k in self.order[:-1]:
                self.out_copy(k, part).wait_recv()
                total = total + self.out_buf[k - 1, at, :].astype(F32)
            self.owned[at, :] = total
        for part in range(PARTS):
            self.near_copy(0, part).wait_send()
            self.near_copy(1, part).wait_send()
            self.far_copy(part).wait_send()
        for part in range(self.wparts):
            for k in self.order:
                self.in_copy(k, part).wait_send()
                if k:
                    self.out_copy(k, part).wait_send()


def reduction_scratch(outer_n, tokens, grads):
    dma = pltpu.SemaphoreType.DMA
    parts = _parts(grads[0])
    return [pltpu.VMEM((2,) + tokens, BF), pltpu.VMEM((2,) + tokens, BF), pltpu.VMEM(tokens, BF),
            pltpu.VMEM(tokens, BF), pltpu.VMEM((outer_n,) + grads, BF), pltpu.VMEM((outer_n,) + grads, BF),
            pltpu.VMEM((outer_n - 1,) + grads, BF), pltpu.VMEM((outer_n - 1,) + grads, BF),
            dma((2, 2, PARTS)), dma((2, PARTS)), dma((2, outer_n, parts)), dma((2, outer_n - 1, parts)),
            dma((2 + outer_n,))]


def _sigmoid(v):
    return 1.0 / (1.0 + jnp.exp(-v))


def _softplus(t):
    return jnp.maximum(t, 0.0) + jnp.log1p(jnp.exp(-jnp.abs(t)))


def _dot_last(a, b):
    return lax.dot_general(a, b, (((1,), (1,)), ((), ())), preferred_element_type=F32)


def _dot_exact(a, b):
    return jnp.dot(a, b, precision=lax.Precision.HIGHEST, preferred_element_type=F32)


def _halves(v):
    high = v.astype(BF)
    return high, (v - high.astype(F32)).astype(BF)


def _dot_three(a, b):
    a_high, a_low = _halves(a)
    b_high, b_low = _halves(b)
    return _dot_last(jnp.concatenate([a_high, a_low, a_high], axis=1),
                     jnp.concatenate([b_high, b_high, b_low], axis=1))


def _rows_sum(v):
    return v.reshape(v.shape[0] // 8, 8, v.shape[1]).sum(axis=0)


def _split(lo, v):
    zero = jnp.zeros_like(v)
    return [jnp.where(lo, v, zero), jnp.where(lo, zero, v)]


def _times(dt_raw, head, rows, cols):
    t = dt_raw + head[0:1, :]
    delta = _softplus(t)
    rate = -jnp.exp(head[1:2, :])
    tri = (rows >= cols).astype(F32)
    cum = _dot_exact(tri, delta * (rate * LOG2E))
    return t, delta, rate, cum


def _pair_cols(lo, v, q):
    return jnp.where(lo, v[:, 2 * q : 2 * q + 1], v[:, 2 * q + 1 : 2 * q + 2])


def _conv(buf, start, cols, w, length):
    shifted = [buf[start + k : start + k + length, cols] for k in range(TAPS)]
    v = w[TAPS : TAPS + 1, :] + w[0:1, :] * shifted[0]
    for k in range(1, TAPS):
        v = v + w[k : k + 1, :] * shifted[k]
    return v, shifted


def forward_kernel(width, p_ref, dg_ref, convx_ref, convbc_ref, head_ref, lane_ref,
                   y_ref, h_ref, s_ref, state, xbuf, bcbuf, sums, sum_sem):
    tokens = p_ref.shape[0]
    pairs = width // LANES
    step = pl.program_id(0)
    z, y_at, x, c = _place()
    me = x * 2 + c
    half = sums.shape[1] // 2
    tensor_peers = [_peer(z, y_at, (x + k) % 2, (c + j) % 2) for k in (0, 1) for j in (0, 1) if k or j]

    @pl.when(step == 0)
    def _():
        barrier = pltpu.get_barrier_semaphore()
        for peer in tensor_peers:
            pl.semaphore_signal(barrier, inc=1, device_id=peer, device_id_type=MESH)
        pl.semaphore_wait(barrier, len(tensor_peers))
        state[...] = jnp.zeros_like(state)
        xbuf[0:8, :] = jnp.zeros((8, width), F32)
        bcbuf[0:8, :] = jnp.zeros((8, 2 * LANES), F32)

    @pl.when(step > 0)
    def _():
        xbuf[0:8, :] = xbuf[tokens : tokens + 8, :]
        bcbuf[0:8, :] = bcbuf[tokens : tokens + 8, :]

    xbuf[8 : 8 + tokens, :] = p_ref[:, width : 2 * width]
    bcbuf[8 : 8 + tokens, :] = p_ref[:, 2 * width : 2 * width + 2 * LANES]
    rows = lax.broadcasted_iota(jnp.int32, (CHUNK, CHUNK), 0)
    cols = lax.broadcasted_iota(jnp.int32, (CHUNK, CHUNK), 1)
    lo = cols < LANES // 2
    head = head_ref[...]
    ones = jnp.ones((8, LANES), F32)
    for sub in range(tokens // CHUNK):
        base = sub * CHUNK
        span = slice(base, base + CHUNK)
        vbc, _ = _conv(bcbuf, base + 5, slice(0, 2 * LANES), convbc_ref[...], CHUNK)
        bc = vbc * _sigmoid(vbc)
        b_in, c_out = bc[:, :LANES], bc[:, LANES:]
        c_high, c_low = _halves(c_out)
        c_wide = jnp.concatenate([c_high, c_low, c_high], axis=1)
        _, delta, _, cum = _times(p_ref[span, 2 * width + 2 * LANES :], head, rows, cols)
        cum_t = cum.T
        scores = jnp.where(rows >= cols, _dot_three(c_out, b_in), 0.0)
        last = cum[CHUNK - 1 : CHUNK, :]
        tail = jnp.exp2(last - cum)
        grow = jnp.exp2(cum)
        decay = jnp.exp2(last)
        b_t = b_in.T.astype(BF)
        squares = jnp.zeros((CHUNK, LANES), F32)
        inner = jnp.zeros((CHUNK, LANES), F32)
        h_ref[sub] = state[...]
        for q in range(pairs):
            lanes = slice(q * LANES, (q + 1) * LANES)
            v, _ = _conv(xbuf, base + 5, lanes, convx_ref[:, lanes], CHUNK)
            x_act = v * _sigmoid(v)
            u = x_act * _pair_cols(lo, delta, q)
            left = []
            for h in (2 * q, 2 * q + 1):
                e = jnp.exp2(jnp.minimum(cum[:, h : h + 1] - cum_t[h : h + 1, :], 0.0))
                left.append((e * scores).astype(BF))
            held = state[:, lanes]
            held_high, held_low = _halves(held)
            y = jnp.dot(jnp.concatenate(left, axis=1), jnp.concatenate(_split(lo, u.astype(BF)), axis=0),
                        preferred_element_type=F32)
            outer = jnp.dot(c_wide, jnp.concatenate([held_high, held_high, held_low], axis=0),
                            preferred_element_type=F32)
            y = y + outer * _pair_cols(lo, grow, q) + lane_ref[0:1, lanes] * x_act
            y_ref[span, lanes] = y
            uw = (u * _pair_cols(lo, tail, q)).astype(BF)
            factor = _pair_cols(lo[0:1, :], decay, q)
            state[:, lanes] = held * factor + jnp.dot(b_t, uw, preferred_element_type=F32)
            z = p_ref[span, lanes]
            product = y * (z * _sigmoid(z))
            squares = squares + product * product
            inner = inner + dg_ref[span, lanes].astype(F32) * lane_ref[1:2, lanes] * product
        row_sq = lax.dot_general(ones, squares, (((1,), (1,)), ((), ())),
                                 precision=lax.Precision.HIGHEST, preferred_element_type=F32)
        row_in = lax.dot_general(ones, inner, (((1,), (1,)), ((), ())),
                                 precision=lax.Precision.HIGHEST, preferred_element_type=F32)
        at = step * (tokens // CHUNK) + sub
        sums[me, pl.ds(at, 1), :] = row_sq[0:1, :]
        sums[me, pl.ds(half + at, 1), :] = row_in[0:1, :]

    @pl.when(step == pl.num_programs(0) - 1)
    def _():
        copies = [_remote(sums.at[me], sums.at[me], sum_sem.at[0, i], sum_sem.at[1, i], peer)
                  for i, peer in enumerate(tensor_peers)]
        for copy in copies:
            copy.start()
        for copy in copies:
            copy.wait_recv()
        s_ref[...] = (sums[0] + sums[1]) + (sums[2] + sums[3])
        for copy in copies:
            copy.wait_send()


def backward_kernel(width, outer_n, p_ref, prev_ref, y_ref, dy_ref, h_ref,
                    convx_ref, convbc_ref, head_ref, lane_ref, partial, grads,
                    dp_ref, gx_ref, gbc_ref, gh_ref, block_sum, owned,
                    grad_state, carry_hg, xbuf, bcbuf, dvx, dvbc, *comm):
    tokens = p_ref.shape[0]
    pairs = width // LANES
    step = pl.program_id(0)
    is_first_block = step == pl.num_programs(0) - 1
    length = partial.shape[0]
    reduction = _Reduction(outer_n, partial, grads, block_sum, owned, *comm)

    @pl.when(step == 0)
    def _():
        reduction.begin()

    for at, piece in reduction.plan(length // tokens):
        @pl.when(step == at)
        def _(piece=piece):
            piece()

    @pl.when(step == 0)
    def _():
        grad_state[...] = jnp.zeros_like(grad_state)
        carry_hg[...] = jnp.zeros_like(carry_hg)
        dvx[0:8, :] = jnp.zeros((8, width), F32)
        dvbc[0:8, :] = jnp.zeros((8, 2 * LANES), F32)
        gx_ref[...] = jnp.zeros_like(gx_ref)
        gbc_ref[...] = jnp.zeros_like(gbc_ref)
        gh_ref[...] = jnp.zeros_like(gh_ref)

    keep = jnp.where(is_first_block, 0.0, 1.0)
    xbuf[0:8, :] = prev_ref[:, width : 2 * width] * keep
    bcbuf[0:8, :] = prev_ref[:, 2 * width : 2 * width + 2 * LANES] * keep
    xbuf[8 : 8 + tokens, :] = p_ref[:, width : 2 * width]
    bcbuf[8 : 8 + tokens, :] = p_ref[:, 2 * width : 2 * width + 2 * LANES]
    rows = lax.broadcasted_iota(jnp.int32, (CHUNK, CHUNK), 0)
    cols = lax.broadcasted_iota(jnp.int32, (CHUNK, CHUNK), 1)
    lo = cols < LANES // 2
    head = head_ref[...]
    for sub in reversed(range(tokens // CHUNK)):
        base = sub * CHUNK
        span = slice(base, base + CHUNK)
        vbc, shifted_bc = _conv(bcbuf, base + 5, slice(0, 2 * LANES), convbc_ref[...], CHUNK)
        sbc = _sigmoid(vbc)
        bc = vbc * sbc
        b_in, c_out = bc[:, :LANES], bc[:, LANES:]
        b_half, c_half = b_in.astype(BF), c_out.astype(BF)
        t, delta, rate, cum = _times(p_ref[span, 2 * width + 2 * LANES :], head, rows, cols)
        cum_t = cum.T
        causal_t = cols >= rows
        scores_t = jnp.where(causal_t, _dot_three(b_in, c_out), 0.0)
        last = cum[CHUNK - 1 : CHUNK, :]
        tail = jnp.exp2(last - cum)
        grow = jnp.exp2(cum)
        decay = jnp.exp2(last)
        c_t = c_out.T.astype(BF)
        d_scores = jnp.zeros((CHUNK, CHUNK), F32)
        d_b = jnp.zeros((CHUNK, LANES), F32)
        d_c = jnp.zeros((CHUNK, LANES), F32)
        per_head = jnp.zeros((CHUNK, LANES), F32)
        hg_heads = jnp.zeros((8, LANES), F32)
        dvx[CHUNK : CHUNK + 8, :] = dvx[0:8, :]
        dvbc[CHUNK : CHUNK + 8, :] = dvbc[0:8, :]
        for q in range(pairs):
            lanes = slice(q * LANES, (q + 1) * LANES)
            wide = _pair_cols(lo, delta, q)
            skip = lane_ref[0:1, lanes]
            v, shifted = _conv(xbuf, base + 5, lanes, convx_ref[:, lanes], CHUNK)
            sv = _sigmoid(v)
            x_act = v * sv
            u = x_act * wide
            u_half = u.astype(BF)
            y = y_ref[span, lanes]
            dy_half = dy_ref[span, lanes]
            dy = dy_half.astype(F32)
            dy_block = jnp.concatenate(_split(lo, dy_half), axis=0)
            d_m = _dot_last(u_half, dy_block)
            left, left_b = [], []
            for a in (0, 1):
                h = 2 * q + a
                e = jnp.exp2(jnp.minimum(cum_t[h : h + 1, :] - cum[:, h : h + 1], 0.0))
                left.append((e * scores_t).astype(BF))
                d_scores = d_scores + e * d_m[:, a * CHUNK : (a + 1) * CHUNK]
                left_b.append((b_in * tail[:, h : h + 1]).astype(BF))
            g_held = grad_state[:, lanes]
            g_half, g_low = _halves(g_held)
            h_held = h_ref[sub, :, lanes]
            h_half, h_low = _halves(h_held)
            right = jnp.concatenate([dy_block] + _split(lo, g_half), axis=0)
            du = jnp.dot(jnp.concatenate(left + left_b, axis=1), right, preferred_element_type=F32)
            dx = du * wide + skip * dy
            dv = dx * (sv * (1.0 + v * (1.0 - sv)))
            dvx[0:CHUNK, lanes] = dv
            w = convx_ref[:, lanes]
            d_in = w[TAPS - 1 : TAPS, :] * dv
            for k in range(TAPS - 1):
                ahead = TAPS - 1 - k
                d_in = d_in + w[k : k + 1, :] * dvx[ahead : ahead + CHUNK, lanes]
            dp_ref[span, lanes] = d_in.astype(BF)
            for k in range(TAPS):
                gx_ref[k, :, lanes] += _rows_sum(dv * shifted[k])
            gx_ref[4, :, lanes] += _rows_sum(dv)
            gx_ref[5, :, lanes] += _rows_sum(dy * x_act)
            edy = (dy * _pair_cols(lo, grow, q)).astype(BF)
            uw = (u * _pair_cols(lo, tail, q)).astype(BF)
            d_c = d_c + _dot_last(jnp.concatenate([edy, edy], axis=1), jnp.concatenate([h_half, h_low], axis=1))
            d_b = d_b + _dot_last(jnp.concatenate([uw, uw], axis=1), jnp.concatenate([g_half, g_low], axis=1))
            g_new = g_held * _pair_cols(lo[0:1, :], decay, q) + jnp.dot(
                c_t, edy, preferred_element_type=F32)
            grad_state[:, lanes] = g_new
            r1 = x_act * du
            r2 = dy * (y - skip * x_act)
            sel1 = (cols == 2 * q + (rows >= LANES // 2).astype(jnp.int32)).astype(BF)
            sel2 = (cols == LANES // 2 + 2 * q + (rows >= LANES // 2).astype(jnp.int32)).astype(BF)
            r1h = r1.astype(BF)
            r1l = (r1 - r1h.astype(F32)).astype(BF)
            r2h = r2.astype(BF)
            r2l = (r2 - r2h.astype(F32)).astype(BF)
            per_head = per_head + jnp.dot(
                jnp.concatenate([r1h, r1l, r2h, r2l], axis=1),
                jnp.concatenate([sel1, sel1, sel2, sel2], axis=0), preferred_element_type=F32)
            hg_heads = hg_heads + _dot_exact(carry_hg[:, lanes], sel1.astype(F32))
            carry_hg[:, lanes] = _rows_sum(g_new * h_held)
        d_scores = jnp.where(causal_t, d_scores, 0.0)
        ds_half = d_scores.astype(BF)
        d_b = d_b + jnp.dot(ds_half, c_half, preferred_element_type=F32)
        d_c = d_c + jnp.dot(d_scores.T.astype(BF), b_half, preferred_element_type=F32)
        dvb = jnp.concatenate([d_b, d_c], axis=1) * (sbc * (1.0 + vbc * (1.0 - sbc)))
        dvbc[0:CHUNK, :] = dvb
        wbc = convbc_ref[...]
        d_bc = wbc[TAPS - 1 : TAPS, :] * dvb
        for k in range(TAPS - 1):
            ahead = TAPS - 1 - k
            d_bc = d_bc + wbc[k : k + 1, :] * dvbc[ahead : ahead + CHUNK, :]
        dp_ref[span, width : width + 2 * LANES] = d_bc.astype(BF)
        for k in range(TAPS):
            gbc_ref[k] += _rows_sum(dvb * shifted_bc[k])
        gbc_ref[4] += _rows_sum(dvb)
        direct = per_head
        through = pltpu.roll(per_head, LANES // 2, 1)
        d_cum = through - delta * direct
        suffix = _dot_exact((cols >= rows).astype(F32), d_cum)
        d_log = suffix + jnp.sum(hg_heads, axis=0, keepdims=True)
        valid = cols < 2 * pairs
        d_delta = direct + rate * d_log
        d_dt = jnp.where(valid, d_delta * _sigmoid(t), 0.0)
        dp_ref[span, width + 2 * LANES :] = d_dt.astype(BF)
        gh_ref[0] += _rows_sum(d_dt)
        gh_ref[1] += _rows_sum(jnp.where(valid, delta * d_log, 0.0)) * rate

    @pl.when(is_first_block)
    def _():
        reduction.end()


def ssd_forward(proj, dg, convx, convbc, head, lane, tokens=256):
    length, total = proj.shape
    width = convx.shape[1]
    subs = tokens // CHUNK
    whole = lambda a: pl.BlockSpec(a.shape, lambda i: (0,) * a.ndim)
    return pl.pallas_call(
        functools.partial(forward_kernel, width),
        grid=(length // tokens,),
        in_specs=[pl.BlockSpec((tokens, total), lambda i: (i, 0)),
                  pl.BlockSpec((tokens, width), lambda i: (i, 0)),
                  whole(convx), whole(convbc), whole(head), whole(lane)],
        out_specs=[pl.BlockSpec((tokens, width), lambda i: (i, 0)),
                   pl.BlockSpec((subs, LANES, width), lambda i: (i, 0, 0)),
                   pl.BlockSpec((2 * length // CHUNK, CHUNK), lambda i: (0, 0))],
        out_shape=[jax.ShapeDtypeStruct((length, width), F32),
                   jax.ShapeDtypeStruct((length // CHUNK, LANES, width), F32),
                   jax.ShapeDtypeStruct((2 * length // CHUNK, CHUNK), F32)],
        scratch_shapes=[pltpu.VMEM((LANES, width), F32),
                        pltpu.VMEM((tokens + 8, width), F32),
                        pltpu.VMEM((tokens + 8, 2 * LANES), F32),
                        pltpu.VMEM((4, 2 * length // CHUNK, CHUNK), F32),
                        pltpu.SemaphoreType.DMA((2, 3))],
        compiler_params=pltpu.CompilerParams(collective_id=2, has_side_effects=True),
        cost_estimate=pl.CostEstimate(flops=4 * 10**9, bytes_accessed=30 * 2**20, transcendentals=10**7),
        name="scan_forward",
    )(proj, dg, convx, convbc, head, lane)


def ssd_backward(proj, y, dy, states, convx, convbc, head, lane, partial, grads, tokens=256):
    length, total = proj.shape
    width = convx.shape[1]
    subs = tokens // CHUNK
    n = length // tokens
    dp, tp = lax.axis_size("dp"), lax.axis_size("tensor")
    whole = lambda a: pl.BlockSpec(a.shape, lambda i: (0,) * a.ndim)
    rev = lambda i: (n - 1 - i, 0)
    own = lambda shape: pl.BlockSpec(shape, lambda i: (0, 0))
    hbm = pl.BlockSpec(memory_space=pl.ANY)
    block_shape = (length // tp, partial.shape[1])
    owned_shape = (grads.shape[0] // dp, grads.shape[1])
    return pl.pallas_call(
        functools.partial(backward_kernel, width, dp // 2),
        grid=(n,),
        in_specs=[pl.BlockSpec((tokens, total), rev),
                  pl.BlockSpec((8, total), lambda i: (jnp.maximum((n - 1 - i) * (tokens // 8) - 1, 0), 0)),
                  pl.BlockSpec((tokens, width), rev),
                  pl.BlockSpec((tokens, width), rev),
                  pl.BlockSpec((subs, LANES, width), lambda i: (n - 1 - i, 0, 0)),
                  whole(convx), whole(convbc), whole(head), whole(lane), hbm, hbm],
        out_specs=[pl.BlockSpec((tokens, total - width), rev),
                   pl.BlockSpec((6, 8, width), lambda i: (0, 0, 0)),
                   pl.BlockSpec((5, 8, 2 * LANES), lambda i: (0, 0, 0)),
                   pl.BlockSpec((2, 8, LANES), lambda i: (0, 0, 0)),
                   own(block_shape), own(owned_shape)],
        out_shape=[jax.ShapeDtypeStruct((length, total - width), BF),
                   jax.ShapeDtypeStruct((6, 8, width), F32),
                   jax.ShapeDtypeStruct((5, 8, 2 * LANES), F32),
                   jax.ShapeDtypeStruct((2, 8, LANES), F32),
                   jax.ShapeDtypeStruct(block_shape, F32),
                   jax.ShapeDtypeStruct(owned_shape, F32)],
        scratch_shapes=[pltpu.VMEM((LANES, width), F32),
                        pltpu.VMEM((8, width), F32),
                        pltpu.VMEM((tokens + 8, width), F32),
                        pltpu.VMEM((tokens + 8, 2 * LANES), F32),
                        pltpu.VMEM((CHUNK + 8, width), F32),
                        pltpu.VMEM((CHUNK + 8, 2 * LANES), F32)] + reduction_scratch(dp // 2, block_shape, owned_shape),
        compiler_params=pltpu.CompilerParams(collective_id=3, has_side_effects=True, vmem_limit_bytes=62 * 2**20),
        cost_estimate=pl.CostEstimate(flops=12 * 10**9, bytes_accessed=50 * 2**20, transcendentals=10**7),
        name="scan_backward",
    )(proj, proj, y, dy, states, convx, convbc, head, lane, partial, grads)


def middle_kernel(width, inner_channels, z_ref, y_ref, dg_ref, s_ref, lane_ref, normed, cot, out_t,
                  dy_ref, dz_ref, out_ref, grads_ref, gg_ref, gated, acc_z, acc_o):
    tokens = z_ref.shape[0]
    step = pl.program_id(0)
    half = s_ref.shape[0] // 2

    @pl.when(step == 0)
    def _():
        gg_ref[...] = jnp.zeros_like(gg_ref)
        acc_z[...] = jnp.zeros_like(acc_z)
        acc_o[...] = jnp.zeros_like(acc_o)

    for sub in range(tokens // CHUNK):
        span = slice(sub * CHUNK, (sub + 1) * CHUNK)
        at = step * (tokens // CHUNK) + sub
        wide = lambda row: jnp.broadcast_to(row, (8, CHUNK)).T[:, 0:1]
        squares, dots = wide(s_ref[pl.ds(at, 1), :]), wide(s_ref[pl.ds(half + at, 1), :])
        inv = lax.rsqrt(squares / inner_channels + EPSILON)
        mean = inv * dots / inner_channels
        for q in range(width // LANES):
            lanes = slice(q * LANES, (q + 1) * LANES)
            gain = lane_ref[1:2, lanes]
            y, z, dg = y_ref[span, lanes], z_ref[span, lanes], dg_ref[span, lanes]
            sz = _sigmoid(z)
            act = z * sz
            quot = y * act * inv
            gg_ref[:, lanes] += _rows_sum(dg * quot)
            gated[span, lanes] = (quot * gain).astype(BF)
            d_prod = inv * (dg * gain - quot * mean)
            dy_ref[span, lanes] = (d_prod * act).astype(BF)
            dz_ref[span, lanes] = (d_prod * y * sz * (1.0 + z * (1.0 - sz))).astype(BF)
    out_ref[...] = _dot_last(gated[...], out_t[...]).astype(BF)
    first = lambda a, b: lax.dot_general(a, b, (((0,), (0,)), ((), ())), preferred_element_type=F32)
    acc_z[...] += first(normed[...], dz_ref[...])
    acc_o[...] += first(cot[...], gated[...])

    @pl.when(step == pl.num_programs(0) - 1)
    def _():
        grads_ref[:, :width] = acc_z[...].astype(BF)
        grads_ref[:, width:] = acc_o[...].astype(BF)


def middle(proj, y, dg, sums, lane, normed, cot, out_t, inner_channels, tokens=512):
    length, model = normed.shape
    width = y.shape[1]
    at = lambda cols: pl.BlockSpec((tokens, cols), lambda i: (i, 0))
    once = lambda shape: pl.BlockSpec(shape, lambda i: (0, 0), pipeline_mode=pl.Buffered(1))
    return pl.pallas_call(
        functools.partial(middle_kernel, width, inner_channels),
        grid=(length // tokens,),
        in_specs=[at(width), at(width), at(width), once(sums.shape), once(lane.shape), at(model), at(model),
                  once(out_t.shape)],
        out_specs=[at(width), at(width), at(model), once((model, 2 * width)), once((8, width))],
        out_shape=[jax.ShapeDtypeStruct((length, width), BF),
                   jax.ShapeDtypeStruct((length, width), BF),
                   jax.ShapeDtypeStruct((length, model), BF),
                   jax.ShapeDtypeStruct((model, 2 * width), BF),
                   jax.ShapeDtypeStruct((8, width), F32)],
        scratch_shapes=[pltpu.VMEM((tokens, width), BF),
                        pltpu.VMEM((model, width), F32),
                        pltpu.VMEM((model, width), F32)],
        cost_estimate=pl.CostEstimate(flops=15 * 10**9, bytes_accessed=50 * 2**20, transcendentals=10**6),
        name="middle",
    )(proj, y, dg, sums, lane, normed, cot, out_t)


def pad_rows(a, rows):
    return jnp.pad(a, ((0, rows - a.shape[0]), (0, 0)))


def pack_params(conv_x_weight, conv_x_bias, conv_bc_weight, conv_bc_bias, dt_bias, a_log, skip_gain, gate_gain):
    width = conv_x_weight.shape[1]
    convx = pad_rows(jnp.concatenate([conv_x_weight, conv_x_bias[None]], 0), 8)
    convbc = pad_rows(jnp.concatenate([conv_bc_weight, conv_bc_bias[None]], 0), 8)
    heads = dt_bias.shape[0]
    head = jnp.pad(jnp.stack([dt_bias, a_log]), ((0, 6), (0, LANES - heads)))
    lane = pad_rows(jnp.stack([jnp.repeat(skip_gain, width // heads), gate_gain]), 8)
    return convx, convbc, head, lane
def gather_kernel(outer_n, heads, small, wzx, wdt, wbc, wout, resid_in, cot_in,
                  small_all, normed_out, cot_out, weight_out, wout_out, proj, d_gated,
                  normed, cot, weight, w_out, resid, cot_f, stage, stage_g,
                  small_t, small_d, bc_slots, dt_slots,
                  small_sem_t, small_sem_d, bc_sem_t, bc_sem_d, dt_sem, norm_sem, cot_sem, zx_sem, wo_sem,
                  local_sem, stage_sem, stage_g_sem):
    z, y, x, c = _place()
    me = _peer(z, y, x, c)
    t = x * 2 + c
    d = z * 2 + y
    block, zx_cols = wzx.shape
    bc_cols = wbc.shape[1]
    bc_rows = wbc.shape[0]
    wparts = _parts(block)
    bsize = block // wparts
    own_rows, model = resid.shape
    size = own_rows // PARTS
    length = normed.shape[0]
    tile = stage.shape[1]
    loads = [pltpu.make_async_copy(resid_in, resid, local_sem.at[0]),
             pltpu.make_async_copy(cot_in, cot_f, local_sem.at[1])]
    for copy in loads:
        copy.start()
    _greet(outer_n)
    dp_peers = [(k, j) for k in range(outer_n) for j in (0, 1) if k or j]
    tensor_peers = [(k, j) for k in (0, 1) for j in (0, 1) if k or j]
    order = list(range(1, outer_n))
    order.sort(key=lambda k: -min(k, outer_n - k))
    at_dp = lambda k, j: _peer((z + k) % outer_n, (y + j) % 2, x, c)
    at_tensor = lambda k, j: _peer(z, y, (x + k) % 2, (c + j) % 2)

    small_first = [_remote(small, small_d.at[i], small_sem_d.at[0, i], small_sem_d.at[1, i], at_dp(k, j))
                   for i, (k, j) in enumerate(dp_peers)]
    bc_first = [_remote(wbc, bc_slots.at[t, d], bc_sem_d.at[0, i], bc_sem_d.at[1, i], at_dp(k, j))
                for i, (k, j) in enumerate(dp_peers)]
    dt_first = [_remote(wdt, dt_slots.at[d], dt_sem.at[0, i], dt_sem.at[1, i], at_dp(k, j))
                for i, (k, j) in enumerate(dp_peers)]
    for copy in small_first + bc_first + dt_first:
        copy.start()

    def rows_of(outer, inner, part):
        return _rows((outer * 2 + inner) * block + part * bsize, bsize)

    def across(src, dst, cols, sem, k, part):
        return _remote(src.at[pl.ds(part * bsize, bsize), :], dst.at[rows_of(z, y, part), cols],
                       sem.at[0, k, part], sem.at[1, k, part], _peer(lax.rem(z + k, outer_n), y, x, c))

    def beside(src, dst, cols, sem, part):
        return _remote(src.at[pl.ds(part * bsize, bsize), :], dst.at[rows_of(z, y, part), cols],
                       sem.at[2, 0, part], sem.at[3, 0, part], _peer(z, 1 - y, x, c))

    def onward(dst, cols, sem, k, part):
        view = dst.at[rows_of(lax.rem(z - k + outer_n, outer_n), y, part), cols]
        return _remote(view, view, sem.at[2, k, part], sem.at[3, k, part], _peer(z, 1 - y, x, c))

    def send_out(src, dst, cols, sem):
        for part in range(wparts):
            for k in order:
                across(src, dst, cols, sem, k, part).start()
            beside(src, dst, cols, sem, part).start()

    def pass_on(src, dst, cols, sem, part):
        for k in order:
            across(src, dst, cols, sem, k, part).wait_recv()
            onward(dst, cols, sem, k, part).start()

    def finish(src, dst, cols, sem):
        for part in range(wparts):
            for k in range(outer_n):
                onward(dst, cols, sem, k, part).wait_recv()

    def finish_sends(src, dst, cols, sem):
        for part in range(wparts):
            beside(src, dst, cols, sem, part).wait_send()
            for k in order:
                across(src, dst, cols, sem, k, part).wait_send()
                onward(dst, cols, sem, k, part).wait_send()

    zx = (wzx, weight, pl.ds(0, zx_cols), zx_sem)
    wo = (wout, w_out, pl.ds(0, wout.shape[1]), wo_sem)
    send_out(*zx)
    mine = _rows(d * block, block)
    place = [pltpu.make_async_copy(wzx, weight.at[mine, pl.ds(0, zx_cols)], local_sem.at[2]),
             pltpu.make_async_copy(wout, w_out.at[mine, :], local_sem.at[3])]
    for copy in place:
        copy.start()
    bc_slots[t, d] = wbc[...]
    dt_slots[d] = wdt[...]
    loads[0].wait()
    values = resid[...]
    inv = lax.rsqrt(jnp.mean(values * values, axis=-1, keepdims=True) + EPSILON)

    for copy in small_first + bc_first:
        copy.wait_recv()
    total = small[...]
    for i in range(len(dp_peers)):
        total = total + small_d[i]
    small_t[3] = total
    small_second = [_remote(small_t.at[3], small_t.at[i], small_sem_t.at[0, i], small_sem_t.at[1, i], at_tensor(k, j))
                    for i, (k, j) in enumerate(tensor_peers)]
    bc_second = [_remote(bc_slots.at[t], bc_slots.at[t], bc_sem_t.at[0, i], bc_sem_t.at[1, i], at_tensor(k, j))
                 for i, (k, j) in enumerate(tensor_peers)]
    for copy in small_second:
        copy.start()
    send_out(*wo)
    for copy in small_second:
        copy.wait_recv()
    total = small_t[3]
    for i in range(3):
        total = total + small_t[i]
    small_all[...] = total
    own_at = _rows(t * own_rows, own_rows)
    for j in range(model // LANES):
        lanes = slice(j * LANES, (j + 1) * LANES)
        normed[own_at, lanes] = (resid[:, lanes] * inv * total[j : j + 1, :]).astype(BF)

    def token_rows(far, near, part):
        return _rows((far * 2 + near) * own_rows + part * size, size)

    def token_copy(buf, sem, which, part):
        far = 1 - x if which == 2 else x
        view = buf.at[token_rows(far, c, part), :]
        peer = _peer(z, y, 1 - x, c) if which == 0 else _peer(z, y, x, 1 - c)
        return _remote(view, view, sem.at[0, which, part], sem.at[1, which, part], peer)

    def send_tokens(buf, sem):
        for part in range(PARTS):
            token_copy(buf, sem, 0, part).start()
            token_copy(buf, sem, 1, part).start()

    def pass_tokens(buf, sem, part):
        token_copy(buf, sem, 0, part).wait_recv()
        token_copy(buf, sem, 2, part).start()

    def finish_tokens(buf, sem):
        for part in range(PARTS):
            token_copy(buf, sem, 1, part).wait_recv()
            token_copy(buf, sem, 2, part).wait_recv()

    send_tokens(normed, norm_sem)
    for copy in bc_second:
        copy.start()
    loads[1].wait()
    cot[own_at, :] = cot_f[...].astype(BF)
    send_tokens(cot, cot_sem)
    for copy in dt_first:
        copy.wait_recv()
    for copy in place:
        copy.wait()
    for i in range(outer_n * 2):
        columns = dt_slots[i].astype(F32)
        columns = jnp.concatenate([columns, jnp.zeros((LANES - columns.shape[0], columns.shape[1]), F32)], axis=0)
        weight[i * block : (i + 1) * block, zx_cols + bc_cols :] = columns.T[:block, :].astype(BF)
    for part in range(max(PARTS, wparts)):
        if part < wparts:
            pass_on(*zx, part)
        if part < PARTS:
            pass_tokens(normed, norm_sem, part)
    for copy in bc_second:
        copy.wait_recv()
    for i in range(outer_n * 2):
        for j in range(4):
            first = i * block + j * bc_rows
            weight[first : first + bc_rows, zx_cols : zx_cols + bc_cols] = bc_slots[j, i]
    finish_tokens(normed, norm_sem)
    finish(*zx)
    save = [pltpu.make_async_copy(normed, normed_out, local_sem.at[4]),
            pltpu.make_async_copy(weight, weight_out, local_sem.at[5])]
    for copy in save:
        copy.start()

    steps = length // tile

    def store(ref, buf, sem, i):
        slot = lax.rem(i, 2)
        return pltpu.make_async_copy(buf.at[slot], ref.at[pl.ds(pl.multiple_of(i * tile, tile), tile), :], sem.at[slot])

    @pl.loop(0, steps)
    def _(i):
        @pl.when(i >= 2)
        def _():
            store(proj, stage, stage_sem, i - 2).wait()

        rows = pl.ds(pl.multiple_of(i * tile, tile), tile)
        stage[lax.rem(i, 2)] = jnp.dot(normed[rows, :], weight[...], preferred_element_type=F32)
        store(proj, stage, stage_sem, i).start()

        @pl.when(i < wparts)
        def _():
            pass_on(*wo, i)

        @pl.when(i < PARTS)
        def _():
            pass_tokens(cot, cot_sem, i)

    for i in range(steps, wparts):
        pass_on(*wo, i)
    for i in range(steps, PARTS):
        pass_tokens(cot, cot_sem, i)
    finish_tokens(cot, cot_sem)
    finish(*wo)
    save_late = [pltpu.make_async_copy(cot, cot_out, local_sem.at[6]),
                 pltpu.make_async_copy(w_out, wout_out, local_sem.at[7])]
    for copy in save_late:
        copy.start()

    @pl.loop(0, steps)
    def _(i):
        @pl.when(i >= 2)
        def _():
            store(d_gated, stage_g, stage_g_sem, i - 2).wait()

        rows = pl.ds(pl.multiple_of(i * tile, tile), tile)
        stage_g[lax.rem(i, 2)] = jnp.dot(cot[rows, :], w_out[...], preferred_element_type=F32)
        store(d_gated, stage_g, stage_g_sem, i).start()

    for i in range(max(steps - 2, 0), steps):
        store(proj, stage, stage_sem, i).wait()
        store(d_gated, stage_g, stage_g_sem, i).wait()
    finish_sends(*zx)
    finish_sends(*wo)
    for part in range(PARTS):
        for which in range(3):
            token_copy(normed, norm_sem, which, part).wait_send()
            token_copy(cot, cot_sem, which, part).wait_send()
    for copy in small_first + bc_first + dt_first + small_second + bc_second:
        copy.wait_send()
    for copy in save + save_late:
        copy.wait()


def gather_all(small, resid, cot, wzx, wdt, wbc, wout, tile=256):
    dp, tp = lax.axis_size("dp"), lax.axis_size("tensor")
    outer_n = dp // 2
    block, zx_cols = wzx.shape
    total = zx_cols + wbc.shape[1] + LANES
    width = wout.shape[1]
    heads = wdt.shape[1]
    length, model = resid.shape[0] * tp, resid.shape[1]
    wdt = jnp.pad(wdt.T, ((0, -heads % 16), (0, -block % LANES)))
    wparts = _parts(block)
    vm = pl.BlockSpec(memory_space=pltpu.VMEM)
    hbm = pl.BlockSpec(memory_space=pl.ANY)
    dma = pltpu.SemaphoreType.DMA
    shape = jax.ShapeDtypeStruct
    return pl.pallas_call(
        functools.partial(gather_kernel, outer_n, heads),
        in_specs=[vm] * 5 + [hbm] * 2,
        out_specs=[vm] + [hbm] * 6,
        out_shape=[shape(small.shape, F32), shape((length, model), BF), shape((length, model), BF),
                   shape((model, total), BF), shape((model, width), BF),
                   shape((length, total), F32), shape((length, width), F32)],
        scratch_shapes=[pltpu.VMEM((length, model), BF), pltpu.VMEM((length, model), BF),
                        pltpu.VMEM((model, total), BF), pltpu.VMEM((model, width), BF),
                        pltpu.VMEM(resid.shape, F32), pltpu.VMEM(resid.shape, F32),
                        pltpu.VMEM((2, tile, total), F32), pltpu.VMEM((2, tile, width), F32),
                        pltpu.VMEM((4,) + small.shape, F32), pltpu.VMEM((dp - 1,) + small.shape, F32),
                        pltpu.VMEM((4, dp) + wbc.shape, BF), pltpu.VMEM((dp,) + wdt.shape, BF),
                        dma((2, 3)), dma((2, dp - 1)), dma((2, 3)), dma((2, dp - 1)), dma((2, dp - 1)),
                        dma((2, 3, PARTS)), dma((2, 3, PARTS)), dma((4, outer_n, wparts)), dma((4, outer_n, wparts)),
                        dma((8,)), dma((2,)), dma((2,))],
        compiler_params=pltpu.CompilerParams(collective_id=0, has_side_effects=True, vmem_limit_bytes=62 * 2**20),
        cost_estimate=pl.CostEstimate(flops=17 * 10**9, bytes_accessed=60 * 2**20, transcendentals=0),
        name="gather_all",
    )(small, wzx, wdt, wbc, wout, resid, cot)


def final_kernel(outer_n, both_rows, gain_rows, dz_in, rest_in, weight_in, normed_in, resid_in, small,
                 d_local, owned, small_out, bc_out,
                 dz, rest, weight, normed, resid, g_all, tok, near_buf, far_src, far_buf, in_buf, out_src, out_buf,
                 small_d, small_t, gain_d, gain_t, gain_acc, bc_src, bc_buf,
                 load_sem, near_sem, far_sem, in_sem, out_sem, small_sem_d, small_sem_t, gain_sem_d, gain_sem_t, bc_sem):
    z, y, x, c = _place()
    me = _peer(z, y, x, c)
    t = x * 2 + c
    own_rows, model = d_local.shape
    block, cols = owned.shape
    width = dz.shape[1]
    wparts = _parts(block)
    bsize = block // wparts
    size = own_rows // PARTS
    half = own_rows // 2
    per_group = next(g for g in range(1, outer_n + 1) if (2 * g * block) % LANES == 0)
    groups = outer_n // per_group
    loads = [pltpu.make_async_copy(src, dst, load_sem.at[i]) for i, (src, dst) in enumerate(
        [(dz_in, dz), (rest_in, rest), (weight_in, weight), (normed_in, normed), (resid_in, resid)])]
    for copy in loads:
        copy.start()
    _greet(outer_n)
    dp_peers = [(k, j) for k in range(outer_n) for j in (0, 1) if k or j]
    tensor_peers = [(k, j) for k in (0, 1) for j in (0, 1) if k or j]

    def dp_copies(src, dst, sem):
        return [_remote(src, dst.at[k * 2 + j], sem.at[0, i], sem.at[1, i],
                        _peer((z + k) % outer_n, (y + j) % 2, x, c)) for i, (k, j) in enumerate(dp_peers)]

    def tensor_copies(src, dst, sem):
        return [_remote(src, dst.at[k * 2 + j], sem.at[0, i], sem.at[1, i],
                        _peer(z, y, (x + k) % 2, (c + j) % 2)) for i, (k, j) in enumerate(tensor_peers)]

    def dp_total(buf):
        total = None
        for zz in range(outer_n):
            for yy in (0, 1):
                term = buf[lax.rem(z - zz + outer_n, outer_n) * 2 + lax.rem(y - yy + 2, 2)]
                total = term if total is None else total + term
        return total

    def near_copy(i, part):
        at = pl.ds(part * size, size)
        return _remote(tok.at[2 * i, at, :], near_buf.at[i, at, :], near_sem.at[0, i, part], near_sem.at[1, i, part],
                       _peer(z, y, x, 1 - c))

    def far_copy(part):
        at = pl.ds(part * size, size)
        return _remote(far_src.at[at, :], far_buf.at[at, :], far_sem.at[0, part], far_sem.at[1, part],
                       _peer(z, y, 1 - x, c))

    def in_copy(k, zz, part):
        at = pl.ds(part * bsize, bsize)
        return _remote(g_all.at[zz, 1 - y, at, :], in_buf.at[k, at, :], in_sem.at[0, k, part], in_sem.at[1, k, part],
                       _peer(z, 1 - y, x, c))

    def out_copy(k, part):
        at = pl.ds(part * bsize, bsize)
        return _remote(out_src.at[k - 1, at, :], out_buf.at[k - 1, at, :], out_sem.at[0, k - 1, part],
                       out_sem.at[1, k - 1, part], _peer((z + k) % outer_n, y, x, c))

    def token_product(i, part):
        far, near = ((1 - x, 1 - c), (1 - x, c), (x, 1 - c), (x, c))[i]
        rows = pl.ds(pl.multiple_of((far * 2 + near) * own_rows + part * half, LANES), half)
        value = _dot_last(dz[rows, :], weight[:, :width]) + _dot_last(rest[rows, :], weight[:, width:])
        at = pl.ds(pl.multiple_of(part * half, LANES), half)
        if i < 3:
            tok[i, at, :] = value.astype(BF)
        else:
            d_local[at, :] = value

    def group(i):
        grp = lax.rem(z // per_group + 1 + i, groups)
        at = pl.ds(pl.multiple_of(grp * (2 * per_group * block), LANES), 2 * per_group * block)
        value = lax.dot_general(normed[:, at], rest[...], (((0,), (0,)), ((), ())), preferred_element_type=F32)
        for j in range(per_group):
            zz = grp * per_group + j
            for yy in (0, 1):
                first = (2 * j + yy) * block
                g_all[zz, yy] = value[first : first + block, :].astype(BF)
            k = lax.rem(zz - z + outer_n, outer_n)
            for part in range(wparts):
                in_copy(k, zz, part).start()

    def token_step(part):
        at = pl.ds(part * size, size)
        near_copy(0, part).wait_recv()
        far_src[at, :] = (tok[1, at, :].astype(F32) + near_buf[0, at, :].astype(F32)).astype(BF)
        far_copy(part).start()

    def grad_step(k, part):
        at = pl.ds(part * bsize, bsize)
        zz = lax.rem(z + k, outer_n)
        in_copy(k, zz, part).wait_recv()
        both = g_all[zz, y, at, :].astype(F32) + in_buf[k, at, :].astype(F32)
        if k:
            out_src[k - 1, at, :] = both.astype(BF)
            out_copy(k, part).start()
        else:
            owned[at, :] = both

    small_d[0] = small[...]
    first = dp_copies(small, small_d, small_sem_d)
    for copy in first:
        copy.start()
    for copy in loads[:3]:
        copy.wait()
    parts_half = PARTS // 2

    @pl.loop(0, 2)
    def _(part):
        token_product(0, part)

    for part in range(PARTS):
        near_copy(0, part).start()
    loads[3].wait()
    group(0)

    @pl.loop(0, 2)
    def _(part):
        token_product(1, part)

    for part in range(PARTS):
        token_step(part)

    @pl.loop(1, groups)
    def _(i):
        group(i)

    order = list(range(1, outer_n)) + [0]
    todo = [(k, part) for k in order for part in range(wparts)]
    quarter = -(-len(todo) // 4)
    for k, part in todo[:quarter]:
        grad_step(k, part)

    @pl.loop(0, 2)
    def _(part):
        token_product(2, part)

    for part in range(PARTS):
        near_copy(1, part).start()
    for copy in first:
        copy.wait_recv()
    total = dp_total(small_d)
    small_out[...] = total
    small_t[0] = total[:both_rows, :]
    second = tensor_copies(small_t.at[0], small_t, small_sem_t)
    for copy in second:
        copy.start()
    for k, part in todo[quarter : 2 * quarter]:
        grad_step(k, part)

    @pl.loop(0, 2)
    def _(part):
        token_product(3, part)

    for k, part in todo[2 * quarter : 3 * quarter]:
        grad_step(k, part)
    loads[4].wait()
    gain_acc[...] = jnp.zeros_like(gain_acc)
    for part in range(PARTS):
        at = pl.ds(part * size, size)
        near_copy(1, part).wait_recv()
        far_copy(part).wait_recv()
        got = d_local[at, :] + near_buf[1, at, :].astype(F32) + far_buf[at, :].astype(F32)
        d_local[at, :] = got
        values = resid[at, :]
        inv = lax.rsqrt(jnp.mean(values * values, axis=-1, keepdims=True) + EPSILON)
        gain_acc[...] += _rows_sum(got * values * inv)
    for j in range(gain_rows):
        gain_d[0, j : j + 1, :] = jnp.sum(gain_acc[:, j * LANES : (j + 1) * LANES], axis=0, keepdims=True)
    gain_first = dp_copies(gain_d.at[0], gain_d, gain_sem_d)
    for copy in gain_first:
        copy.start()
    for k, part in todo[3 * quarter :]:
        grad_step(k, part)
    for part in range(wparts):
        at = pl.ds(part * bsize, bsize)
        total = owned[at, :]
        for k in order[:-1]:
            out_copy(k, part).wait_recv()
            total = total + out_buf[k - 1, at, :].astype(F32)
        owned[at, :] = total
    bc_rows = block // 4
    for i in range(4):
        bc_src[i] = owned[i * bc_rows : (i + 1) * bc_rows, width : width + 2 * LANES]
    bc_copies = []
    for i, (k, j) in enumerate(tensor_peers):
        other = lax.rem(x + k, 2) * 2 + lax.rem(c + j, 2)
        bc_copies.append(_remote(bc_src.at[other], bc_buf.at[i], bc_sem.at[0, i], bc_sem.at[1, i],
                                 _peer(z, y, (x + k) % 2, (c + j) % 2)))
    for copy in bc_copies:
        copy.start()
    for copy in gain_first:
        copy.wait_recv()
    total = dp_total(gain_d)
    gain_t[0] = total
    gain_second = tensor_copies(gain_t.at[0], gain_t, gain_sem_t)
    for copy in gain_second:
        copy.start()
    for copy in second:
        copy.wait_recv()
    small_out[0:both_rows, :] = (small_t[0] + small_t[1]) + (small_t[2] + small_t[3])
    for copy in bc_copies:
        copy.wait_recv()
    bc_out[...] = (bc_src[t] + bc_buf[0]) + (bc_buf[1] + bc_buf[2])
    for copy in gain_second:
        copy.wait_recv()
    gains = (gain_t[0] + gain_t[1]) + (gain_t[2] + gain_t[3])
    small_out[0:gain_rows, :] = gains[:gain_rows, :]
    for part in range(PARTS):
        near_copy(0, part).wait_send()
        near_copy(1, part).wait_send()
        far_copy(part).wait_send()
    for k in range(outer_n):
        zz = lax.rem(z + k, outer_n)
        for part in range(wparts):
            in_copy(k, zz, part).wait_send()
            if k:
                out_copy(k, part).wait_send()
    for copy in first + second + gain_first + gain_second + bc_copies:
        copy.wait_send()


def final_sums(dz, rest, weight, normed, resid, small, both_rows):
    dp, tp = lax.axis_size("dp"), lax.axis_size("tensor")
    outer_n = dp // 2
    own_rows, model = resid.shape
    block, cols = model // dp, rest.shape[1]
    gain_rows = model // LANES
    gain_pad = -(-gain_rows // 8) * 8
    wparts = _parts(block)
    vm = pl.BlockSpec(memory_space=pltpu.VMEM)
    hbm = pl.BlockSpec(memory_space=pl.ANY)
    dma = pltpu.SemaphoreType.DMA
    tokens = (own_rows, model)
    bc = (4, block // 4, 2 * LANES)
    return pl.pallas_call(
        functools.partial(final_kernel, outer_n, both_rows, gain_rows),
        in_specs=[hbm] * 5 + [vm],
        out_specs=[vm] * 4,
        out_shape=[jax.ShapeDtypeStruct(tokens, F32),
                   jax.ShapeDtypeStruct((block, cols), F32),
                   jax.ShapeDtypeStruct(small.shape, F32),
                   jax.ShapeDtypeStruct(bc[1:], F32)],
        scratch_shapes=[pltpu.VMEM(dz.shape, BF), pltpu.VMEM(rest.shape, BF), pltpu.VMEM(weight.shape, BF),
                        pltpu.VMEM(normed.shape, BF), pltpu.VMEM(tokens, F32),
                        pltpu.VMEM((outer_n, 2, block, cols), BF),
                        pltpu.VMEM((3,) + tokens, BF), pltpu.VMEM((2,) + tokens, BF),
                        pltpu.VMEM(tokens, BF), pltpu.VMEM(tokens, BF),
                        pltpu.VMEM((outer_n, block, cols), BF),
                        pltpu.VMEM((outer_n - 1, block, cols), BF), pltpu.VMEM((outer_n - 1, block, cols), BF),
                        pltpu.VMEM((dp,) + small.shape, F32), pltpu.VMEM((4, both_rows, LANES), F32),
                        pltpu.VMEM((dp, gain_pad, LANES), F32), pltpu.VMEM((4, gain_pad, LANES), F32),
                        pltpu.VMEM((8, model), F32), pltpu.VMEM(bc, F32), pltpu.VMEM((3,) + bc[1:], F32),
                        dma((5,)), dma((2, 2, PARTS)), dma((2, PARTS)), dma((2, outer_n, wparts)),
                        dma((2, outer_n - 1, wparts)), dma((2, dp - 1)), dma((2, 3)), dma((2, dp - 1)), dma((2, 3)),
                        dma((2, 3))],
        compiler_params=pltpu.CompilerParams(collective_id=1, has_side_effects=True, vmem_limit_bytes=63 * 2**20),
        cost_estimate=pl.CostEstimate(flops=20 * 10**9, bytes_accessed=40 * 2**20, transcendentals=0),
        name="final_sums",
    )(dz, rest, weight, normed, resid, small)


def _spread(values, index, count):
    size = values.shape[-1]
    full = jnp.zeros(values.shape[:-1] + (size * count,), F32)
    return lax.dynamic_update_slice_in_dim(full, values, index * size, axis=values.ndim - 1)


def _own(values, index, count):
    size = values.shape[-1] // count
    return lax.dynamic_slice_in_dim(values, index * size, size, axis=values.ndim - 1)


def on_device(
    resid_in, norm_gain, proj_zx, proj_dt, proj_bc, conv_x_weight, conv_x_bias, conv_bc_weight,
    conv_bc_bias, dt_bias, a_log, skip_gain, gate_gain, proj_out, cotangent,
):
    dp, tp = lax.axis_size("dp"), lax.axis_size("tensor")
    index = lax.axis_index("dp") * tp + lax.axis_index("tensor")
    count = dp * tp
    model = resid_in.shape[-1]
    width = conv_x_weight.shape[1]
    heads = dt_bias.shape[0]
    inner_channels = width * tp
    states2 = 2 * LANES
    rows = proj_zx.shape[0]
    resid, cot = resid_in[0], cotangent[0]
    small = jnp.concatenate([
        _spread(norm_gain, index, count).reshape(-1, LANES),
        _spread(conv_bc_weight, index, count).reshape(-1, LANES),
        _spread(conv_bc_bias, index, count).reshape(-1, LANES)], axis=0)
    gain_rows = model // LANES
    both_rows = -(-small.shape[0] // 8) * 8
    small = pad_rows(small, both_rows)
    small_all, normed, cot_full, weight, out_t, proj, d_gated = gather_all(
        small, resid, cot, proj_zx.reshape(rows, 2 * width), proj_dt, proj_bc, proj_out.T)
    full_cbw = small_all[gain_rows : gain_rows + 4 * states2 // LANES].reshape(4, states2)
    full_cbb = small_all[gain_rows + 4 * states2 // LANES : gain_rows + 5 * states2 // LANES].reshape(states2)
    full_gain = small_all[:gain_rows].reshape(model)
    packs = pack_params(conv_x_weight, conv_x_bias, full_cbw, full_cbb, dt_bias, a_log, skip_gain, gate_gain)
    y, states, partial = ssd_forward(proj, d_gated, *packs)
    dy, dz, out_partial, grads_zo, ggain = middle(proj, y, d_gated, partial, packs[3], normed, cot_full, out_t, inner_channels)
    d_rest, gx, gbc, gh, block_sum, owned_zo = ssd_backward(proj, y, dy, states, *packs, out_partial, grads_zo)
    block_out = resid + block_sum
    gx = jnp.concatenate([gx.sum(1), ggain.sum(0)[None]], 0)
    gbc, gh = gbc.sum(1), gh.sum(1)
    to_sum = jnp.concatenate([
        pad_rows(jnp.concatenate([jnp.zeros((gain_rows, LANES), F32), gbc.reshape(-1, LANES)], 0), both_rows),
        gx.reshape(-1, LANES), gh], axis=0)
    to_sum = pad_rows(to_sum, -(-to_sum.shape[0] // 8) * 8)
    d_local, owned, totals, grad_bc = final_sums(dz, d_rest, weight, normed, resid, to_sum, both_rows)
    inv_in = lax.rsqrt(jnp.mean(resid * resid, axis=-1, keepdims=True) + EPSILON)
    scaled = resid * inv_in
    d_scaled = d_local * full_gain
    grad_resid = inv_in * (d_scaled - scaled * jnp.mean(d_scaled * scaled, axis=-1, keepdims=True)) + cot
    grad_zx = jnp.stack([owned_zo[:, :width], owned[:, :width]], axis=1)
    grad_dt = owned[:, width + states2 : width + states2 + heads]
    owned_out = owned_zo[:, width:].T
    owned_gain = _own(totals[:gain_rows].reshape(model), index, count)
    at = gain_rows + 4 * states2 // LANES
    owned_cbw = _own(totals[gain_rows:at].reshape(4, states2), index, count)
    owned_cbb = _own(totals[at : at + states2 // LANES].reshape(states2), index, count)
    gx_all = totals[both_rows : both_rows + 7 * width // LANES].reshape(7, width)
    gh_all = totals[both_rows + 7 * width // LANES :]
    skip = gx_all[5].reshape(heads, -1).sum(1)
    return (
        block_out[None], grad_resid[None], owned_gain, grad_zx, grad_dt, grad_bc, gx_all[:4], gx_all[4],
        owned_cbw, owned_cbb, gh_all[0, :heads], gh_all[1, :heads], skip, gx_all[6], owned_out,
    )


def solution(mesh):
    specs = (
        P("dp", "tensor", None), P(("dp", "tensor")), P("dp", None, "tensor"), P("dp", "tensor"),
        P(("dp", "tensor"), None), P(None, "tensor"), P("tensor"), P(None, ("dp", "tensor")),
        P(("dp", "tensor")), P("tensor"), P("tensor"), P("tensor"), P("tensor"), P("tensor", "dp"),
        P("dp", "tensor", None),
    )
    outs = (specs[0], specs[0]) + specs[1:14]
    return jax.shard_map(on_device, mesh=mesh, in_specs=specs, out_specs=outs, check_vma=False)
```

```python
import functools, math
import jax, jax.numpy as jnp
from jax import lax
from jax.experimental import pallas as pl
from jax.experimental.pallas import tpu as pltpu
from jax.sharding import PartitionSpec as P

EPSILON = 1e-05
CHUNK = 128
LANES = 128
TAPS = 4
LOG2E = 1.4426950408889634
BF = jnp.bfloat16
F32 = jnp.float32


MESH = pl.DeviceIdType.MESH
PARTS = 4
ROW_PARTS = 6


def _place():
    d, t = lax.axis_index("dp"), lax.axis_index("tensor")
    return d // 2, d % 2, t // 2, t % 2


def _peer(outer, inner, far, near):
    return (outer * 2 + inner, far * 2 + near)


def _greet(outer_n):
    z, y, x, c = _place()
    barrier = pltpu.get_barrier_semaphore()
    peers = []
    for k in range(outer_n):
        for j in (0, 1):
            if k or j:
                peers.append(_peer((z + k) % outer_n, (y + j) % 2, x, c))
    for k in (0, 1):
        for j in (0, 1):
            if k or j:
                peers.append(_peer(z, y, (x + k) % 2, (c + j) % 2))
    for peer in peers:
        pl.semaphore_signal(barrier, inc=1, device_id=peer, device_id_type=MESH)
    pl.semaphore_wait(barrier, len(peers))


def _parts(rows):
    return max(p for p in range(1, ROW_PARTS + 1) if rows % (16 * p) == 0)


def _remote(src, dst, send, recv, peer):
    return pltpu.make_async_remote_copy(
        src_ref=src, dst_ref=dst, send_sem=send, recv_sem=recv, device_id=peer, device_id_type=MESH)


def _rows(start, size):
    return pl.ds(pl.multiple_of(start, 16), size)


class _Reduction:
    def __init__(self, outer_n, partial, grads, resid, block_sum, owned, resid_buf, own_tokens, near_buf, far_src, far_buf,
                 own_grads, in_buf, out_src, out_buf, near_sem, far_sem, in_sem, out_sem, local_sem):
        self.__dict__.update(locals())
        self.z, self.y, self.x, self.c = _place()
        self.me = _peer(self.z, self.y, self.x, self.c)
        self.own_rows = block_sum.shape[0]
        self.block = owned.shape[0]
        self.wparts = _parts(self.block)
        self.size = self.own_rows // PARTS
        self.bsize = self.block // self.wparts
        order = list(range(1, outer_n))
        order.sort(key=lambda k: -min(k, outer_n - k))
        self.order = order + [0]

    def token_rows(self, far, near, part):
        return _rows((far * 2 + near) * self.own_rows + part * self.size, self.size)

    def grad_rows(self, outer, inner, part):
        return _rows((outer * 2 + inner) * self.block + part * self.bsize, self.bsize)

    def near_copy(self, i, part):
        far = (1 - self.x, self.x)[i]
        at = pl.ds(part * self.size, self.size)
        return _remote(self.partial.at[self.token_rows(far, 1 - self.c, part), :], self.near_buf.at[i, at, :],
                       self.near_sem.at[0, i, part], self.near_sem.at[1, i, part],
                       _peer(self.z, self.y, self.x, 1 - self.c))

    def far_copy(self, part):
        at = pl.ds(part * self.size, self.size)
        return _remote(self.far_src.at[at, :], self.far_buf.at[at, :], self.far_sem.at[0, part],
                       self.far_sem.at[1, part], _peer(self.z, self.y, 1 - self.x, self.c))

    def in_copy(self, k, part):
        at = pl.ds(part * self.bsize, self.bsize)
        rows = self.grad_rows((self.z + k) % self.outer_n, 1 - self.y, part)
        return _remote(self.grads.at[rows, :], self.in_buf.at[k, at, :], self.in_sem.at[0, k, part],
                       self.in_sem.at[1, k, part], _peer(self.z, 1 - self.y, self.x, self.c))

    def out_copy(self, k, part):
        at = pl.ds(part * self.bsize, self.bsize)
        return _remote(self.out_src.at[k - 1, at, :], self.out_buf.at[k - 1, at, :], self.out_sem.at[0, k - 1, part],
                       self.out_sem.at[1, k - 1, part], _peer((self.z + k) % self.outer_n, self.y, self.x, self.c))

    def local_copies(self):
        copies = [pltpu.make_async_copy(self.resid, self.resid_buf, self.local_sem.at[2 + self.outer_n])]
        for i, far in enumerate((1 - self.x, self.x)):
            rows = _rows((far * 2 + self.c) * self.own_rows, self.own_rows)
            copies.append(pltpu.make_async_copy(self.partial.at[rows, :], self.own_tokens.at[i], self.local_sem.at[i]))
        for k in range(self.outer_n):
            rows = _rows((((self.z + k) % self.outer_n) * 2 + self.y) * self.block, self.block)
            copies.append(pltpu.make_async_copy(self.grads.at[rows, :], self.own_grads.at[k], self.local_sem.at[2 + k]))
        return copies

    def begin(self):
        _greet(self.outer_n)
        for part in range(PARTS):
            self.near_copy(0, part).start()
        for k in self.order:
            for part in range(self.wparts):
                self.in_copy(k, part).start()
        for part in range(PARTS):
            self.near_copy(1, part).start()
        for copy in self.local_copies():
            copy.start()

    def ready(self):
        for copy in self.local_copies():
            copy.wait()

    def token_step(self, part):
        at = pl.ds(part * self.size, self.size)
        self.near_copy(0, part).wait_recv()
        self.far_src[at, :] = (self.own_tokens[0, at, :].astype(F32) + self.near_buf[0, at, :].astype(F32)).astype(BF)
        self.far_copy(part).start()

    def grad_step(self, k, part):
        at = pl.ds(part * self.bsize, self.bsize)
        self.in_copy(k, part).wait_recv()
        both = self.own_grads[k, at, :].astype(F32) + self.in_buf[k, at, :].astype(F32)
        if k:
            self.out_src[k - 1, at, :] = both.astype(BF)
            self.out_copy(k, part).start()
        else:
            self.owned[at, :] = both

    def grad_steps(self):
        return [(k, part) for k in self.order for part in range(self.wparts)]

    def plan(self, steps):
        pieces = [(1, self.ready)]
        for part in range(PARTS):
            pieces.append((min(1 + part, steps - 1), functools.partial(self.token_step, part)))
        todo = self.grad_steps()
        self.late = len(todo) // 8
        for i, (k, part) in enumerate(todo[: len(todo) - self.late]):
            pieces.append((min(1 + (i + 2) * (steps - 1) // len(todo), steps - 1),
                           functools.partial(self.grad_step, k, part)))
        return pieces

    def end(self):
        for k, part in self.grad_steps()[-self.late :]:
            self.grad_step(k, part)
        for part in range(PARTS):
            at = pl.ds(part * self.size, self.size)
            self.near_copy(1, part).wait_recv()
            self.far_copy(part).wait_recv()
            self.block_sum[at, :] = (self.own_tokens[1, at, :].astype(F32) + self.near_buf[1, at, :].astype(F32)
                                     + self.far_buf[at, :].astype(F32)) + self.resid_buf[at, :]
        for part in range(self.wparts):
            at = pl.ds(part * self.bsize, self.bsize)
            total = self.owned[at, :]
            for k in self.order[:-1]:
                self.out_copy(k, part).wait_recv()
                total = total + self.out_buf[k - 1, at, :].astype(F32)
            self.owned[at, :] = total
        for part in range(PARTS):
            self.near_copy(0, part).wait_send()
            self.near_copy(1, part).wait_send()
            self.far_copy(part).wait_send()
        for part in range(self.wparts):
            for k in self.order:
                self.in_copy(k, part).wait_send()
                if k:
                    self.out_copy(k, part).wait_send()


def reduction_scratch(outer_n, tokens, grads):
    dma = pltpu.SemaphoreType.DMA
    parts = _parts(grads[0])
    return [pltpu.VMEM(tokens, F32), pltpu.VMEM((2,) + tokens, BF), pltpu.VMEM((2,) + tokens, BF), pltpu.VMEM(tokens, BF),
            pltpu.VMEM(tokens, BF), pltpu.VMEM((outer_n,) + grads, BF), pltpu.VMEM((outer_n,) + grads, BF),
            pltpu.VMEM((outer_n - 1,) + grads, BF), pltpu.VMEM((outer_n - 1,) + grads, BF),
            dma((2, 2, PARTS)), dma((2, PARTS)), dma((2, outer_n, parts)), dma((2, outer_n - 1, parts)),
            dma((3 + outer_n,))]


def _sigmoid(v):
    return 0.5 * jnp.tanh(0.5 * v) + 0.5


def _softplus(t):
    return jnp.maximum(t, 0.0) + jnp.log1p(jnp.exp(-jnp.abs(t)))


def _dot_last(a, b):
    return lax.dot_general(a, b, (((1,), (1,)), ((), ())), preferred_element_type=F32)


def _dot_exact(a, b):
    return jnp.dot(a, b, precision=lax.Precision.HIGHEST, preferred_element_type=F32)


def _halves(v):
    high = v.astype(BF)
    return high, (v - high.astype(F32)).astype(BF)


def _dot_three(a, b):
    a_high, a_low = _halves(a)
    b_high, b_low = _halves(b)
    return _dot_last(jnp.concatenate([a_high, a_low, a_high], axis=1),
                     jnp.concatenate([b_high, b_high, b_low], axis=1))


def _rows_sum(v):
    return v.reshape(v.shape[0] // 8, 8, v.shape[1]).sum(axis=0)


def _split(lo, v):
    zero = jnp.zeros_like(v)
    return [jnp.where(lo, v, zero), jnp.where(lo, zero, v)]


def _times(dt_raw, head, rows, cols):
    t = dt_raw + head[0:1, :]
    delta = _softplus(t)
    rate = -jnp.exp(head[1:2, :])
    tri = (rows >= cols).astype(F32)
    cum = _dot_exact(tri, delta * (rate * LOG2E))
    return t, delta, rate, cum


def _conv(buf, start, cols, w, length):
    ahead = buf[start : start + 8 + length, cols]
    shifted = [pltpu.roll(ahead, TAPS - 1 - k, 0)[8:] for k in range(TAPS - 1)] + [ahead[8:]]
    v = w[TAPS : TAPS + 1, :] + w[0:1, :] * shifted[0]
    for k in range(1, TAPS):
        v = v + w[k : k + 1, :] * shifted[k]
    return v, shifted


def _conv_back(dv, after, w):
    behind = jnp.concatenate([dv, after], axis=0)
    length = dv.shape[0]
    total = w[TAPS - 1 : TAPS, :] * dv
    for k in range(TAPS - 1):
        total = total + w[k : k + 1, :] * pltpu.roll(behind, length + 8 - (TAPS - 1 - k), 0)[:length]
    return total


def _fill_spread(spread, head_width):
    shape = spread.shape
    head = lax.broadcasted_iota(jnp.int32, shape, 0) % LANES
    lane = lax.broadcasted_iota(jnp.int32, shape, 1)
    spread[...] = (lane // head_width == head).astype(F32).astype(BF)


def _widen(wide, delta, tail, grow, spread):
    high, low = _halves(jnp.concatenate([delta, tail, grow], axis=0))
    wide[...] = jnp.dot(jnp.concatenate([high, low], axis=1), spread[...], preferred_element_type=F32)


def forward_kernel(width, p_ref, dg_ref, convx_ref, convbc_ref, head_ref, lane_ref,
                   y_ref, h_ref, s_ref, state, xbuf, bcbuf, spread, wide, sums, sum_sem):
    tokens = p_ref.shape[0]
    pairs = width // LANES
    step = pl.program_id(0)
    z, y_at, x, c = _place()
    me = x * 2 + c
    half = sums.shape[1] // 2
    tensor_peers = [_peer(z, y_at, (x + k) % 2, (c + j) % 2) for k in (0, 1) for j in (0, 1) if k or j]

    @pl.when(step == 0)
    def _():
        barrier = pltpu.get_barrier_semaphore()
        for peer in tensor_peers:
            pl.semaphore_signal(barrier, inc=1, device_id=peer, device_id_type=MESH)
        pl.semaphore_wait(barrier, len(tensor_peers))
        state[...] = jnp.zeros_like(state)
        _fill_spread(spread, LANES // 2)
        xbuf[0:8, :] = jnp.zeros((8, width), F32)
        bcbuf[0:8, :] = jnp.zeros((8, 2 * LANES), F32)

    @pl.when(step > 0)
    def _():
        xbuf[0:8, :] = xbuf[tokens : tokens + 8, :]
        bcbuf[0:8, :] = bcbuf[tokens : tokens + 8, :]

    xbuf[8 : 8 + tokens, :] = p_ref[:, width : 2 * width]
    bcbuf[8 : 8 + tokens, :] = p_ref[:, 2 * width : 2 * width + 2 * LANES]
    rows = lax.broadcasted_iota(jnp.int32, (CHUNK, CHUNK), 0)
    cols = lax.broadcasted_iota(jnp.int32, (CHUNK, CHUNK), 1)
    lo = cols < LANES // 2
    head = head_ref[...]
    ones = jnp.ones((8, LANES), F32)
    for sub in range(tokens // CHUNK):
        base = sub * CHUNK
        span = slice(base, base + CHUNK)
        vbc, _ = _conv(bcbuf, base, slice(0, 2 * LANES), convbc_ref[...], CHUNK)
        bc = vbc * _sigmoid(vbc)
        b_in, c_out = bc[:, :LANES], bc[:, LANES:]
        c_high, c_low = _halves(c_out)
        c_wide = jnp.concatenate([c_high, c_low, c_high], axis=1)
        _, delta, _, cum = _times(p_ref[span, 2 * width + 2 * LANES :], head, rows, cols)
        cum_t = cum.T
        scores = jnp.where(rows >= cols, _dot_three(c_out, b_in), 0.0)
        last = cum[CHUNK - 1 : CHUNK, :]
        tail = jnp.exp2(last - cum)
        grow = jnp.exp2(cum)
        _widen(wide, delta, tail, grow, spread)
        b_t = b_in.T.astype(BF)
        squares = jnp.zeros((CHUNK, LANES), F32)
        inner = jnp.zeros((CHUNK, LANES), F32)
        h_ref[sub] = state[...]
        for q in range(pairs):
            lanes = slice(q * LANES, (q + 1) * LANES)
            v, _ = _conv(xbuf, base, lanes, convx_ref[:, lanes], CHUNK)
            x_act = v * _sigmoid(v)
            u = x_act * wide[0:CHUNK, lanes]
            left = []
            for h in (2 * q, 2 * q + 1):
                e = jnp.exp2(jnp.minimum(cum[:, h : h + 1] - cum_t[h : h + 1, :], 0.0))
                left.append((e * scores).astype(BF))
            held = state[:, lanes]
            held_high, held_low = _halves(held)
            y = jnp.dot(jnp.concatenate(left, axis=1), jnp.concatenate(_split(lo, u.astype(BF)), axis=0),
                        preferred_element_type=F32)
            outer = jnp.dot(c_wide, jnp.concatenate([held_high, held_high, held_low], axis=0),
                            preferred_element_type=F32)
            y = y + outer * wide[2 * CHUNK :, lanes] + lane_ref[0:1, lanes] * x_act
            y_ref[span, lanes] = y
            uw = (u * wide[CHUNK : 2 * CHUNK, lanes]).astype(BF)
            factor = wide[3 * CHUNK - 1 : 3 * CHUNK, lanes]
            state[:, lanes] = held * factor + jnp.dot(b_t, uw, preferred_element_type=F32)
            z = p_ref[span, lanes]
            product = y * (z * _sigmoid(z))
            squares = squares + product * product
            inner = inner + dg_ref[span, lanes].astype(F32) * lane_ref[1:2, lanes] * product
        row_sq = lax.dot_general(ones, squares, (((1,), (1,)), ((), ())),
                                 precision=lax.Precision.HIGHEST, preferred_element_type=F32)
        row_in = lax.dot_general(ones, inner, (((1,), (1,)), ((), ())),
                                 precision=lax.Precision.HIGHEST, preferred_element_type=F32)
        at = step * (tokens // CHUNK) + sub
        sums[me, pl.ds(at, 1), :] = row_sq[0:1, :]
        sums[me, pl.ds(half + at, 1), :] = row_in[0:1, :]

    @pl.when(step == pl.num_programs(0) - 1)
    def _():
        copies = [_remote(sums.at[me], sums.at[me], sum_sem.at[0, i], sum_sem.at[1, i], peer)
                  for i, peer in enumerate(tensor_peers)]
        for copy in copies:
            copy.start()
        for copy in copies:
            copy.wait_recv()
        s_ref[...] = (sums[0] + sums[1]) + (sums[2] + sums[3])
        for copy in copies:
            copy.wait_send()


def backward_kernel(width, outer_n, p_ref, prev_ref, y_ref, dy_ref, h_ref,
                    convx_ref, convbc_ref, head_ref, lane_ref, partial, grads, resid,
                    dp_ref, gx_ref, gbc_ref, gh_ref, block_sum, owned,
                    grad_state, carry_hg, xbuf, bcbuf, after_x, after_bc, spread, wide, *comm):
    tokens = p_ref.shape[0]
    pairs = width // LANES
    step = pl.program_id(0)
    is_first_block = step == pl.num_programs(0) - 1
    length = partial.shape[0]
    reduction = _Reduction(outer_n, partial, grads, resid, block_sum, owned, *comm)

    @pl.when(step == 0)
    def _():
        reduction.begin()

    for at, piece in reduction.plan(length // tokens):
        @pl.when(step == at)
        def _(piece=piece):
            piece()

    @pl.when(step == 0)
    def _():
        grad_state[...] = jnp.zeros_like(grad_state)
        carry_hg[...] = jnp.zeros_like(carry_hg)
        after_x[...] = jnp.zeros_like(after_x)
        after_bc[...] = jnp.zeros_like(after_bc)
        _fill_spread(spread, LANES // 2)
        gx_ref[...] = jnp.zeros_like(gx_ref)
        gbc_ref[...] = jnp.zeros_like(gbc_ref)
        gh_ref[...] = jnp.zeros_like(gh_ref)

    keep = jnp.where(is_first_block, 0.0, 1.0)
    xbuf[0:8, :] = prev_ref[:, width : 2 * width] * keep
    bcbuf[0:8, :] = prev_ref[:, 2 * width : 2 * width + 2 * LANES] * keep
    xbuf[8 : 8 + tokens, :] = p_ref[:, width : 2 * width]
    bcbuf[8 : 8 + tokens, :] = p_ref[:, 2 * width : 2 * width + 2 * LANES]
    rows = lax.broadcasted_iota(jnp.int32, (CHUNK, CHUNK), 0)
    cols = lax.broadcasted_iota(jnp.int32, (CHUNK, CHUNK), 1)
    lo = cols < LANES // 2
    head = head_ref[...]
    for sub in reversed(range(tokens // CHUNK)):
        base = sub * CHUNK
        span = slice(base, base + CHUNK)
        vbc, shifted_bc = _conv(bcbuf, base, slice(0, 2 * LANES), convbc_ref[...], CHUNK)
        sbc = _sigmoid(vbc)
        bc = vbc * sbc
        b_in, c_out = bc[:, :LANES], bc[:, LANES:]
        b_half, c_half = b_in.astype(BF), c_out.astype(BF)
        t, delta, rate, cum = _times(p_ref[span, 2 * width + 2 * LANES :], head, rows, cols)
        cum_t = cum.T
        causal_t = cols >= rows
        scores_t = jnp.where(causal_t, _dot_three(b_in, c_out), 0.0)
        last = cum[CHUNK - 1 : CHUNK, :]
        tail = jnp.exp2(last - cum)
        grow = jnp.exp2(cum)
        _widen(wide, delta, tail, grow, spread)
        c_t = c_out.T.astype(BF)
        d_scores = jnp.zeros((CHUNK, CHUNK), F32)
        d_b = jnp.zeros((CHUNK, LANES), F32)
        d_c = jnp.zeros((CHUNK, LANES), F32)
        per_head = jnp.zeros((CHUNK, LANES), F32)
        hg_heads = jnp.zeros((8, LANES), F32)
        for q in range(pairs):
            lanes = slice(q * LANES, (q + 1) * LANES)
            step_wide = wide[0:CHUNK, lanes]
            skip = lane_ref[0:1, lanes]
            v, shifted = _conv(xbuf, base, lanes, convx_ref[:, lanes], CHUNK)
            sv = _sigmoid(v)
            x_act = v * sv
            u = x_act * step_wide
            u_half = u.astype(BF)
            y = y_ref[span, lanes]
            dy_half = dy_ref[span, lanes]
            dy = dy_half.astype(F32)
            dy_block = jnp.concatenate(_split(lo, dy_half), axis=0)
            d_m = _dot_last(u_half, dy_block)
            left, left_b = [], []
            for a in (0, 1):
                h = 2 * q + a
                e = jnp.exp2(jnp.minimum(cum_t[h : h + 1, :] - cum[:, h : h + 1], 0.0))
                left.append((e * scores_t).astype(BF))
                d_scores = d_scores + e * d_m[:, a * CHUNK : (a + 1) * CHUNK]
                left_b.append((b_in * tail[:, h : h + 1]).astype(BF))
            g_held = grad_state[:, lanes]
            g_half, g_low = _halves(g_held)
            h_held = h_ref[sub, :, lanes]
            h_half, h_low = _halves(h_held)
            right = jnp.concatenate([dy_block] + _split(lo, g_half), axis=0)
            du = jnp.dot(jnp.concatenate(left + left_b, axis=1), right, preferred_element_type=F32)
            dx = du * step_wide + skip * dy
            dv = dx * (sv * (1.0 + v * (1.0 - sv)))
            d_in = _conv_back(dv, after_x[:, lanes], convx_ref[:, lanes])
            after_x[:, lanes] = dv[0:8, :]
            dp_ref[span, lanes] = d_in.astype(BF)
            for k in range(TAPS):
                gx_ref[k, :, lanes] += _rows_sum(dv * shifted[k])
            gx_ref[4, :, lanes] += _rows_sum(dv)
            gx_ref[5, :, lanes] += _rows_sum(dy * x_act)
            edy = (dy * wide[2 * CHUNK :, lanes]).astype(BF)
            uw = (u * wide[CHUNK : 2 * CHUNK, lanes]).astype(BF)
            d_c = d_c + _dot_last(jnp.concatenate([edy, edy], axis=1), jnp.concatenate([h_half, h_low], axis=1))
            d_b = d_b + _dot_last(jnp.concatenate([uw, uw], axis=1), jnp.concatenate([g_half, g_low], axis=1))
            g_new = g_held * wide[3 * CHUNK - 1 : 3 * CHUNK, lanes] + jnp.dot(
                c_t, edy, preferred_element_type=F32)
            grad_state[:, lanes] = g_new
            r1 = x_act * du
            r2 = dy * (y - skip * x_act)
            sel1 = (cols == 2 * q + (rows >= LANES // 2).astype(jnp.int32)).astype(BF)
            sel2 = (cols == LANES // 2 + 2 * q + (rows >= LANES // 2).astype(jnp.int32)).astype(BF)
            r1h = r1.astype(BF)
            r1l = (r1 - r1h.astype(F32)).astype(BF)
            r2h = r2.astype(BF)
            r2l = (r2 - r2h.astype(F32)).astype(BF)
            per_head = per_head + jnp.dot(
                jnp.concatenate([r1h, r1l, r2h, r2l], axis=1),
                jnp.concatenate([sel1, sel1, sel2, sel2], axis=0), preferred_element_type=F32)
            hg_heads = hg_heads + _dot_exact(carry_hg[:, lanes], sel1.astype(F32))
            carry_hg[:, lanes] = _rows_sum(g_new * h_held)
        d_scores = jnp.where(causal_t, d_scores, 0.0)
        ds_half = d_scores.astype(BF)
        d_b = d_b + jnp.dot(ds_half, c_half, preferred_element_type=F32)
        d_c = d_c + jnp.dot(d_scores.T.astype(BF), b_half, preferred_element_type=F32)
        dvb = jnp.concatenate([d_b, d_c], axis=1) * (sbc * (1.0 + vbc * (1.0 - sbc)))
        d_bc = _conv_back(dvb, after_bc[...], convbc_ref[...])
        after_bc[...] = dvb[0:8, :]
        dp_ref[span, width : width + 2 * LANES] = d_bc.astype(BF)
        for k in range(TAPS):
            gbc_ref[k] += _rows_sum(dvb * shifted_bc[k])
        gbc_ref[4] += _rows_sum(dvb)
        direct = per_head
        through = pltpu.roll(per_head, LANES // 2, 1)
        d_cum = through - delta * direct
        suffix = _dot_exact((cols >= rows).astype(F32), d_cum)
        d_log = suffix + jnp.sum(hg_heads, axis=0, keepdims=True)
        valid = cols < 2 * pairs
        d_delta = direct + rate * d_log
        d_dt = jnp.where(valid, d_delta * _sigmoid(t), 0.0)
        dp_ref[span, width + 2 * LANES :] = d_dt.astype(BF)
        gh_ref[0] += _rows_sum(d_dt)
        gh_ref[1] += _rows_sum(jnp.where(valid, delta * d_log, 0.0)) * rate

    @pl.when(is_first_block)
    def _():
        reduction.end()


def ssd_forward(proj, dg, convx, convbc, head, lane, tokens=256):
    length, total = proj.shape
    width = convx.shape[1]
    subs = tokens // CHUNK
    whole = lambda a: pl.BlockSpec(a.shape, lambda i: (0,) * a.ndim)
    return pl.pallas_call(
        functools.partial(forward_kernel, width),
        grid=(length // tokens,),
        in_specs=[pl.BlockSpec((tokens, total), lambda i: (i, 0)),
                  pl.BlockSpec((tokens, width), lambda i: (i, 0)),
                  whole(convx), whole(convbc), whole(head), whole(lane)],
        out_specs=[pl.BlockSpec((tokens, width), lambda i: (i, 0)),
                   pl.BlockSpec((subs, LANES, width), lambda i: (i, 0, 0)),
                   pl.BlockSpec((2 * length // CHUNK, CHUNK), lambda i: (0, 0))],
        out_shape=[jax.ShapeDtypeStruct((length, width), F32),
                   jax.ShapeDtypeStruct((length // CHUNK, LANES, width), F32),
                   jax.ShapeDtypeStruct((2 * length // CHUNK, CHUNK), F32)],
        scratch_shapes=[pltpu.VMEM((LANES, width), F32),
                        pltpu.VMEM((tokens + 8, width), F32),
                        pltpu.VMEM((tokens + 8, 2 * LANES), F32),
                        pltpu.VMEM((2 * LANES, width), BF),
                        pltpu.VMEM((3 * CHUNK, width), F32),
                        pltpu.VMEM((4, 2 * length // CHUNK, CHUNK), F32),
                        pltpu.SemaphoreType.DMA((2, 3))],
        compiler_params=pltpu.CompilerParams(collective_id=2, has_side_effects=True),
        cost_estimate=pl.CostEstimate(flops=4 * 10**9, bytes_accessed=30 * 2**20, transcendentals=10**7),
        name="scan_forward",
    )(proj, dg, convx, convbc, head, lane)


def ssd_backward(proj, y, dy, states, convx, convbc, head, lane, partial, grads, resid, tokens=256):
    length, total = proj.shape
    width = convx.shape[1]
    subs = tokens // CHUNK
    n = length // tokens
    dp, tp = lax.axis_size("dp"), lax.axis_size("tensor")
    whole = lambda a: pl.BlockSpec(a.shape, lambda i: (0,) * a.ndim)
    rev = lambda i: (n - 1 - i, 0)
    own = lambda shape: pl.BlockSpec(shape, lambda i: (0, 0))
    hbm = pl.BlockSpec(memory_space=pl.ANY)
    block_shape = (length // tp, partial.shape[1])
    owned_shape = (grads.shape[0] // dp, grads.shape[1])
    return pl.pallas_call(
        functools.partial(backward_kernel, width, dp // 2),
        grid=(n,),
        in_specs=[pl.BlockSpec((tokens, total), rev),
                  pl.BlockSpec((8, total), lambda i: (jnp.maximum((n - 1 - i) * (tokens // 8) - 1, 0), 0)),
                  pl.BlockSpec((tokens, width), rev),
                  pl.BlockSpec((tokens, width), rev),
                  pl.BlockSpec((subs, LANES, width), lambda i: (n - 1 - i, 0, 0)),
                  whole(convx), whole(convbc), whole(head), whole(lane), hbm, hbm, hbm],
        out_specs=[pl.BlockSpec((tokens, total - width), rev),
                   pl.BlockSpec((6, 8, width), lambda i: (0, 0, 0)),
                   pl.BlockSpec((5, 8, 2 * LANES), lambda i: (0, 0, 0)),
                   pl.BlockSpec((2, 8, LANES), lambda i: (0, 0, 0)),
                   own(block_shape), own(owned_shape)],
        out_shape=[jax.ShapeDtypeStruct((length, total - width), BF),
                   jax.ShapeDtypeStruct((6, 8, width), F32),
                   jax.ShapeDtypeStruct((5, 8, 2 * LANES), F32),
                   jax.ShapeDtypeStruct((2, 8, LANES), F32),
                   jax.ShapeDtypeStruct(block_shape, F32),
                   jax.ShapeDtypeStruct(owned_shape, F32)],
        scratch_shapes=[pltpu.VMEM((LANES, width), F32),
                        pltpu.VMEM((8, width), F32),
                        pltpu.VMEM((tokens + 8, width), F32),
                        pltpu.VMEM((tokens + 8, 2 * LANES), F32),
                        pltpu.VMEM((8, width), F32),
                        pltpu.VMEM((8, 2 * LANES), F32),
                        pltpu.VMEM((2 * LANES, width), BF),
                        pltpu.VMEM((3 * CHUNK, width), F32)] + reduction_scratch(dp // 2, block_shape, owned_shape),
        compiler_params=pltpu.CompilerParams(collective_id=3, has_side_effects=True, vmem_limit_bytes=62 * 2**20),
        cost_estimate=pl.CostEstimate(flops=12 * 10**9, bytes_accessed=50 * 2**20, transcendentals=10**7),
        name="scan_backward",
    )(proj, proj, y, dy, states, convx, convbc, head, lane, partial, grads, resid)


def middle_kernel(width, inner_channels, z_ref, y_ref, dg_ref, s_ref, lane_ref, normed, cot, out_t,
                  dy_ref, dz_ref, out_ref, grads_ref, gg_ref, gated, acc_z, acc_o):
    tokens = z_ref.shape[0]
    step = pl.program_id(0)
    half = s_ref.shape[0] // 2

    @pl.when(step == 0)
    def _():
        gg_ref[...] = jnp.zeros_like(gg_ref)
        acc_z[...] = jnp.zeros_like(acc_z)
        acc_o[...] = jnp.zeros_like(acc_o)

    for sub in range(tokens // CHUNK):
        span = slice(sub * CHUNK, (sub + 1) * CHUNK)
        at = step * (tokens // CHUNK) + sub
        wide = lambda row: jnp.broadcast_to(row, (8, CHUNK)).T[:, 0:1]
        squares, dots = wide(s_ref[pl.ds(at, 1), :]), wide(s_ref[pl.ds(half + at, 1), :])
        inv = lax.rsqrt(squares / inner_channels + EPSILON)
        mean = inv * dots / inner_channels
        for q in range(width // LANES):
            lanes = slice(q * LANES, (q + 1) * LANES)
            gain = lane_ref[1:2, lanes]
            y, z, dg = y_ref[span, lanes], z_ref[span, lanes], dg_ref[span, lanes]
            sz = _sigmoid(z)
            act = z * sz
            quot = y * act * inv
            gg_ref[:, lanes] += _rows_sum(dg * quot)
            gated[span, lanes] = (quot * gain).astype(BF)
            d_prod = inv * (dg * gain - quot * mean)
            dy_ref[span, lanes] = (d_prod * act).astype(BF)
            dz_ref[span, lanes] = (d_prod * y * sz * (1.0 + z * (1.0 - sz))).astype(BF)
    out_ref[...] = _dot_last(gated[...], out_t[...]).astype(BF)
    first = lambda a, b: lax.dot_general(a, b, (((0,), (0,)), ((), ())), preferred_element_type=F32)
    acc_z[...] += first(normed[...], dz_ref[...])
    acc_o[...] += first(cot[...], gated[...])

    @pl.when(step == pl.num_programs(0) - 1)
    def _():
        grads_ref[:, :width] = acc_z[...].astype(BF)
        grads_ref[:, width:] = acc_o[...].astype(BF)


def middle(proj, y, dg, sums, lane, normed, cot, out_t, inner_channels, tokens=512):
    length, model = normed.shape
    width = y.shape[1]
    at = lambda cols: pl.BlockSpec((tokens, cols), lambda i: (i, 0))
    once = lambda shape: pl.BlockSpec(shape, lambda i: (0, 0), pipeline_mode=pl.Buffered(1))
    return pl.pallas_call(
        functools.partial(middle_kernel, width, inner_channels),
        grid=(length // tokens,),
        in_specs=[at(width), at(width), at(width), once(sums.shape), once(lane.shape), at(model), at(model),
                  once(out_t.shape)],
        out_specs=[at(width), at(width), at(model), once((model, 2 * width)), once((8, width))],
        out_shape=[jax.ShapeDtypeStruct((length, width), BF),
                   jax.ShapeDtypeStruct((length, width), BF),
                   jax.ShapeDtypeStruct((length, model), BF),
                   jax.ShapeDtypeStruct((model, 2 * width), BF),
                   jax.ShapeDtypeStruct((8, width), F32)],
        scratch_shapes=[pltpu.VMEM((tokens, width), BF),
                        pltpu.VMEM((model, width), F32),
                        pltpu.VMEM((model, width), F32)],
        cost_estimate=pl.CostEstimate(flops=15 * 10**9, bytes_accessed=50 * 2**20, transcendentals=10**6),
        name="middle",
    )(proj, y, dg, sums, lane, normed, cot, out_t)


def pad_rows(a, rows):
    return jnp.pad(a, ((0, rows - a.shape[0]), (0, 0)))


def pack_params(conv_x_weight, conv_x_bias, conv_bc_weight, conv_bc_bias, dt_bias, a_log, skip_gain, gate_gain):
    width = conv_x_weight.shape[1]
    convx = pad_rows(jnp.concatenate([conv_x_weight, conv_x_bias[None]], 0), 8)
    convbc = pad_rows(jnp.concatenate([conv_bc_weight, conv_bc_bias[None]], 0), 8)
    heads = dt_bias.shape[0]
    head = jnp.pad(jnp.stack([dt_bias, a_log]), ((0, 6), (0, LANES - heads)))
    lane = pad_rows(jnp.stack([jnp.repeat(skip_gain, width // heads), gate_gain]), 8)
    return convx, convbc, head, lane
def gather_kernel(outer_n, heads, small, wzx, wdt, wbc, wout, resid_in, cot_in,
                  small_all, inv_out, normed_out, cot_out, weight_out, wout_out, proj, d_gated,
                  normed, cot, weight, w_out, resid, cot_f, stage, stage_g,
                  small_t, small_d, bc_slots, dt_slots,
                  small_sem_t, small_sem_d, bc_sem_t, bc_sem_d, dt_sem, norm_sem, cot_sem, zx_sem, wo_sem,
                  local_sem, stage_sem, stage_g_sem):
    z, y, x, c = _place()
    me = _peer(z, y, x, c)
    t = x * 2 + c
    d = z * 2 + y
    block, zx_cols = wzx.shape
    bc_cols = wbc.shape[1]
    bc_rows = wbc.shape[0]
    wparts = _parts(block)
    bsize = block // wparts
    own_rows, model = resid.shape
    size = own_rows // PARTS
    length = normed.shape[0]
    tile = stage.shape[1]
    loads = [pltpu.make_async_copy(resid_in, resid, local_sem.at[0]),
             pltpu.make_async_copy(cot_in, cot_f, local_sem.at[1])]
    for copy in loads:
        copy.start()
    _greet(outer_n)
    dp_peers = [(k, j) for k in range(outer_n) for j in (0, 1) if k or j]
    tensor_peers = [(k, j) for k in (0, 1) for j in (0, 1) if k or j]
    order = list(range(1, outer_n))
    order.sort(key=lambda k: -min(k, outer_n - k))
    at_dp = lambda k, j: _peer((z + k) % outer_n, (y + j) % 2, x, c)
    at_tensor = lambda k, j: _peer(z, y, (x + k) % 2, (c + j) % 2)

    small_first = [_remote(small, small_d.at[i], small_sem_d.at[0, i], small_sem_d.at[1, i], at_dp(k, j))
                   for i, (k, j) in enumerate(dp_peers)]
    bc_first = [_remote(wbc, bc_slots.at[t, d], bc_sem_d.at[0, i], bc_sem_d.at[1, i], at_dp(k, j))
                for i, (k, j) in enumerate(dp_peers)]
    dt_first = [_remote(wdt, dt_slots.at[d], dt_sem.at[0, i], dt_sem.at[1, i], at_dp(k, j))
                for i, (k, j) in enumerate(dp_peers)]
    for copy in small_first + bc_first + dt_first:
        copy.start()

    def rows_of(outer, inner, part):
        return _rows((outer * 2 + inner) * block + part * bsize, bsize)

    def across(src, dst, cols, sem, k, part):
        return _remote(src.at[pl.ds(part * bsize, bsize), :], dst.at[rows_of(z, y, part), cols],
                       sem.at[0, k, part], sem.at[1, k, part], _peer(lax.rem(z + k, outer_n), y, x, c))

    def beside(src, dst, cols, sem, part):
        return _remote(src.at[pl.ds(part * bsize, bsize), :], dst.at[rows_of(z, y, part), cols],
                       sem.at[2, 0, part], sem.at[3, 0, part], _peer(z, 1 - y, x, c))

    def onward(dst, cols, sem, k, part):
        view = dst.at[rows_of(lax.rem(z - k + outer_n, outer_n), y, part), cols]
        return _remote(view, view, sem.at[2, k, part], sem.at[3, k, part], _peer(z, 1 - y, x, c))

    def send_out(src, dst, cols, sem):
        for part in range(wparts):
            for k in order:
                across(src, dst, cols, sem, k, part).start()
            beside(src, dst, cols, sem, part).start()

    def pass_on(src, dst, cols, sem, part):
        for k in order:
            across(src, dst, cols, sem, k, part).wait_recv()
            onward(dst, cols, sem, k, part).start()

    def finish(src, dst, cols, sem):
        for part in range(wparts):
            for k in range(outer_n):
                onward(dst, cols, sem, k, part).wait_recv()

    def finish_sends(src, dst, cols, sem):
        for part in range(wparts):
            beside(src, dst, cols, sem, part).wait_send()
            for k in order:
                across(src, dst, cols, sem, k, part).wait_send()
                onward(dst, cols, sem, k, part).wait_send()

    zx = (wzx, weight, pl.ds(0, zx_cols), zx_sem)
    wo = (wout, w_out, pl.ds(0, wout.shape[1]), wo_sem)
    send_out(*zx)
    mine = _rows(d * block, block)
    place = [pltpu.make_async_copy(wzx, weight.at[mine, pl.ds(0, zx_cols)], local_sem.at[2]),
             pltpu.make_async_copy(wout, w_out.at[mine, :], local_sem.at[3])]
    for copy in place:
        copy.start()
    bc_slots[t, d] = wbc[...]
    dt_slots[d] = wdt[...]
    loads[0].wait()
    values = resid[...]
    inv = lax.rsqrt(jnp.mean(values * values, axis=-1, keepdims=True) + EPSILON)
    inv_out[...] = jnp.broadcast_to(inv, inv_out.shape)

    for copy in small_first + bc_first:
        copy.wait_recv()
    total = small[...]
    for i in range(len(dp_peers)):
        total = total + small_d[i]
    small_t[3] = total
    small_second = [_remote(small_t.at[3], small_t.at[i], small_sem_t.at[0, i], small_sem_t.at[1, i], at_tensor(k, j))
                    for i, (k, j) in enumerate(tensor_peers)]
    bc_second = [_remote(bc_slots.at[t], bc_slots.at[t], bc_sem_t.at[0, i], bc_sem_t.at[1, i], at_tensor(k, j))
                 for i, (k, j) in enumerate(tensor_peers)]
    for copy in small_second:
        copy.start()
    send_out(*wo)
    for copy in small_second:
        copy.wait_recv()
    total = small_t[3]
    for i in range(3):
        total = total + small_t[i]
    small_all[...] = total
    own_at = _rows(t * own_rows, own_rows)
    for j in range(model // LANES):
        lanes = slice(j * LANES, (j + 1) * LANES)
        normed[own_at, lanes] = (resid[:, lanes] * inv * total[j : j + 1, :]).astype(BF)

    def token_rows(far, near, part):
        return _rows((far * 2 + near) * own_rows + part * size, size)

    def token_copy(buf, sem, which, part):
        far = 1 - x if which == 2 else x
        view = buf.at[token_rows(far, c, part), :]
        peer = _peer(z, y, 1 - x, c) if which == 0 else _peer(z, y, x, 1 - c)
        return _remote(view, view, sem.at[0, which, part], sem.at[1, which, part], peer)

    def send_tokens(buf, sem):
        for part in range(PARTS):
            token_copy(buf, sem, 0, part).start()
            token_copy(buf, sem, 1, part).start()

    def pass_tokens(buf, sem, part):
        token_copy(buf, sem, 0, part).wait_recv()
        token_copy(buf, sem, 2, part).start()

    def finish_tokens(buf, sem):
        for part in range(PARTS):
            token_copy(buf, sem, 1, part).wait_recv()
            token_copy(buf, sem, 2, part).wait_recv()

    send_tokens(normed, norm_sem)
    for copy in bc_second:
        copy.start()
    loads[1].wait()
    cot[own_at, :] = cot_f[...].astype(BF)
    send_tokens(cot, cot_sem)
    for copy in dt_first:
        copy.wait_recv()
    for copy in place:
        copy.wait()
    for i in range(outer_n * 2):
        columns = dt_slots[i].astype(F32)
        columns = jnp.concatenate([columns, jnp.zeros((LANES - columns.shape[0], columns.shape[1]), F32)], axis=0)
        weight[i * block : (i + 1) * block, zx_cols + bc_cols :] = columns.T[:block, :].astype(BF)
    for part in range(max(PARTS, wparts)):
        if part < wparts:
            pass_on(*zx, part)
        if part < PARTS:
            pass_tokens(normed, norm_sem, part)
    for copy in bc_second:
        copy.wait_recv()
    for i in range(outer_n * 2):
        for j in range(4):
            first = i * block + j * bc_rows
            weight[first : first + bc_rows, zx_cols : zx_cols + bc_cols] = bc_slots[j, i]
    finish_tokens(normed, norm_sem)
    finish(*zx)
    save = [pltpu.make_async_copy(normed, normed_out, local_sem.at[4]),
            pltpu.make_async_copy(weight, weight_out, local_sem.at[5])]
    for copy in save:
        copy.start()

    steps = length // tile

    def store(ref, buf, sem, i):
        slot = lax.rem(i, 2)
        return pltpu.make_async_copy(buf.at[slot], ref.at[pl.ds(pl.multiple_of(i * tile, tile), tile), :], sem.at[slot])

    @pl.loop(0, steps)
    def _(i):
        @pl.when(i >= 2)
        def _():
            store(proj, stage, stage_sem, i - 2).wait()

        rows = pl.ds(pl.multiple_of(i * tile, tile), tile)
        stage[lax.rem(i, 2)] = jnp.dot(normed[rows, :], weight[...], preferred_element_type=F32)
        store(proj, stage, stage_sem, i).start()

        @pl.when(i < wparts)
        def _():
            pass_on(*wo, i)

        @pl.when(i < PARTS)
        def _():
            pass_tokens(cot, cot_sem, i)

    for i in range(steps, wparts):
        pass_on(*wo, i)
    for i in range(steps, PARTS):
        pass_tokens(cot, cot_sem, i)
    finish_tokens(cot, cot_sem)
    finish(*wo)
    save_late = [pltpu.make_async_copy(cot, cot_out, local_sem.at[6]),
                 pltpu.make_async_copy(w_out, wout_out, local_sem.at[7])]
    for copy in save_late:
        copy.start()

    @pl.loop(0, steps)
    def _(i):
        @pl.when(i >= 2)
        def _():
            store(d_gated, stage_g, stage_g_sem, i - 2).wait()

        rows = pl.ds(pl.multiple_of(i * tile, tile), tile)
        stage_g[lax.rem(i, 2)] = jnp.dot(cot[rows, :], w_out[...], preferred_element_type=F32)
        store(d_gated, stage_g, stage_g_sem, i).start()

    for i in range(max(steps - 2, 0), steps):
        store(proj, stage, stage_sem, i).wait()
        store(d_gated, stage_g, stage_g_sem, i).wait()
    finish_sends(*zx)
    finish_sends(*wo)
    for part in range(PARTS):
        for which in range(3):
            token_copy(normed, norm_sem, which, part).wait_send()
            token_copy(cot, cot_sem, which, part).wait_send()
    for copy in small_first + bc_first + dt_first + small_second + bc_second:
        copy.wait_send()
    for copy in save + save_late:
        copy.wait()


def gather_all(small, resid, cot, wzx, wdt, wbc, wout, tile=256):
    dp, tp = lax.axis_size("dp"), lax.axis_size("tensor")
    outer_n = dp // 2
    block, zx_cols = wzx.shape
    total = zx_cols + wbc.shape[1] + LANES
    width = wout.shape[1]
    heads = wdt.shape[1]
    length, model = resid.shape[0] * tp, resid.shape[1]
    wdt = jnp.pad(wdt.T, ((0, -heads % 16), (0, -block % LANES)))
    wparts = _parts(block)
    vm = pl.BlockSpec(memory_space=pltpu.VMEM)
    hbm = pl.BlockSpec(memory_space=pl.ANY)
    dma = pltpu.SemaphoreType.DMA
    shape = jax.ShapeDtypeStruct
    return pl.pallas_call(
        functools.partial(gather_kernel, outer_n, heads),
        in_specs=[vm] * 5 + [hbm] * 2,
        out_specs=[vm] * 2 + [hbm] * 6,
        out_shape=[shape(small.shape, F32), shape((resid.shape[0], LANES), F32), shape((length, model), BF), shape((length, model), BF),
                   shape((model, total), BF), shape((model, width), BF),
                   shape((length, total), F32), shape((length, width), F32)],
        scratch_shapes=[pltpu.VMEM((length, model), BF), pltpu.VMEM((length, model), BF),
                        pltpu.VMEM((model, total), BF), pltpu.VMEM((model, width), BF),
                        pltpu.VMEM(resid.shape, F32), pltpu.VMEM(resid.shape, F32),
                        pltpu.VMEM((2, tile, total), F32), pltpu.VMEM((2, tile, width), F32),
                        pltpu.VMEM((4,) + small.shape, F32), pltpu.VMEM((dp - 1,) + small.shape, F32),
                        pltpu.VMEM((4, dp) + wbc.shape, BF), pltpu.VMEM((dp,) + wdt.shape, BF),
                        dma((2, 3)), dma((2, dp - 1)), dma((2, 3)), dma((2, dp - 1)), dma((2, dp - 1)),
                        dma((2, 3, PARTS)), dma((2, 3, PARTS)), dma((4, outer_n, wparts)), dma((4, outer_n, wparts)),
                        dma((8,)), dma((2,)), dma((2,))],
        compiler_params=pltpu.CompilerParams(collective_id=0, has_side_effects=True, vmem_limit_bytes=62 * 2**20),
        cost_estimate=pl.CostEstimate(flops=17 * 10**9, bytes_accessed=60 * 2**20, transcendentals=0),
        name="gather_all",
    )(small, wzx, wdt, wbc, wout, resid, cot)


def final_kernel(outer_n, both_rows, gain_rows, dz_in, rest_in, weight_in, normed_in, small, gain,
                 d_local, owned, small_out, bc_out,
                 dz, rest, weight, normed, g_all, tok, near_buf, far_src, far_buf, in_buf, out_src, out_buf,
                 small_d, small_t, gain_d, gain_t, gain_acc, bc_src, bc_buf,
                 load_sem, near_sem, far_sem, in_sem, out_sem, small_sem_d, small_sem_t, gain_sem_d, gain_sem_t, bc_sem):
    z, y, x, c = _place()
    me = _peer(z, y, x, c)
    t = x * 2 + c
    own_rows, model = d_local.shape
    block, cols = owned.shape
    width = dz.shape[1]
    wparts = _parts(block)
    bsize = block // wparts
    size = own_rows // PARTS
    half = own_rows // 2
    per_group = next(g for g in range(1, outer_n + 1) if (2 * g * block) % LANES == 0)
    groups = outer_n // per_group
    loads = [pltpu.make_async_copy(src, dst, load_sem.at[i]) for i, (src, dst) in enumerate(
        [(rest_in, rest), (normed_in, normed), (dz_in, dz), (weight_in, weight)])]
    for copy in loads:
        copy.start()
    _greet(outer_n)
    dp_peers = [(k, j) for k in range(outer_n) for j in (0, 1) if k or j]
    tensor_peers = [(k, j) for k in (0, 1) for j in (0, 1) if k or j]

    def dp_copies(src, dst, sem):
        return [_remote(src, dst.at[k * 2 + j], sem.at[0, i], sem.at[1, i],
                        _peer((z + k) % outer_n, (y + j) % 2, x, c)) for i, (k, j) in enumerate(dp_peers)]

    def tensor_copies(src, dst, sem):
        return [_remote(src, dst.at[k * 2 + j], sem.at[0, i], sem.at[1, i],
                        _peer(z, y, (x + k) % 2, (c + j) % 2)) for i, (k, j) in enumerate(tensor_peers)]

    def dp_total(buf):
        total = None
        for zz in range(outer_n):
            for yy in (0, 1):
                term = buf[lax.rem(z - zz + outer_n, outer_n) * 2 + lax.rem(y - yy + 2, 2)]
                total = term if total is None else total + term
        return total

    def near_copy(i, part):
        at = pl.ds(part * size, size)
        return _remote(tok.at[2 * i, at, :], near_buf.at[i, at, :], near_sem.at[0, i, part], near_sem.at[1, i, part],
                       _peer(z, y, x, 1 - c))

    def far_copy(part):
        at = pl.ds(part * size, size)
        return _remote(far_src.at[at, :], far_buf.at[at, :], far_sem.at[0, part], far_sem.at[1, part],
                       _peer(z, y, 1 - x, c))

    def in_copy(k, zz, part):
        at = pl.ds(part * bsize, bsize)
        return _remote(g_all.at[zz, 1 - y, at, :], in_buf.at[k, at, :], in_sem.at[0, k, part], in_sem.at[1, k, part],
                       _peer(z, 1 - y, x, c))

    def out_copy(k, part):
        at = pl.ds(part * bsize, bsize)
        return _remote(out_src.at[k - 1, at, :], out_buf.at[k - 1, at, :], out_sem.at[0, k - 1, part],
                       out_sem.at[1, k - 1, part], _peer((z + k) % outer_n, y, x, c))

    def token_product(i, part):
        a, b = i // 2, i % 2
        far, near = (1 - x) * (1 - a) + x * a, (1 - c) * (1 - b) + c * b
        rows = pl.ds(pl.multiple_of((far * 2 + near) * own_rows + part * half, LANES), half)
        value = _dot_last(dz[rows, :], weight[:, :width]) + _dot_last(rest[rows, :], weight[:, width:])
        gain_acc[...] += _rows_sum(value * normed[rows, :].astype(F32))
        at = pl.ds(pl.multiple_of(part * half, LANES), half)

        @pl.when(i < 3)
        def _():
            tok[i, at, :] = value.astype(BF)

        @pl.when(i == 3)
        def _():
            d_local[at, :] = value

    def group(i):
        grp = lax.rem(z // per_group + 1 + i, groups)
        at = pl.ds(pl.multiple_of(grp * (2 * per_group * block), LANES), 2 * per_group * block)
        value = lax.dot_general(normed[:, at], rest[...], (((0,), (0,)), ((), ())), preferred_element_type=F32)
        for j in range(per_group):
            zz = grp * per_group + j
            for yy in (0, 1):
                first = (2 * j + yy) * block
                g_all[zz, yy] = value[first : first + block, :].astype(BF)
            k = lax.rem(zz - z + outer_n, outer_n)
            for part in range(wparts):
                in_copy(k, zz, part).start()

    def token_step(part):
        at = pl.ds(part * size, size)
        near_copy(0, part).wait_recv()
        far_src[at, :] = (tok[1, at, :].astype(F32) + near_buf[0, at, :].astype(F32)).astype(BF)
        far_copy(part).start()

    def grad_step(k, part):
        at = pl.ds(part * bsize, bsize)
        zz = lax.rem(z + k, outer_n)
        in_copy(k, zz, part).wait_recv()
        both = g_all[zz, y, at, :].astype(F32) + in_buf[k, at, :].astype(F32)
        if k:
            out_src[k - 1, at, :] = both.astype(BF)
            out_copy(k, part).start()
        else:
            owned[at, :] = both

    small_d[0] = small[...]
    first = dp_copies(small, small_d, small_sem_d)
    for copy in first:
        copy.start()
    for copy in loads[:2]:
        copy.wait()
    gain_acc[...] = jnp.zeros_like(gain_acc)
    parts_half = PARTS // 2
    order = list(range(1, outer_n)) + [0]
    todo = [(k, part) for k in order for part in range(wparts)]
    cut = lambda eighths: todo[: eighths * len(todo) // 8]
    per_slot = -(-groups // 4)
    second = tensor_copies(small_t.at[0], small_t, small_sem_t)

    def near_start(i, which):
        for part in range(which * parts_half, (which + 1) * parts_half):
            near_copy(i, part).start()

    def far_start(which):
        for part in range(which * parts_half, (which + 1) * parts_half):
            token_step(part)

    def grads_between(low, high):
        for k, part in cut(high)[len(cut(low)) :]:
            grad_step(k, part)

    def small_second():
        for copy in first:
            copy.wait_recv()
        total = dp_total(small_d)
        small_out[...] = total
        small_t[0] = total[:both_rows, :]
        for copy in second:
            copy.start()

    after = {
        0: lambda: near_start(0, 0),
        1: lambda: far_start(0),
        2: lambda: near_start(0, 1),
        3: lambda: (far_start(1), small_second(), grads_between(0, 1)),
        4: lambda: (near_start(1, 0), grads_between(1, 2)),
        5: lambda: grads_between(2, 4),
        6: lambda: (near_start(1, 1), grads_between(4, 5)),
        7: lambda: grads_between(5, 6),
    }

    @pl.loop(0, 8)
    def _(it):
        for r in range(per_slot):
            @pl.when((it % 2 == 0) & (it // 2 * per_slot + r < groups))
            def _():
                group(it // 2 * per_slot + r)

        @pl.when(it == 0)
        def _():
            for copy in loads[2:]:
                copy.wait()

        token_product(it // 4 * 2 + it % 2, it // 2 % 2)
        for step, piece in after.items():
            @pl.when(it == step)
            def _(piece=piece):
                piece()

    for j in range(gain_rows):
        gain_d[0, j : j + 1, :] = jnp.sum(
            gain_acc[:, j * LANES : (j + 1) * LANES], axis=0, keepdims=True) / gain[j : j + 1, :]
    gain_first = dp_copies(gain_d.at[0], gain_d, gain_sem_d)
    for copy in gain_first:
        copy.start()
    gain_second = tensor_copies(gain_t.at[0], gain_t, gain_sem_t)

    def token_finish(part):
        at = pl.ds(part * size, size)
        near_copy(1, part).wait_recv()
        far_copy(part).wait_recv()
        d_local[at, :] = d_local[at, :] + near_buf[1, at, :].astype(F32) + far_buf[at, :].astype(F32)

    grads_between(6, 7)
    for copy in gain_first:
        copy.wait_recv()
    gain_t[0] = dp_total(gain_d)
    for copy in gain_second:
        copy.start()
    for part in range(parts_half):
        token_finish(part)
    grads_between(7, 8)
    for part in range(parts_half, PARTS):
        token_finish(part)
    for part in range(wparts):
        at = pl.ds(part * bsize, bsize)
        total = owned[at, :]
        for k in order[:-1]:
            out_copy(k, part).wait_recv()
            total = total + out_buf[k - 1, at, :].astype(F32)
        owned[at, :] = total
    bc_rows = block // 4
    for i in range(4):
        bc_src[i] = owned[i * bc_rows : (i + 1) * bc_rows, width : width + 2 * LANES]
    bc_copies = []
    for i, (k, j) in enumerate(tensor_peers):
        other = lax.rem(x + k, 2) * 2 + lax.rem(c + j, 2)
        bc_copies.append(_remote(bc_src.at[other], bc_buf.at[i], bc_sem.at[0, i], bc_sem.at[1, i],
                                 _peer(z, y, (x + k) % 2, (c + j) % 2)))
    for copy in bc_copies:
        copy.start()
    for copy in second:
        copy.wait_recv()
    small_out[0:both_rows, :] = (small_t[0] + small_t[1]) + (small_t[2] + small_t[3])
    for copy in bc_copies:
        copy.wait_recv()
    bc_out[...] = (bc_src[t] + bc_buf[0]) + (bc_buf[1] + bc_buf[2])
    for copy in gain_second:
        copy.wait_recv()
    gains = (gain_t[0] + gain_t[1]) + (gain_t[2] + gain_t[3])
    small_out[0:gain_rows, :] = gains[:gain_rows, :]
    for part in range(PARTS):
        near_copy(0, part).wait_send()
        near_copy(1, part).wait_send()
        far_copy(part).wait_send()
    for k in range(outer_n):
        zz = lax.rem(z + k, outer_n)
        for part in range(wparts):
            in_copy(k, zz, part).wait_send()
            if k:
                out_copy(k, part).wait_send()
    for copy in first + second + gain_first + gain_second + bc_copies:
        copy.wait_send()


def final_sums(dz, rest, weight, normed, small, gain, both_rows):
    dp, tp = lax.axis_size("dp"), lax.axis_size("tensor")
    outer_n = dp // 2
    own_rows, model = normed.shape[0] // tp, normed.shape[1]
    block, cols = model // dp, rest.shape[1]
    gain_rows = model // LANES
    gain_pad = -(-gain_rows // 8) * 8
    wparts = _parts(block)
    vm = pl.BlockSpec(memory_space=pltpu.VMEM)
    hbm = pl.BlockSpec(memory_space=pl.ANY)
    dma = pltpu.SemaphoreType.DMA
    tokens = (own_rows, model)
    bc = (4, block // 4, 2 * LANES)
    return pl.pallas_call(
        functools.partial(final_kernel, outer_n, both_rows, gain_rows),
        in_specs=[hbm] * 4 + [vm] * 2,
        out_specs=[vm] * 4,
        out_shape=[jax.ShapeDtypeStruct(tokens, F32),
                   jax.ShapeDtypeStruct((block, cols), F32),
                   jax.ShapeDtypeStruct(small.shape, F32),
                   jax.ShapeDtypeStruct(bc[1:], F32)],
        scratch_shapes=[pltpu.VMEM(dz.shape, BF), pltpu.VMEM(rest.shape, BF), pltpu.VMEM(weight.shape, BF),
                        pltpu.VMEM(normed.shape, BF),
                        pltpu.VMEM((outer_n, 2, block, cols), BF),
                        pltpu.VMEM((3,) + tokens, BF), pltpu.VMEM((2,) + tokens, BF),
                        pltpu.VMEM(tokens, BF), pltpu.VMEM(tokens, BF),
                        pltpu.VMEM((outer_n, block, cols), BF),
                        pltpu.VMEM((outer_n - 1, block, cols), BF), pltpu.VMEM((outer_n - 1, block, cols), BF),
                        pltpu.VMEM((dp,) + small.shape, F32), pltpu.VMEM((4, both_rows, LANES), F32),
                        pltpu.VMEM((dp, gain_pad, LANES), F32), pltpu.VMEM((4, gain_pad, LANES), F32),
                        pltpu.VMEM((8, model), F32), pltpu.VMEM(bc, F32), pltpu.VMEM((3,) + bc[1:], F32),
                        dma((4,)), dma((2, 2, PARTS)), dma((2, PARTS)), dma((2, outer_n, wparts)),
                        dma((2, outer_n - 1, wparts)), dma((2, dp - 1)), dma((2, 3)), dma((2, dp - 1)), dma((2, 3)),
                        dma((2, 3))],
        compiler_params=pltpu.CompilerParams(collective_id=1, has_side_effects=True, vmem_limit_bytes=63 * 2**20),
        cost_estimate=pl.CostEstimate(flops=20 * 10**9, bytes_accessed=40 * 2**20, transcendentals=0),
        name="final_sums",
    )(dz, rest, weight, normed, small, gain)


def _spread(values, index, count):
    size = values.shape[-1]
    full = jnp.zeros(values.shape[:-1] + (size * count,), F32)
    return lax.dynamic_update_slice_in_dim(full, values, index * size, axis=values.ndim - 1)


def _own(values, index, count):
    size = values.shape[-1] // count
    return lax.dynamic_slice_in_dim(values, index * size, size, axis=values.ndim - 1)


def on_device(
    resid_in, norm_gain, proj_zx, proj_dt, proj_bc, conv_x_weight, conv_x_bias, conv_bc_weight,
    conv_bc_bias, dt_bias, a_log, skip_gain, gate_gain, proj_out, cotangent,
):
    dp, tp = lax.axis_size("dp"), lax.axis_size("tensor")
    index = lax.axis_index("dp") * tp + lax.axis_index("tensor")
    count = dp * tp
    model = resid_in.shape[-1]
    width = conv_x_weight.shape[1]
    heads = dt_bias.shape[0]
    inner_channels = width * tp
    states2 = 2 * LANES
    rows = proj_zx.shape[0]
    resid, cot = resid_in[0], cotangent[0]
    small = jnp.concatenate([
        _spread(norm_gain, index, count).reshape(-1, LANES),
        _spread(conv_bc_weight, index, count).reshape(-1, LANES),
        _spread(conv_bc_bias, index, count).reshape(-1, LANES)], axis=0)
    gain_rows = model // LANES
    both_rows = -(-small.shape[0] // 8) * 8
    small = pad_rows(small, both_rows)
    small_all, inv_in, normed, cot_full, weight, out_t, proj, d_gated = gather_all(
        small, resid, cot, proj_zx.reshape(rows, 2 * width), proj_dt, proj_bc, proj_out.T)
    full_cbw = small_all[gain_rows : gain_rows + 4 * states2 // LANES].reshape(4, states2)
    full_cbb = small_all[gain_rows + 4 * states2 // LANES : gain_rows + 5 * states2 // LANES].reshape(states2)
    full_gain = small_all[:gain_rows].reshape(model)
    packs = pack_params(conv_x_weight, conv_x_bias, full_cbw, full_cbb, dt_bias, a_log, skip_gain, gate_gain)
    y, states, partial = ssd_forward(proj, d_gated, *packs)
    dy, dz, out_partial, grads_zo, ggain = middle(proj, y, d_gated, partial, packs[3], normed, cot_full, out_t, inner_channels)
    d_rest, gx, gbc, gh, block_out, owned_zo = ssd_backward(proj, y, dy, states, *packs, out_partial, grads_zo, resid)
    gx = jnp.concatenate([gx.sum(1), ggain.sum(0)[None]], 0)
    gbc, gh = gbc.sum(1), gh.sum(1)
    to_sum = jnp.concatenate([
        pad_rows(jnp.concatenate([jnp.zeros((gain_rows, LANES), F32), gbc.reshape(-1, LANES)], 0), both_rows),
        gx.reshape(-1, LANES), gh], axis=0)
    to_sum = pad_rows(to_sum, -(-to_sum.shape[0] // 8) * 8)
    d_local, owned, totals, grad_bc = final_sums(dz, d_rest, weight, normed, to_sum, small_all, both_rows)
    inv_in = inv_in[:, :1]
    scaled = resid * inv_in
    d_scaled = d_local * full_gain
    grad_resid = inv_in * (d_scaled - scaled * jnp.mean(d_scaled * scaled, axis=-1, keepdims=True)) + cot
    grad_zx = jnp.stack([owned_zo[:, :width], owned[:, :width]], axis=1)
    grad_dt = owned[:, width + states2 : width + states2 + heads]
    owned_out = owned_zo[:, width:].T
    owned_gain = _own(totals[:gain_rows].reshape(model), index, count)
    at = gain_rows + 4 * states2 // LANES
    owned_cbw = _own(totals[gain_rows:at].reshape(4, states2), index, count)
    owned_cbb = _own(totals[at : at + states2 // LANES].reshape(states2), index, count)
    gx_all = totals[both_rows : both_rows + 7 * width // LANES].reshape(7, width)
    gh_all = totals[both_rows + 7 * width // LANES :]
    skip = gx_all[5].reshape(heads, -1).sum(1)
    return (
        block_out[None], grad_resid[None], owned_gain, grad_zx, grad_dt, grad_bc, gx_all[:4], gx_all[4],
        owned_cbw, owned_cbb, gh_all[0, :heads], gh_all[1, :heads], skip, gx_all[6], owned_out,
    )


def solution(mesh):
    specs = (
        P("dp", "tensor", None), P(("dp", "tensor")), P("dp", None, "tensor"), P("dp", "tensor"),
        P(("dp", "tensor"), None), P(None, "tensor"), P("tensor"), P(None, ("dp", "tensor")),
        P(("dp", "tensor")), P("tensor"), P("tensor"), P("tensor"), P("tensor"), P("tensor", "dp"),
        P("dp", "tensor", None),
    )
    outs = (specs[0], specs[0]) + specs[1:14]
    return jax.shard_map(on_device, mesh=mesh, in_specs=specs, out_specs=outs, check_vma=False)
```

```python
import functools, math
import jax, jax.numpy as jnp
from jax import lax
from jax.experimental import pallas as pl
from jax.experimental.pallas import tpu as pltpu
from jax.sharding import PartitionSpec as P

EPSILON = 1e-05
CHUNK = 128
LANES = 128
TAPS = 4
LOG2E = 1.4426950408889634
BF = jnp.bfloat16
F32 = jnp.float32


MESH = pl.DeviceIdType.MESH
PARTS = 4
ROW_PARTS = 6


def _place():
    d, t = lax.axis_index("dp"), lax.axis_index("tensor")
    return d // 2, d % 2, t // 2, t % 2


def _peer(outer, inner, far, near):
    return (outer * 2 + inner, far * 2 + near)


def _greet(outer_n):
    z, y, x, c = _place()
    barrier = pltpu.get_barrier_semaphore()
    peers = []
    for k in range(outer_n):
        for j in (0, 1):
            if k or j:
                peers.append(_peer((z + k) % outer_n, (y + j) % 2, x, c))
    for k in (0, 1):
        for j in (0, 1):
            if k or j:
                peers.append(_peer(z, y, (x + k) % 2, (c + j) % 2))
    for peer in peers:
        pl.semaphore_signal(barrier, inc=1, device_id=peer, device_id_type=MESH)
    pl.semaphore_wait(barrier, len(peers))


def _parts(rows):
    return max(p for p in range(1, ROW_PARTS + 1) if rows % (16 * p) == 0)


def _remote(src, dst, send, recv, peer):
    return pltpu.make_async_remote_copy(
        src_ref=src, dst_ref=dst, send_sem=send, recv_sem=recv, device_id=peer, device_id_type=MESH)


def _rows(start, size):
    return pl.ds(pl.multiple_of(start, 16), size)


class _RowSums:
    def __init__(self, outer_n, block, source, mine, owned, in_buf, pair_src, pair_buf, cross_src, cross_buf,
                 in_sem, pair_sem, cross_sem):
        self.__dict__.update(locals())
        self.z, self.y, self.x, self.c = _place()
        self.h, self.l = self.z // 2, self.z % 2
        self.pairs = outer_n // 2
        self.parts = _parts(block)
        self.size = block // self.parts
        self.order = list(range(1, self.pairs)) + [0]

    def outer_of(self, r, m):
        low = self.l if m else 1 - self.l
        return lax.rem(self.h + r, self.pairs) * 2 + low

    def slot_of(self, outer):
        r = lax.rem(outer // 2 - self.h + self.pairs, self.pairs)
        low = outer % 2
        return r * 2 + 1 - (low + self.l - 2 * low * self.l)

    def at(self, part):
        return pl.ds(part * self.size, self.size)

    def in_copy(self, slot, outer, part):
        return _remote(self.source(slot, outer, 1 - self.y, part), self.in_buf.at[slot, self.at(part), :],
                       self.in_sem.at[0, slot, part], self.in_sem.at[1, slot, part],
                       _peer(self.z, 1 - self.y, self.x, self.c))

    def pair_copy(self, r, part):
        return _remote(self.pair_src.at[r, self.at(part), :], self.pair_buf.at[r, self.at(part), :],
                       self.pair_sem.at[0, r, part], self.pair_sem.at[1, r, part],
                       _peer(self.h * 2 + 1 - self.l, self.y, self.x, self.c))

    def cross_copy(self, r, part):
        return _remote(self.cross_src.at[r - 1, self.at(part), :], self.cross_buf.at[r - 1, self.at(part), :],
                       self.cross_sem.at[0, r - 1, part], self.cross_sem.at[1, r - 1, part],
                       _peer(lax.rem(self.h + r, self.pairs) * 2 + self.l, self.y, self.x, self.c))

    def todo(self):
        return [(r, m, part) for r in self.order for m in (0, 1) for part in range(self.parts)]

    def step(self, r, m, part):
        at = self.at(part)
        outer = self.outer_of(r, m)
        self.in_copy(r * 2 + m, outer, part).wait_recv()
        both = self.mine(r * 2 + m, outer, part) + self.in_buf[r * 2 + m, at, :].astype(F32)
        if m == 0:
            self.pair_src[r, at, :] = both.astype(BF)
            self.pair_copy(r, part).start()
            return
        self.pair_copy(r, part).wait_recv()
        both = both + self.pair_buf[r, at, :].astype(F32)
        if r:
            self.cross_src[r - 1, at, :] = both.astype(BF)
            self.cross_copy(r, part).start()
        else:
            self.owned[at, :] = both

    def finish(self):
        for part in range(self.parts):
            at = self.at(part)
            total = self.owned[at, :]
            for r in self.order[:-1]:
                self.cross_copy(r, part).wait_recv()
                total = total + self.cross_buf[r - 1, at, :].astype(F32)
            self.owned[at, :] = total

    def wait_sends(self):
        for r, m, part in self.todo():
            self.in_copy(r * 2 + m, self.outer_of(r, m), part).wait_send()
            if m == 0:
                self.pair_copy(r, part).wait_send()
            elif r:
                self.cross_copy(r, part).wait_send()


def row_sums_scratch(outer_n, shape):
    dma = pltpu.SemaphoreType.DMA
    parts, pairs = _parts(shape[0]), outer_n // 2
    return [pltpu.VMEM((outer_n,) + shape, BF), pltpu.VMEM((pairs,) + shape, BF), pltpu.VMEM((pairs,) + shape, BF),
            pltpu.VMEM((pairs - 1,) + shape, BF), pltpu.VMEM((pairs - 1,) + shape, BF),
            dma((2, outer_n, parts)), dma((2, pairs, parts)), dma((2, pairs - 1, parts))]


class _Reduction:
    def __init__(self, outer_n, partial, grads, resid, block_sum, owned, resid_buf, own_tokens, near_buf, far_src,
                 far_buf, own_grads, send_grads, near_sem, far_sem, local_sem, *row_sums):
        self.__dict__.update(locals())
        self.z, self.y, self.x, self.c = _place()
        self.own_rows = block_sum.shape[0]
        self.block = owned.shape[0]
        self.size = self.own_rows // PARTS
        block, size = self.block, self.block // _parts(self.block)
        self.sums = _RowSums(
            outer_n, block,
            lambda slot, outer, inner, part: send_grads.at[slot, pl.ds(part * size, size), :],
            lambda slot, outer, part: own_grads[slot, pl.ds(part * size, size), :].astype(F32),
            owned, *row_sums)

    def token_rows(self, far, near, part):
        return _rows((far * 2 + near) * self.own_rows + part * self.size, self.size)

    def near_copy(self, i, part):
        far = (1 - self.x, self.x)[i]
        at = pl.ds(part * self.size, self.size)
        return _remote(self.partial.at[self.token_rows(far, 1 - self.c, part), :], self.near_buf.at[i, at, :],
                       self.near_sem.at[0, i, part], self.near_sem.at[1, i, part],
                       _peer(self.z, self.y, self.x, 1 - self.c))

    def far_copy(self, part):
        at = pl.ds(part * self.size, self.size)
        return _remote(self.far_src.at[at, :], self.far_buf.at[at, :], self.far_sem.at[0, part],
                       self.far_sem.at[1, part], _peer(self.z, self.y, 1 - self.x, self.c))

    def local_copies(self):
        copies = [pltpu.make_async_copy(self.resid, self.resid_buf, self.local_sem.at[0])]
        for i, far in enumerate((1 - self.x, self.x)):
            rows = _rows((far * 2 + self.c) * self.own_rows, self.own_rows)
            copies.append(pltpu.make_async_copy(self.partial.at[rows, :], self.own_tokens.at[i], self.local_sem.at[1 + i]))
        for r in range(self.outer_n // 2):
            for m in (0, 1):
                rows = _rows((self.sums.outer_of(r, m) * 2 + self.y) * self.block, self.block)
                copies.append(pltpu.make_async_copy(self.grads.at[rows, :], self.own_grads.at[r * 2 + m],
                                                    self.local_sem.at[3 + r * 2 + m]))
        return copies

    def send_loads(self):
        copies = []
        for r in self.sums.order:
            for m in (0, 1):
                rows = _rows((self.sums.outer_of(r, m) * 2 + 1 - self.y) * self.block, self.block)
                copies.append(pltpu.make_async_copy(self.grads.at[rows, :], self.send_grads.at[r * 2 + m],
                                                    self.local_sem.at[3 + self.outer_n + r * 2 + m]))
        return copies

    def begin(self):
        loads = self.send_loads()
        for copy in loads:
            copy.start()
        _greet(self.outer_n)
        for part in range(PARTS):
            self.near_copy(0, part).start()
        for i, (r, m, part) in enumerate(self.sums.todo()):
            if part == 0:
                loads[i // self.sums.parts].wait()
            self.sums.in_copy(r * 2 + m, self.sums.outer_of(r, m), part).start()
        for part in range(PARTS):
            self.near_copy(1, part).start()
        for copy in self.local_copies():
            copy.start()

    def ready(self):
        for copy in self.local_copies():
            copy.wait()

    def token_step(self, part):
        at = pl.ds(part * self.size, self.size)
        self.near_copy(0, part).wait_recv()
        self.far_src[at, :] = (self.own_tokens[0, at, :].astype(F32) + self.near_buf[0, at, :].astype(F32)).astype(BF)
        self.far_copy(part).start()

    def plan(self, steps):
        pieces = [(1, self.ready)]
        for part in range(PARTS):
            pieces.append((min(1 + part, steps - 1), functools.partial(self.token_step, part)))
        todo = self.sums.todo()
        self.late = len(todo) // 8
        for i, item in enumerate(todo[: len(todo) - self.late]):
            pieces.append((min(1 + (i + 3) * (steps - 1) // len(todo), steps - 1),
                           functools.partial(self.sums.step, *item)))
        return pieces

    def end(self):
        for part in range(PARTS):
            at = pl.ds(part * self.size, self.size)
            self.near_copy(1, part).wait_recv()
            self.far_copy(part).wait_recv()
            self.block_sum[at, :] = (self.own_tokens[1, at, :].astype(F32) + self.near_buf[1, at, :].astype(F32)
                                     + self.far_buf[at, :].astype(F32)) + self.resid_buf[at, :]
        for item in self.sums.todo()[-self.late :]:
            self.sums.step(*item)
        self.sums.finish()
        for part in range(PARTS):
            self.near_copy(0, part).wait_send()
            self.near_copy(1, part).wait_send()
            self.far_copy(part).wait_send()
        self.sums.wait_sends()


def reduction_scratch(outer_n, tokens, grads):
    dma = pltpu.SemaphoreType.DMA
    return [pltpu.VMEM(tokens, F32), pltpu.VMEM((2,) + tokens, BF), pltpu.VMEM((2,) + tokens, BF),
            pltpu.VMEM(tokens, BF), pltpu.VMEM(tokens, BF), pltpu.VMEM((outer_n,) + grads, BF), pltpu.VMEM((outer_n,) + grads, BF),
            dma((2, 2, PARTS)), dma((2, PARTS)), dma((3 + 2 * outer_n,))] + row_sums_scratch(outer_n, grads)


def _sigmoid(v):
    return 0.5 * jnp.tanh(0.5 * v) + 0.5


def _softplus(t):
    return jnp.maximum(t, 0.0) + jnp.log1p(jnp.exp(-jnp.abs(t)))


def _dot_last(a, b):
    return lax.dot_general(a, b, (((1,), (1,)), ((), ())), preferred_element_type=F32)


def _dot_exact(a, b):
    return jnp.dot(a, b, precision=lax.Precision.HIGHEST, preferred_element_type=F32)


def _halves(v):
    high = v.astype(BF)
    return high, (v - high.astype(F32)).astype(BF)


def _dot_three(a, b):
    a_high, a_low = _halves(a)
    b_high, b_low = _halves(b)
    return _dot_last(jnp.concatenate([a_high, a_low, a_high], axis=1),
                     jnp.concatenate([b_high, b_high, b_low], axis=1))


def _rows_sum(v):
    return v.reshape(v.shape[0] // 8, 8, v.shape[1]).sum(axis=0)


def _split(lo, v):
    zero = jnp.zeros_like(v)
    return [jnp.where(lo, v, zero), jnp.where(lo, zero, v)]


def _times(dt_raw, head, rows, cols):
    t = dt_raw + head[0:1, :]
    delta = _softplus(t)
    rate = -jnp.exp(head[1:2, :])
    tri = (rows >= cols).astype(F32)
    cum = _dot_exact(tri, delta * (rate * LOG2E))
    return t, delta, rate, cum


def _conv(buf, start, cols, w, length):
    ahead = buf[start : start + 8 + length, cols]
    shifted = [pltpu.roll(ahead, TAPS - 1 - k, 0)[8:] for k in range(TAPS - 1)] + [ahead[8:]]
    v = w[TAPS : TAPS + 1, :] + w[0:1, :] * shifted[0]
    for k in range(1, TAPS):
        v = v + w[k : k + 1, :] * shifted[k]
    return v, shifted


def _conv_back(dv, after, w):
    behind = jnp.concatenate([dv, after], axis=0)
    length = dv.shape[0]
    total = w[TAPS - 1 : TAPS, :] * dv
    for k in range(TAPS - 1):
        total = total + w[k : k + 1, :] * pltpu.roll(behind, length + 8 - (TAPS - 1 - k), 0)[:length]
    return total


def _fill_spread(spread, head_width):
    shape = spread.shape
    head = lax.broadcasted_iota(jnp.int32, shape, 0) % LANES
    lane = lax.broadcasted_iota(jnp.int32, shape, 1)
    spread[...] = (lane // head_width == head).astype(F32).astype(BF)


def _widen(wide, delta, tail, grow, spread):
    high, low = _halves(jnp.concatenate([delta, tail, grow], axis=0))
    wide[...] = jnp.dot(jnp.concatenate([high, low], axis=1), spread[...], preferred_element_type=F32)


def forward_kernel(width, p_ref, dg_ref, convx_ref, convbc_ref, head_ref, lane_ref,
                   y_ref, h_ref, s_ref, state, xbuf, bcbuf, spread, wide, sums, sum_sem):
    tokens = p_ref.shape[0]
    pairs = width // LANES
    step = pl.program_id(0)
    z, y_at, x, c = _place()
    me = x * 2 + c
    half = sums.shape[1] // 2
    tensor_peers = [_peer(z, y_at, (x + k) % 2, (c + j) % 2) for k in (0, 1) for j in (0, 1) if k or j]

    @pl.when(step == 0)
    def _():
        barrier = pltpu.get_barrier_semaphore()
        for peer in tensor_peers:
            pl.semaphore_signal(barrier, inc=1, device_id=peer, device_id_type=MESH)
        pl.semaphore_wait(barrier, len(tensor_peers))
        state[...] = jnp.zeros_like(state)
        _fill_spread(spread, LANES // 2)
        xbuf[0:8, :] = jnp.zeros((8, width), F32)
        bcbuf[0:8, :] = jnp.zeros((8, 2 * LANES), F32)

    @pl.when(step > 0)
    def _():
        xbuf[0:8, :] = xbuf[tokens : tokens + 8, :]
        bcbuf[0:8, :] = bcbuf[tokens : tokens + 8, :]

    xbuf[8 : 8 + tokens, :] = p_ref[:, width : 2 * width]
    bcbuf[8 : 8 + tokens, :] = p_ref[:, 2 * width : 2 * width + 2 * LANES]
    rows = lax.broadcasted_iota(jnp.int32, (CHUNK, CHUNK), 0)
    cols = lax.broadcasted_iota(jnp.int32, (CHUNK, CHUNK), 1)
    lo = cols < LANES // 2
    head = head_ref[...]
    ones = jnp.ones((8, LANES), F32)
    for sub in range(tokens // CHUNK):
        base = sub * CHUNK
        span = slice(base, base + CHUNK)
        vbc, _ = _conv(bcbuf, base, slice(0, 2 * LANES), convbc_ref[...], CHUNK)
        bc = vbc * _sigmoid(vbc)
        b_in, c_out = bc[:, :LANES], bc[:, LANES:]
        c_high, c_low = _halves(c_out)
        c_wide = jnp.concatenate([c_high, c_low, c_high], axis=1)
        _, delta, _, cum = _times(p_ref[span, 2 * width + 2 * LANES :], head, rows, cols)
        cum_t = cum.T
        scores = jnp.where(rows >= cols, _dot_three(c_out, b_in), 0.0)
        last = cum[CHUNK - 1 : CHUNK, :]
        tail = jnp.exp2(last - cum)
        grow = jnp.exp2(cum)
        _widen(wide, delta, tail, grow, spread)
        b_t = b_in.T.astype(BF)
        squares = jnp.zeros((CHUNK, LANES), F32)
        inner = jnp.zeros((CHUNK, LANES), F32)
        h_ref[sub] = state[...]
        for q in range(pairs):
            lanes = slice(q * LANES, (q + 1) * LANES)
            v, _ = _conv(xbuf, base, lanes, convx_ref[:, lanes], CHUNK)
            x_act = v * _sigmoid(v)
            u = x_act * wide[0:CHUNK, lanes]
            left = []
            for h in (2 * q, 2 * q + 1):
                e = jnp.exp2(jnp.minimum(cum[:, h : h + 1] - cum_t[h : h + 1, :], 0.0))
                left.append((e * scores).astype(BF))
            held = state[:, lanes]
            held_high, held_low = _halves(held)
            y = jnp.dot(jnp.concatenate(left, axis=1), jnp.concatenate(_split(lo, u.astype(BF)), axis=0),
                        preferred_element_type=F32)
            outer = jnp.dot(c_wide, jnp.concatenate([held_high, held_high, held_low], axis=0),
                            preferred_element_type=F32)
            y = y + outer * wide[2 * CHUNK :, lanes] + lane_ref[0:1, lanes] * x_act
            y_ref[span, lanes] = y
            uw = (u * wide[CHUNK : 2 * CHUNK, lanes]).astype(BF)
            factor = wide[3 * CHUNK - 1 : 3 * CHUNK, lanes]
            state[:, lanes] = held * factor + jnp.dot(b_t, uw, preferred_element_type=F32)
            z = p_ref[span, lanes]
            product = y * (z * _sigmoid(z))
            squares = squares + product * product
            inner = inner + dg_ref[span, lanes].astype(F32) * lane_ref[1:2, lanes] * product
        row_sq = lax.dot_general(ones, squares, (((1,), (1,)), ((), ())),
                                 precision=lax.Precision.HIGHEST, preferred_element_type=F32)
        row_in = lax.dot_general(ones, inner, (((1,), (1,)), ((), ())),
                                 precision=lax.Precision.HIGHEST, preferred_element_type=F32)
        at = step * (tokens // CHUNK) + sub
        sums[me, pl.ds(at, 1), :] = row_sq[0:1, :]
        sums[me, pl.ds(half + at, 1), :] = row_in[0:1, :]

    @pl.when(step == pl.num_programs(0) - 1)
    def _():
        copies = [_remote(sums.at[me], sums.at[me], sum_sem.at[0, i], sum_sem.at[1, i], peer)
                  for i, peer in enumerate(tensor_peers)]
        for copy in copies:
            copy.start()
        for copy in copies:
            copy.wait_recv()
        s_ref[...] = (sums[0] + sums[1]) + (sums[2] + sums[3])
        for copy in copies:
            copy.wait_send()


def backward_kernel(width, outer_n, p_ref, prev_ref, y_ref, dy_ref, h_ref,
                    convx_ref, convbc_ref, head_ref, lane_ref, partial, grads, resid,
                    dp_ref, gx_ref, gbc_ref, gh_ref, block_sum, owned,
                    grad_state, carry_hg, xbuf, bcbuf, after_x, after_bc, spread, wide, *comm):
    tokens = p_ref.shape[0]
    pairs = width // LANES
    step = pl.program_id(0)
    is_first_block = step == pl.num_programs(0) - 1
    length = partial.shape[0]
    reduction = _Reduction(outer_n, partial, grads, resid, block_sum, owned, *comm)

    @pl.when(step == 0)
    def _():
        reduction.begin()

    for at, piece in reduction.plan(length // tokens):
        @pl.when(step == at)
        def _(piece=piece):
            piece()

    @pl.when(step == 0)
    def _():
        grad_state[...] = jnp.zeros_like(grad_state)
        carry_hg[...] = jnp.zeros_like(carry_hg)
        after_x[...] = jnp.zeros_like(after_x)
        after_bc[...] = jnp.zeros_like(after_bc)
        _fill_spread(spread, LANES // 2)
        gx_ref[...] = jnp.zeros_like(gx_ref)
        gbc_ref[...] = jnp.zeros_like(gbc_ref)
        gh_ref[...] = jnp.zeros_like(gh_ref)

    keep = jnp.where(is_first_block, 0.0, 1.0)
    xbuf[0:8, :] = prev_ref[:, width : 2 * width] * keep
    bcbuf[0:8, :] = prev_ref[:, 2 * width : 2 * width + 2 * LANES] * keep
    xbuf[8 : 8 + tokens, :] = p_ref[:, width : 2 * width]
    bcbuf[8 : 8 + tokens, :] = p_ref[:, 2 * width : 2 * width + 2 * LANES]
    rows = lax.broadcasted_iota(jnp.int32, (CHUNK, CHUNK), 0)
    cols = lax.broadcasted_iota(jnp.int32, (CHUNK, CHUNK), 1)
    lo = cols < LANES // 2
    head = head_ref[...]
    for sub in reversed(range(tokens // CHUNK)):
        base = sub * CHUNK
        span = slice(base, base + CHUNK)
        vbc, shifted_bc = _conv(bcbuf, base, slice(0, 2 * LANES), convbc_ref[...], CHUNK)
        sbc = _sigmoid(vbc)
        bc = vbc * sbc
        b_in, c_out = bc[:, :LANES], bc[:, LANES:]
        b_half, c_half = b_in.astype(BF), c_out.astype(BF)
        t, delta, rate, cum = _times(p_ref[span, 2 * width + 2 * LANES :], head, rows, cols)
        cum_t = cum.T
        causal_t = cols >= rows
        scores_t = jnp.where(causal_t, _dot_three(b_in, c_out), 0.0)
        last = cum[CHUNK - 1 : CHUNK, :]
        tail = jnp.exp2(last - cum)
        grow = jnp.exp2(cum)
        _widen(wide, delta, tail, grow, spread)
        c_t = c_out.T.astype(BF)
        d_scores = jnp.zeros((CHUNK, CHUNK), F32)
        d_b = jnp.zeros((CHUNK, LANES), F32)
        d_c = jnp.zeros((CHUNK, LANES), F32)
        per_head = jnp.zeros((CHUNK, LANES), F32)
        hg_heads = jnp.zeros((8, LANES), F32)
        for q in range(pairs):
            lanes = slice(q * LANES, (q + 1) * LANES)
            step_wide = wide[0:CHUNK, lanes]
            skip = lane_ref[0:1, lanes]
            v, shifted = _conv(xbuf, base, lanes, convx_ref[:, lanes], CHUNK)
            sv = _sigmoid(v)
            x_act = v * sv
            u = x_act * step_wide
            u_half = u.astype(BF)
            y = y_ref[span, lanes]
            dy_half = dy_ref[span, lanes]
            dy = dy_half.astype(F32)
            dy_block = jnp.concatenate(_split(lo, dy_half), axis=0)
            d_m = _dot_last(u_half, dy_block)
            left, left_b = [], []
            for a in (0, 1):
                h = 2 * q + a
                e = jnp.exp2(jnp.minimum(cum_t[h : h + 1, :] - cum[:, h : h + 1], 0.0))
                left.append((e * scores_t).astype(BF))
                d_scores = d_scores + e * d_m[:, a * CHUNK : (a + 1) * CHUNK]
                left_b.append((b_in * tail[:, h : h + 1]).astype(BF))
            g_held = grad_state[:, lanes]
            g_half, g_low = _halves(g_held)
            h_held = h_ref[sub, :, lanes]
            h_half, h_low = _halves(h_held)
            right = jnp.concatenate([dy_block] + _split(lo, g_half), axis=0)
            du = jnp.dot(jnp.concatenate(left + left_b, axis=1), right, preferred_element_type=F32)
            dx = du * step_wide + skip * dy
            dv = dx * (sv * (1.0 + v * (1.0 - sv)))
            d_in = _conv_back(dv, after_x[:, lanes], convx_ref[:, lanes])
            after_x[:, lanes] = dv[0:8, :]
            dp_ref[span, lanes] = d_in.astype(BF)
            for k in range(TAPS):
                gx_ref[k, :, lanes] += _rows_sum(dv * shifted[k])
            gx_ref[4, :, lanes] += _rows_sum(dv)
            gx_ref[5, :, lanes] += _rows_sum(dy * x_act)
            edy = (dy * wide[2 * CHUNK :, lanes]).astype(BF)
            uw = (u * wide[CHUNK : 2 * CHUNK, lanes]).astype(BF)
            d_c = d_c + _dot_last(jnp.concatenate([edy, edy], axis=1), jnp.concatenate([h_half, h_low], axis=1))
            d_b = d_b + _dot_last(jnp.concatenate([uw, uw], axis=1), jnp.concatenate([g_half, g_low], axis=1))
            g_new = g_held * wide[3 * CHUNK - 1 : 3 * CHUNK, lanes] + jnp.dot(
                c_t, edy, preferred_element_type=F32)
            grad_state[:, lanes] = g_new
            r1 = x_act * du
            r2 = dy * (y - skip * x_act)
            sel1 = (cols == 2 * q + (rows >= LANES // 2).astype(jnp.int32)).astype(BF)
            sel2 = (cols == LANES // 2 + 2 * q + (rows >= LANES // 2).astype(jnp.int32)).astype(BF)
            r1h = r1.astype(BF)
            r1l = (r1 - r1h.astype(F32)).astype(BF)
            r2h = r2.astype(BF)
            r2l = (r2 - r2h.astype(F32)).astype(BF)
            per_head = per_head + jnp.dot(
                jnp.concatenate([r1h, r1l, r2h, r2l], axis=1),
                jnp.concatenate([sel1, sel1, sel2, sel2], axis=0), preferred_element_type=F32)
            hg_heads = hg_heads + _dot_exact(carry_hg[:, lanes], sel1.astype(F32))
            carry_hg[:, lanes] = _rows_sum(g_new * h_held)
        d_scores = jnp.where(causal_t, d_scores, 0.0)
        ds_half = d_scores.astype(BF)
        d_b = d_b + jnp.dot(ds_half, c_half, preferred_element_type=F32)
        d_c = d_c + jnp.dot(d_scores.T.astype(BF), b_half, preferred_element_type=F32)
        dvb = jnp.concatenate([d_b, d_c], axis=1) * (sbc * (1.0 + vbc * (1.0 - sbc)))
        d_bc = _conv_back(dvb, after_bc[...], convbc_ref[...])
        after_bc[...] = dvb[0:8, :]
        dp_ref[span, width : width + 2 * LANES] = d_bc.astype(BF)
        for k in range(TAPS):
            gbc_ref[k] += _rows_sum(dvb * shifted_bc[k])
        gbc_ref[4] += _rows_sum(dvb)
        direct = per_head
        through = pltpu.roll(per_head, LANES // 2, 1)
        d_cum = through - delta * direct
        suffix = _dot_exact((cols >= rows).astype(F32), d_cum)
        d_log = suffix + jnp.sum(hg_heads, axis=0, keepdims=True)
        valid = cols < 2 * pairs
        d_delta = direct + rate * d_log
        d_dt = jnp.where(valid, d_delta * _sigmoid(t), 0.0)
        dp_ref[span, width + 2 * LANES :] = d_dt.astype(BF)
        gh_ref[0] += _rows_sum(d_dt)
        gh_ref[1] += _rows_sum(jnp.where(valid, delta * d_log, 0.0)) * rate

    @pl.when(is_first_block)
    def _():
        reduction.end()


def ssd_forward(proj, dg, convx, convbc, head, lane, tokens=256):
    length, total = proj.shape
    width = convx.shape[1]
    subs = tokens // CHUNK
    whole = lambda a: pl.BlockSpec(a.shape, lambda i: (0,) * a.ndim)
    return pl.pallas_call(
        functools.partial(forward_kernel, width),
        grid=(length // tokens,),
        in_specs=[pl.BlockSpec((tokens, total), lambda i: (i, 0)),
                  pl.BlockSpec((tokens, width), lambda i: (i, 0)),
                  whole(convx), whole(convbc), whole(head), whole(lane)],
        out_specs=[pl.BlockSpec((tokens, width), lambda i: (i, 0)),
                   pl.BlockSpec((subs, LANES, width), lambda i: (i, 0, 0)),
                   pl.BlockSpec((2 * length // CHUNK, CHUNK), lambda i: (0, 0))],
        out_shape=[jax.ShapeDtypeStruct((length, width), F32),
                   jax.ShapeDtypeStruct((length // CHUNK, LANES, width), F32),
                   jax.ShapeDtypeStruct((2 * length // CHUNK, CHUNK), F32)],
        scratch_shapes=[pltpu.VMEM((LANES, width), F32),
                        pltpu.VMEM((tokens + 8, width), F32),
                        pltpu.VMEM((tokens + 8, 2 * LANES), F32),
                        pltpu.VMEM((2 * LANES, width), BF),
                        pltpu.VMEM((3 * CHUNK, width), F32),
                        pltpu.VMEM((4, 2 * length // CHUNK, CHUNK), F32),
                        pltpu.SemaphoreType.DMA((2, 3))],
        compiler_params=pltpu.CompilerParams(collective_id=2, has_side_effects=True),
        cost_estimate=pl.CostEstimate(flops=4 * 10**9, bytes_accessed=30 * 2**20, transcendentals=10**7),
        name="scan_forward",
    )(proj, dg, convx, convbc, head, lane)


def ssd_backward(proj, y, dy, states, convx, convbc, head, lane, partial, grads, resid, tokens=256):
    length, total = proj.shape
    width = convx.shape[1]
    subs = tokens // CHUNK
    n = length // tokens
    dp, tp = lax.axis_size("dp"), lax.axis_size("tensor")
    whole = lambda a: pl.BlockSpec(a.shape, lambda i: (0,) * a.ndim)
    rev = lambda i: (n - 1 - i, 0)
    own = lambda shape: pl.BlockSpec(shape, lambda i: (0, 0))
    hbm = pl.BlockSpec(memory_space=pl.ANY)
    block_shape = (length // tp, partial.shape[1])
    owned_shape = (grads.shape[0] // dp, grads.shape[1])
    return pl.pallas_call(
        functools.partial(backward_kernel, width, dp // 2),
        grid=(n,),
        in_specs=[pl.BlockSpec((tokens, total), rev),
                  pl.BlockSpec((8, total), lambda i: (jnp.maximum((n - 1 - i) * (tokens // 8) - 1, 0), 0)),
                  pl.BlockSpec((tokens, width), rev),
                  pl.BlockSpec((tokens, width), rev),
                  pl.BlockSpec((subs, LANES, width), lambda i: (n - 1 - i, 0, 0)),
                  whole(convx), whole(convbc), whole(head), whole(lane), hbm, hbm, hbm],
        out_specs=[pl.BlockSpec((tokens, total - width), rev),
                   pl.BlockSpec((6, 8, width), lambda i: (0, 0, 0)),
                   pl.BlockSpec((5, 8, 2 * LANES), lambda i: (0, 0, 0)),
                   pl.BlockSpec((2, 8, LANES), lambda i: (0, 0, 0)),
                   own(block_shape), own(owned_shape)],
        out_shape=[jax.ShapeDtypeStruct((length, total - width), BF),
                   jax.ShapeDtypeStruct((6, 8, width), F32),
                   jax.ShapeDtypeStruct((5, 8, 2 * LANES), F32),
                   jax.ShapeDtypeStruct((2, 8, LANES), F32),
                   jax.ShapeDtypeStruct(block_shape, F32),
                   jax.ShapeDtypeStruct(owned_shape, F32)],
        scratch_shapes=[pltpu.VMEM((LANES, width), F32),
                        pltpu.VMEM((8, width), F32),
                        pltpu.VMEM((tokens + 8, width), F32),
                        pltpu.VMEM((tokens + 8, 2 * LANES), F32),
                        pltpu.VMEM((8, width), F32),
                        pltpu.VMEM((8, 2 * LANES), F32),
                        pltpu.VMEM((2 * LANES, width), BF),
                        pltpu.VMEM((3 * CHUNK, width), F32)] + reduction_scratch(dp // 2, block_shape, owned_shape),
        compiler_params=pltpu.CompilerParams(collective_id=3, has_side_effects=True, vmem_limit_bytes=62 * 2**20),
        cost_estimate=pl.CostEstimate(flops=12 * 10**9, bytes_accessed=50 * 2**20, transcendentals=10**7),
        name="scan_backward",
    )(proj, proj, y, dy, states, convx, convbc, head, lane, partial, grads, resid)


def middle_kernel(width, inner_channels, z_ref, y_ref, dg_ref, s_ref, lane_ref, normed, cot, out_t,
                  dy_ref, dz_ref, out_ref, grads_ref, gg_ref, gated, acc_z, acc_o):
    tokens = z_ref.shape[0]
    step = pl.program_id(0)
    half = s_ref.shape[0] // 2

    @pl.when(step == 0)
    def _():
        gg_ref[...] = jnp.zeros_like(gg_ref)
        acc_z[...] = jnp.zeros_like(acc_z)
        acc_o[...] = jnp.zeros_like(acc_o)

    for sub in range(tokens // CHUNK):
        span = slice(sub * CHUNK, (sub + 1) * CHUNK)
        at = step * (tokens // CHUNK) + sub
        wide = lambda row: jnp.broadcast_to(row, (8, CHUNK)).T[:, 0:1]
        squares, dots = wide(s_ref[pl.ds(at, 1), :]), wide(s_ref[pl.ds(half + at, 1), :])
        inv = lax.rsqrt(squares / inner_channels + EPSILON)
        mean = inv * dots / inner_channels
        for q in range(width // LANES):
            lanes = slice(q * LANES, (q + 1) * LANES)
            gain = lane_ref[1:2, lanes]
            y, z, dg = y_ref[span, lanes], z_ref[span, lanes], dg_ref[span, lanes]
            sz = _sigmoid(z)
            act = z * sz
            quot = y * act * inv
            gg_ref[:, lanes] += _rows_sum(dg * quot)
            gated[span, lanes] = (quot * gain).astype(BF)
            d_prod = inv * (dg * gain - quot * mean)
            dy_ref[span, lanes] = (d_prod * act).astype(BF)
            dz_ref[span, lanes] = (d_prod * y * sz * (1.0 + z * (1.0 - sz))).astype(BF)
    out_ref[...] = _dot_last(gated[...], out_t[...]).astype(BF)
    first = lambda a, b: lax.dot_general(a, b, (((0,), (0,)), ((), ())), preferred_element_type=F32)
    acc_z[...] += first(normed[...], dz_ref[...])
    acc_o[...] += first(cot[...], gated[...])

    @pl.when(step == pl.num_programs(0) - 1)
    def _():
        grads_ref[:, :width] = acc_z[...].astype(BF)
        grads_ref[:, width:] = acc_o[...].astype(BF)


def middle(proj, y, dg, sums, lane, normed, cot, out_t, inner_channels, tokens=512):
    length, model = normed.shape
    width = y.shape[1]
    at = lambda cols: pl.BlockSpec((tokens, cols), lambda i: (i, 0))
    once = lambda shape: pl.BlockSpec(shape, lambda i: (0, 0), pipeline_mode=pl.Buffered(1))
    return pl.pallas_call(
        functools.partial(middle_kernel, width, inner_channels),
        grid=(length // tokens,),
        in_specs=[at(width), at(width), at(width), once(sums.shape), once(lane.shape), at(model), at(model),
                  once(out_t.shape)],
        out_specs=[at(width), at(width), at(model), once((model, 2 * width)), once((8, width))],
        out_shape=[jax.ShapeDtypeStruct((length, width), BF),
                   jax.ShapeDtypeStruct((length, width), BF),
                   jax.ShapeDtypeStruct((length, model), BF),
                   jax.ShapeDtypeStruct((model, 2 * width), BF),
                   jax.ShapeDtypeStruct((8, width), F32)],
        scratch_shapes=[pltpu.VMEM((tokens, width), BF),
                        pltpu.VMEM((model, width), F32),
                        pltpu.VMEM((model, width), F32)],
        cost_estimate=pl.CostEstimate(flops=15 * 10**9, bytes_accessed=50 * 2**20, transcendentals=10**6),
        name="middle",
    )(proj, y, dg, sums, lane, normed, cot, out_t)


def pad_rows(a, rows):
    return jnp.pad(a, ((0, rows - a.shape[0]), (0, 0)))


def pack_params(conv_x_weight, conv_x_bias, conv_bc_weight, conv_bc_bias, dt_bias, a_log, skip_gain, gate_gain):
    width = conv_x_weight.shape[1]
    convx = pad_rows(jnp.concatenate([conv_x_weight, conv_x_bias[None]], 0), 8)
    convbc = pad_rows(jnp.concatenate([conv_bc_weight, conv_bc_bias[None]], 0), 8)
    heads = dt_bias.shape[0]
    head = jnp.pad(jnp.stack([dt_bias, a_log]), ((0, 6), (0, LANES - heads)))
    lane = pad_rows(jnp.stack([jnp.repeat(skip_gain, width // heads), gate_gain]), 8)
    return convx, convbc, head, lane
def gather_kernel(outer_n, heads, small, wzx, wdt, wbc, wout, resid_in, cot_in,
                  small_all, inv_out, normed_out, cot_out, weight_out, wout_out, proj, d_gated,
                  normed, cot, weight, w_out, resid, cot_f, stage, stage_g,
                  small_t, small_d, bc_slots, dt_slots,
                  small_sem_t, small_sem_d, bc_sem_t, bc_sem_d, dt_sem, norm_sem, cot_sem, zx_sem, wo_sem,
                  local_sem, stage_sem, stage_g_sem):
    z, y, x, c = _place()
    me = _peer(z, y, x, c)
    t = x * 2 + c
    d = z * 2 + y
    block, zx_cols = wzx.shape
    bc_cols = wbc.shape[1]
    bc_rows = wbc.shape[0]
    wparts = _parts(block)
    bsize = block // wparts
    own_rows, model = resid.shape
    size = own_rows // PARTS
    length = normed.shape[0]
    tile = stage.shape[1]
    loads = [pltpu.make_async_copy(resid_in, resid, local_sem.at[0]),
             pltpu.make_async_copy(cot_in, cot_f, local_sem.at[1])]
    for copy in loads:
        copy.start()
    _greet(outer_n)
    dp_peers = [(k, j) for k in range(outer_n) for j in (0, 1) if k or j]
    tensor_peers = [(k, j) for k in (0, 1) for j in (0, 1) if k or j]
    at_dp = lambda k, j: _peer((z + k) % outer_n, (y + j) % 2, x, c)
    at_tensor = lambda k, j: _peer(z, y, (x + k) % 2, (c + j) % 2)

    small_first = [_remote(small, small_d.at[i], small_sem_d.at[0, i], small_sem_d.at[1, i], at_dp(k, j))
                   for i, (k, j) in enumerate(dp_peers)]
    bc_first = [_remote(wbc, bc_slots.at[t, d], bc_sem_d.at[0, i], bc_sem_d.at[1, i], at_dp(k, j))
                for i, (k, j) in enumerate(dp_peers)]
    dt_first = [_remote(wdt, dt_slots.at[d], dt_sem.at[0, i], dt_sem.at[1, i], at_dp(k, j))
                for i, (k, j) in enumerate(dp_peers)]
    for copy in small_first + bc_first + dt_first:
        copy.start()

    h, low = z // 2, z % 2
    pairs = outer_n // 2

    def view_of(dst, cols, r, m, inner, part):
        outer = lax.rem(h + r, pairs) * 2 + (low if m else 1 - low)
        return dst.at[_rows((outer * 2 + inner) * block + part * bsize, bsize), cols]

    def piece_of(src, part):
        return src.at[pl.ds(part * bsize, bsize), :]

    def cross(src, dst, cols, sem, k, part):
        return _remote(piece_of(src, part), view_of(dst, cols, 0, 1, y, part), sem.at[0, k * 2 + 1, part],
                       sem.at[1, (pairs - k) * 2 + 1, part], _peer(lax.rem(h + k, pairs) * 2 + low, y, x, c))

    def pair(src, dst, cols, sem, r, part):
        view = view_of(dst, cols, r, 1, y, part)
        return _remote(view if r else piece_of(src, part), view, sem.at[0, r * 2, part], sem.at[1, r * 2, part],
                       _peer(h * 2 + 1 - low, y, x, c))

    def onward(src, dst, cols, sem, r, m, part):
        view = view_of(dst, cols, r, m, y, part)
        slot = r * 2 + m
        return _remote(piece_of(src, part) if slot == 1 else view, view, sem.at[2, slot, part], sem.at[3, slot, part],
                       _peer(z, 1 - y, x, c))

    def arrived(dst, cols, sem, r, m, part):
        view = view_of(dst, cols, r, m, y, part)
        _remote(view, view, sem.at[0, r * 2 + m, part], sem.at[1, r * 2 + m, part], me).wait_recv()

    def send_out(src, dst, cols, sem):
        for part in range(wparts):
            for k in range(1, pairs):
                cross(src, dst, cols, sem, k, part).start()
            pair(src, dst, cols, sem, 0, part).start()
            onward(src, dst, cols, sem, 0, 1, part).start()

    def pass_first(src, dst, cols, sem, part):
        for r in range(1, pairs):
            arrived(dst, cols, sem, r, 1, part)
            pair(src, dst, cols, sem, r, part).start()
            onward(src, dst, cols, sem, r, 1, part).start()
        arrived(dst, cols, sem, 0, 0, part)
        onward(src, dst, cols, sem, 0, 0, part).start()

    def pass_second(src, dst, cols, sem, part):
        for r in range(1, pairs):
            arrived(dst, cols, sem, r, 0, part)
            onward(src, dst, cols, sem, r, 0, part).start()

    def finish(src, dst, cols, sem):
        for part in range(wparts):
            for r in range(pairs):
                for m in (0, 1):
                    view = view_of(dst, cols, r, m, 1 - y, part)
                    _remote(view, view, sem.at[2, r * 2 + m, part], sem.at[3, r * 2 + m, part], me).wait_recv()

    def finish_sends(src, dst, cols, sem):
        for part in range(wparts):
            for r in range(pairs):
                if r:
                    cross(src, dst, cols, sem, r, part).wait_send()
                pair(src, dst, cols, sem, r, part).wait_send()
                for m in (0, 1):
                    onward(src, dst, cols, sem, r, m, part).wait_send()

    zx = (wzx, weight, pl.ds(0, zx_cols), zx_sem)
    wo = (wout, w_out, pl.ds(0, wout.shape[1]), wo_sem)
    send_out(*zx)
    mine = _rows(d * block, block)
    place = [pltpu.make_async_copy(wzx, weight.at[mine, pl.ds(0, zx_cols)], local_sem.at[2]),
             pltpu.make_async_copy(wout, w_out.at[mine, :], local_sem.at[3])]
    for copy in place:
        copy.start()
    bc_slots[t, d] = wbc[...]
    dt_slots[d] = wdt[...]
    loads[0].wait()
    values = resid[...]
    inv = lax.rsqrt(jnp.mean(values * values, axis=-1, keepdims=True) + EPSILON)
    inv_out[...] = jnp.broadcast_to(inv, inv_out.shape)

    for copy in small_first + bc_first:
        copy.wait_recv()
    total = small[...]
    for i in range(len(dp_peers)):
        total = total + small_d[i]
    small_t[3] = total
    small_second = [_remote(small_t.at[3], small_t.at[i], small_sem_t.at[0, i], small_sem_t.at[1, i], at_tensor(k, j))
                    for i, (k, j) in enumerate(tensor_peers)]
    bc_second = [_remote(bc_slots.at[t], bc_slots.at[t], bc_sem_t.at[0, i], bc_sem_t.at[1, i], at_tensor(k, j))
                 for i, (k, j) in enumerate(tensor_peers)]
    for copy in small_second:
        copy.start()
    send_out(*wo)
    for copy in small_second:
        copy.wait_recv()
    total = small_t[3]
    for i in range(3):
        total = total + small_t[i]
    small_all[...] = total
    own_at = _rows(t * own_rows, own_rows)
    for j in range(model // LANES):
        lanes = slice(j * LANES, (j + 1) * LANES)
        normed[own_at, lanes] = (resid[:, lanes] * inv * total[j : j + 1, :]).astype(BF)

    def token_rows(far, near, part):
        return _rows((far * 2 + near) * own_rows + part * size, size)

    def token_copy(buf, sem, which, part):
        far = 1 - x if which == 2 else x
        view = buf.at[token_rows(far, c, part), :]
        peer = _peer(z, y, 1 - x, c) if which == 0 else _peer(z, y, x, 1 - c)
        return _remote(view, view, sem.at[0, which, part], sem.at[1, which, part], peer)

    def send_tokens(buf, sem):
        for part in range(PARTS):
            token_copy(buf, sem, 0, part).start()
            token_copy(buf, sem, 1, part).start()

    def pass_tokens(buf, sem, part):
        token_copy(buf, sem, 0, part).wait_recv()
        token_copy(buf, sem, 2, part).start()

    def finish_tokens(buf, sem):
        for part in range(PARTS):
            token_copy(buf, sem, 1, part).wait_recv()
            token_copy(buf, sem, 2, part).wait_recv()

    send_tokens(normed, norm_sem)
    for copy in bc_second:
        copy.start()
    loads[1].wait()
    cot[own_at, :] = cot_f[...].astype(BF)
    send_tokens(cot, cot_sem)
    for copy in dt_first:
        copy.wait_recv()
    for copy in place:
        copy.wait()
    for i in range(outer_n * 2):
        columns = dt_slots[i].astype(F32)
        columns = jnp.concatenate([columns, jnp.zeros((LANES - columns.shape[0], columns.shape[1]), F32)], axis=0)
        weight[i * block : (i + 1) * block, zx_cols + bc_cols :] = columns.T[:block, :].astype(BF)
    for part in range(max(PARTS, wparts)):
        if part < wparts:
            pass_first(*zx, part)
        if 1 <= part < wparts:
            pass_second(*zx, part - 1)
        if part < PARTS:
            pass_tokens(normed, norm_sem, part)
    pass_second(*zx, wparts - 1)
    for copy in bc_second:
        copy.wait_recv()
    for i in range(outer_n * 2):
        for j in range(4):
            first = i * block + j * bc_rows
            weight[first : first + bc_rows, zx_cols : zx_cols + bc_cols] = bc_slots[j, i]
    finish_tokens(normed, norm_sem)
    finish(*zx)
    save = [pltpu.make_async_copy(normed, normed_out, local_sem.at[4]),
            pltpu.make_async_copy(weight, weight_out, local_sem.at[5])]
    for copy in save:
        copy.start()

    steps = length // tile

    def store(ref, buf, sem, i):
        slot = lax.rem(i, 2)
        return pltpu.make_async_copy(buf.at[slot], ref.at[pl.ds(pl.multiple_of(i * tile, tile), tile), :], sem.at[slot])

    @pl.loop(0, steps)
    def _(i):
        @pl.when(i >= 2)
        def _():
            store(proj, stage, stage_sem, i - 2).wait()

        rows = pl.ds(pl.multiple_of(i * tile, tile), tile)
        stage[lax.rem(i, 2)] = jnp.dot(normed[rows, :], weight[...], preferred_element_type=F32)
        store(proj, stage, stage_sem, i).start()

        @pl.when(i < wparts)
        def _():
            pass_first(*wo, i)

        @pl.when((i >= 1) & (i < wparts + 1))
        def _():
            pass_second(*wo, i - 1)

        @pl.when(i < PARTS)
        def _():
            pass_tokens(cot, cot_sem, i)

    for i in range(steps, wparts):
        pass_first(*wo, i)
    for i in range(steps - 1, wparts):
        pass_second(*wo, i)
    for i in range(steps, PARTS):
        pass_tokens(cot, cot_sem, i)
    finish_tokens(cot, cot_sem)
    finish(*wo)
    save_late = [pltpu.make_async_copy(cot, cot_out, local_sem.at[6]),
                 pltpu.make_async_copy(w_out, wout_out, local_sem.at[7])]
    for copy in save_late:
        copy.start()

    @pl.loop(0, steps)
    def _(i):
        @pl.when(i >= 2)
        def _():
            store(d_gated, stage_g, stage_g_sem, i - 2).wait()

        rows = pl.ds(pl.multiple_of(i * tile, tile), tile)
        stage_g[lax.rem(i, 2)] = jnp.dot(cot[rows, :], w_out[...], preferred_element_type=F32)
        store(d_gated, stage_g, stage_g_sem, i).start()

    for i in range(max(steps - 2, 0), steps):
        store(proj, stage, stage_sem, i).wait()
        store(d_gated, stage_g, stage_g_sem, i).wait()
    finish_sends(*zx)
    finish_sends(*wo)
    for part in range(PARTS):
        for which in range(3):
            token_copy(normed, norm_sem, which, part).wait_send()
            token_copy(cot, cot_sem, which, part).wait_send()
    for copy in small_first + bc_first + dt_first + small_second + bc_second:
        copy.wait_send()
    for copy in save + save_late:
        copy.wait()


def gather_all(small, resid, cot, wzx, wdt, wbc, wout, tile=256):
    dp, tp = lax.axis_size("dp"), lax.axis_size("tensor")
    outer_n = dp // 2
    block, zx_cols = wzx.shape
    total = zx_cols + wbc.shape[1] + LANES
    width = wout.shape[1]
    heads = wdt.shape[1]
    length, model = resid.shape[0] * tp, resid.shape[1]
    wdt = jnp.pad(wdt.T, ((0, -heads % 16), (0, -block % LANES)))
    wparts = _parts(block)
    vm = pl.BlockSpec(memory_space=pltpu.VMEM)
    hbm = pl.BlockSpec(memory_space=pl.ANY)
    dma = pltpu.SemaphoreType.DMA
    shape = jax.ShapeDtypeStruct
    return pl.pallas_call(
        functools.partial(gather_kernel, outer_n, heads),
        in_specs=[vm] * 5 + [hbm] * 2,
        out_specs=[vm] * 2 + [hbm] * 6,
        out_shape=[shape(small.shape, F32), shape((resid.shape[0], LANES), F32), shape((length, model), BF), shape((length, model), BF),
                   shape((model, total), BF), shape((model, width), BF),
                   shape((length, total), F32), shape((length, width), F32)],
        scratch_shapes=[pltpu.VMEM((length, model), BF), pltpu.VMEM((length, model), BF),
                        pltpu.VMEM((model, total), BF), pltpu.VMEM((model, width), BF),
                        pltpu.VMEM(resid.shape, F32), pltpu.VMEM(resid.shape, F32),
                        pltpu.VMEM((2, tile, total), F32), pltpu.VMEM((2, tile, width), F32),
                        pltpu.VMEM((4,) + small.shape, F32), pltpu.VMEM((dp - 1,) + small.shape, F32),
                        pltpu.VMEM((4, dp) + wbc.shape, BF), pltpu.VMEM((dp,) + wdt.shape, BF),
                        dma((2, 3)), dma((2, dp - 1)), dma((2, 3)), dma((2, dp - 1)), dma((2, dp - 1)),
                        dma((2, 3, PARTS)), dma((2, 3, PARTS)), dma((4, outer_n, wparts)), dma((4, outer_n, wparts)),
                        dma((8,)), dma((2,)), dma((2,))],
        compiler_params=pltpu.CompilerParams(collective_id=0, has_side_effects=True, vmem_limit_bytes=62 * 2**20),
        cost_estimate=pl.CostEstimate(flops=17 * 10**9, bytes_accessed=60 * 2**20, transcendentals=0),
        name="gather_all",
    )(small, wzx, wdt, wbc, wout, resid, cot)


def final_kernel(outer_n, both_rows, gain_rows, dz_in, rest_in, weight_in, normed_in, small, gain,
                 d_local, owned, small_out, bc_out,
                 dz, rest, weight, normed, g_all, tok, near_buf, far_src, far_buf,
                 small_d, small_t, gain_d, gain_t, gain_acc, bc_src, bc_buf,
                 load_sem, near_sem, far_sem, small_sem_d, small_sem_t, gain_sem_d, gain_sem_t, bc_sem, *row_sums):
    z, y, x, c = _place()
    t = x * 2 + c
    own_rows, model = d_local.shape
    block, cols = owned.shape
    width = dz.shape[1]
    wparts = _parts(block)
    bsize = block // wparts
    size = own_rows // PARTS
    half = own_rows // 2
    per_group = next(g for g in range(1, outer_n + 1) if (2 * g * block) % LANES == 0)
    groups = outer_n // per_group
    loads = [pltpu.make_async_copy(src, dst, load_sem.at[i]) for i, (src, dst) in enumerate(
        [(rest_in, rest), (normed_in, normed), (dz_in, dz), (weight_in, weight)])]
    for copy in loads:
        copy.start()
    _greet(outer_n)
    dp_peers = [(k, j) for k in range(outer_n) for j in (0, 1) if k or j]
    tensor_peers = [(k, j) for k in (0, 1) for j in (0, 1) if k or j]

    def dp_copies(src, dst, sem):
        return [_remote(src, dst.at[k * 2 + j], sem.at[0, i], sem.at[1, i],
                        _peer((z + k) % outer_n, (y + j) % 2, x, c)) for i, (k, j) in enumerate(dp_peers)]

    def tensor_copies(src, dst, sem):
        return [_remote(src, dst.at[k * 2 + j], sem.at[0, i], sem.at[1, i],
                        _peer(z, y, (x + k) % 2, (c + j) % 2)) for i, (k, j) in enumerate(tensor_peers)]

    def dp_total(buf):
        total = None
        for zz in range(outer_n):
            for yy in (0, 1):
                term = buf[lax.rem(z - zz + outer_n, outer_n) * 2 + lax.rem(y - yy + 2, 2)]
                total = term if total is None else total + term
        return total

    def near_copy(i, part):
        at = pl.ds(part * size, size)
        return _remote(tok.at[2 * i, at, :], near_buf.at[i, at, :], near_sem.at[0, i, part], near_sem.at[1, i, part],
                       _peer(z, y, x, 1 - c))

    def far_copy(part):
        at = pl.ds(part * size, size)
        return _remote(far_src.at[at, :], far_buf.at[at, :], far_sem.at[0, part], far_sem.at[1, part],
                       _peer(z, y, 1 - x, c))

    sums = _RowSums(
        outer_n, block,
        lambda slot, outer, inner, part: g_all.at[outer, inner, pl.ds(part * bsize, bsize), :],
        lambda slot, outer, part: g_all[outer, y, pl.ds(part * bsize, bsize), :].astype(F32),
        owned, *row_sums)

    def token_product(i, part):
        a, b = i // 2, i % 2
        far, near = (1 - x) * (1 - a) + x * a, (1 - c) * (1 - b) + c * b
        rows = pl.ds(pl.multiple_of((far * 2 + near) * own_rows + part * half, LANES), half)
        value = _dot_last(dz[rows, :], weight[:, :width]) + _dot_last(rest[rows, :], weight[:, width:])
        gain_acc[...] += _rows_sum(value * normed[rows, :].astype(F32))
        at = pl.ds(pl.multiple_of(part * half, LANES), half)

        @pl.when(i < 3)
        def _():
            tok[i, at, :] = value.astype(BF)

        @pl.when(i == 3)
        def _():
            d_local[at, :] = value

    def group(i):
        if per_group == 1:
            r = lax.rem(1 + i // 2, sums.pairs)
            grp = lax.rem(sums.h + r, sums.pairs) * 2 + (1 - sums.l) * (1 - i % 2) + sums.l * (i % 2)
        else:
            grp = lax.rem(z // per_group + 1 + i, groups)
        at = pl.ds(pl.multiple_of(grp * (2 * per_group * block), LANES), 2 * per_group * block)
        value = lax.dot_general(normed[:, at], rest[...], (((0,), (0,)), ((), ())), preferred_element_type=F32)
        for j in range(per_group):
            zz = grp * per_group + j
            for yy in (0, 1):
                first = (2 * j + yy) * block
                g_all[zz, yy] = value[first : first + block, :].astype(BF)
            for part in range(wparts):
                sums.in_copy(sums.slot_of(zz), zz, part).start()

    def token_step(part):
        at = pl.ds(part * size, size)
        near_copy(0, part).wait_recv()
        far_src[at, :] = (tok[1, at, :].astype(F32) + near_buf[0, at, :].astype(F32)).astype(BF)
        far_copy(part).start()

    small_d[0] = small[...]
    first = dp_copies(small, small_d, small_sem_d)
    for copy in first:
        copy.start()
    for copy in loads[:2]:
        copy.wait()
    gain_acc[...] = jnp.zeros_like(gain_acc)
    parts_half = PARTS // 2
    todo = sums.todo()
    cut = lambda eighths: todo[: eighths * len(todo) // 8] if per_group == 1 or eighths == 8 else []
    per_slot = -(-groups // 4)
    second = tensor_copies(small_t.at[0], small_t, small_sem_t)

    def near_start(i, which):
        for part in range(which * parts_half, (which + 1) * parts_half):
            near_copy(i, part).start()

    def far_start(which):
        for part in range(which * parts_half, (which + 1) * parts_half):
            token_step(part)

    def grads_between(low, high):
        for item in cut(high)[len(cut(low)) :]:
            sums.step(*item)

    def small_second():
        for copy in first:
            copy.wait_recv()
        total = dp_total(small_d)
        small_out[...] = total
        small_t[0] = total[:both_rows, :]
        for copy in second:
            copy.start()

    after = {
        0: lambda: near_start(0, 0),
        1: lambda: far_start(0),
        2: lambda: near_start(0, 1),
        3: lambda: (far_start(1), small_second(), grads_between(0, 1)),
        4: lambda: (near_start(1, 0), grads_between(1, 2)),
        5: lambda: grads_between(2, 4),
        6: lambda: (near_start(1, 1), grads_between(4, 5)),
        7: lambda: grads_between(5, 6),
    }

    @pl.loop(0, 8)
    def _(it):
        for r in range(per_slot):
            @pl.when((it % 2 == 0) & (it // 2 * per_slot + r < groups))
            def _():
                group(it // 2 * per_slot + r)

        @pl.when(it == 0)
        def _():
            for copy in loads[2:]:
                copy.wait()

        token_product(it // 4 * 2 + it % 2, it // 2 % 2)
        for step, piece in after.items():
            @pl.when(it == step)
            def _(piece=piece):
                piece()

    for j in range(gain_rows):
        gain_d[0, j : j + 1, :] = jnp.sum(
            gain_acc[:, j * LANES : (j + 1) * LANES], axis=0, keepdims=True) / gain[j : j + 1, :]
    gain_first = dp_copies(gain_d.at[0], gain_d, gain_sem_d)
    for copy in gain_first:
        copy.start()
    gain_second = tensor_copies(gain_t.at[0], gain_t, gain_sem_t)

    def token_finish(part):
        at = pl.ds(part * size, size)
        near_copy(1, part).wait_recv()
        far_copy(part).wait_recv()
        d_local[at, :] = d_local[at, :] + near_buf[1, at, :].astype(F32) + far_buf[at, :].astype(F32)

    grads_between(6, 7)
    for copy in gain_first:
        copy.wait_recv()
    gain_t[0] = dp_total(gain_d)
    for copy in gain_second:
        copy.start()
    for part in range(parts_half):
        token_finish(part)
    grads_between(7, 8)
    for part in range(parts_half, PARTS):
        token_finish(part)
    sums.finish()
    bc_rows = block // 4
    for i in range(4):
        bc_src[i] = owned[i * bc_rows : (i + 1) * bc_rows, width : width + 2 * LANES]
    bc_copies = []
    for i, (k, j) in enumerate(tensor_peers):
        other = lax.rem(x + k, 2) * 2 + lax.rem(c + j, 2)
        bc_copies.append(_remote(bc_src.at[other], bc_buf.at[i], bc_sem.at[0, i], bc_sem.at[1, i],
                                 _peer(z, y, (x + k) % 2, (c + j) % 2)))
    for copy in bc_copies:
        copy.start()
    for copy in second:
        copy.wait_recv()
    small_out[0:both_rows, :] = (small_t[0] + small_t[1]) + (small_t[2] + small_t[3])
    for copy in bc_copies:
        copy.wait_recv()
    bc_out[...] = (bc_src[t] + bc_buf[0]) + (bc_buf[1] + bc_buf[2])
    for copy in gain_second:
        copy.wait_recv()
    gains = (gain_t[0] + gain_t[1]) + (gain_t[2] + gain_t[3])
    small_out[0:gain_rows, :] = gains[:gain_rows, :]
    for part in range(PARTS):
        near_copy(0, part).wait_send()
        near_copy(1, part).wait_send()
        far_copy(part).wait_send()
    sums.wait_sends()
    for copy in first + second + gain_first + gain_second + bc_copies:
        copy.wait_send()


def final_sums(dz, rest, weight, normed, small, gain, both_rows):
    dp, tp = lax.axis_size("dp"), lax.axis_size("tensor")
    outer_n = dp // 2
    own_rows, model = normed.shape[0] // tp, normed.shape[1]
    block, cols = model // dp, rest.shape[1]
    gain_rows = model // LANES
    gain_pad = -(-gain_rows // 8) * 8
    wparts = _parts(block)
    vm = pl.BlockSpec(memory_space=pltpu.VMEM)
    hbm = pl.BlockSpec(memory_space=pl.ANY)
    dma = pltpu.SemaphoreType.DMA
    tokens = (own_rows, model)
    bc = (4, block // 4, 2 * LANES)
    return pl.pallas_call(
        functools.partial(final_kernel, outer_n, both_rows, gain_rows),
        in_specs=[hbm] * 4 + [vm] * 2,
        out_specs=[vm] * 4,
        out_shape=[jax.ShapeDtypeStruct(tokens, F32),
                   jax.ShapeDtypeStruct((block, cols), F32),
                   jax.ShapeDtypeStruct(small.shape, F32),
                   jax.ShapeDtypeStruct(bc[1:], F32)],
        scratch_shapes=[pltpu.VMEM(dz.shape, BF), pltpu.VMEM(rest.shape, BF), pltpu.VMEM(weight.shape, BF),
                        pltpu.VMEM(normed.shape, BF),
                        pltpu.VMEM((outer_n, 2, block, cols), BF),
                        pltpu.VMEM((3,) + tokens, BF), pltpu.VMEM((2,) + tokens, BF),
                        pltpu.VMEM(tokens, BF), pltpu.VMEM(tokens, BF),
                        pltpu.VMEM((dp,) + small.shape, F32), pltpu.VMEM((4, both_rows, LANES), F32),
                        pltpu.VMEM((dp, gain_pad, LANES), F32), pltpu.VMEM((4, gain_pad, LANES), F32),
                        pltpu.VMEM((8, model), F32), pltpu.VMEM(bc, F32), pltpu.VMEM((3,) + bc[1:], F32),
                        dma((4,)), dma((2, 2, PARTS)), dma((2, PARTS)),
                        dma((2, dp - 1)), dma((2, 3)), dma((2, dp - 1)), dma((2, 3)),
                        dma((2, 3))] + row_sums_scratch(outer_n, (block, cols)),
        compiler_params=pltpu.CompilerParams(collective_id=1, has_side_effects=True, vmem_limit_bytes=63 * 2**20),
        cost_estimate=pl.CostEstimate(flops=20 * 10**9, bytes_accessed=40 * 2**20, transcendentals=0),
        name="final_sums",
    )(dz, rest, weight, normed, small, gain)


def _spread(values, index, count):
    size = values.shape[-1]
    full = jnp.zeros(values.shape[:-1] + (size * count,), F32)
    return lax.dynamic_update_slice_in_dim(full, values, index * size, axis=values.ndim - 1)


def _own(values, index, count):
    size = values.shape[-1] // count
    return lax.dynamic_slice_in_dim(values, index * size, size, axis=values.ndim - 1)


def on_device(
    resid_in, norm_gain, proj_zx, proj_dt, proj_bc, conv_x_weight, conv_x_bias, conv_bc_weight,
    conv_bc_bias, dt_bias, a_log, skip_gain, gate_gain, proj_out, cotangent,
):
    dp, tp = lax.axis_size("dp"), lax.axis_size("tensor")
    index = lax.axis_index("dp") * tp + lax.axis_index("tensor")
    count = dp * tp
    model = resid_in.shape[-1]
    width = conv_x_weight.shape[1]
    heads = dt_bias.shape[0]
    inner_channels = width * tp
    states2 = 2 * LANES
    rows = proj_zx.shape[0]
    resid, cot = resid_in[0], cotangent[0]
    small = jnp.concatenate([
        _spread(norm_gain, index, count).reshape(-1, LANES),
        _spread(conv_bc_weight, index, count).reshape(-1, LANES),
        _spread(conv_bc_bias, index, count).reshape(-1, LANES)], axis=0)
    gain_rows = model // LANES
    both_rows = -(-small.shape[0] // 8) * 8
    small = pad_rows(small, both_rows)
    small_all, inv_in, normed, cot_full, weight, out_t, proj, d_gated = gather_all(
        small, resid, cot, proj_zx.reshape(rows, 2 * width), proj_dt, proj_bc, proj_out.T)
    full_cbw = small_all[gain_rows : gain_rows + 4 * states2 // LANES].reshape(4, states2)
    full_cbb = small_all[gain_rows + 4 * states2 // LANES : gain_rows + 5 * states2 // LANES].reshape(states2)
    full_gain = small_all[:gain_rows].reshape(model)
    packs = pack_params(conv_x_weight, conv_x_bias, full_cbw, full_cbb, dt_bias, a_log, skip_gain, gate_gain)
    y, states, partial = ssd_forward(proj, d_gated, *packs)
    dy, dz, out_partial, grads_zo, ggain = middle(proj, y, d_gated, partial, packs[3], normed, cot_full, out_t, inner_channels)
    d_rest, gx, gbc, gh, block_out, owned_zo = ssd_backward(proj, y, dy, states, *packs, out_partial, grads_zo, resid)
    gx = jnp.concatenate([gx.sum(1), ggain.sum(0)[None]], 0)
    gbc, gh = gbc.sum(1), gh.sum(1)
    to_sum = jnp.concatenate([
        pad_rows(jnp.concatenate([jnp.zeros((gain_rows, LANES), F32), gbc.reshape(-1, LANES)], 0), both_rows),
        gx.reshape(-1, LANES), gh], axis=0)
    to_sum = pad_rows(to_sum, -(-to_sum.shape[0] // 8) * 8)
    d_local, owned, totals, grad_bc = final_sums(dz, d_rest, weight, normed, to_sum, small_all, both_rows)
    inv_in = inv_in[:, :1]
    scaled = resid * inv_in
    d_scaled = d_local * full_gain
    grad_resid = inv_in * (d_scaled - scaled * jnp.mean(d_scaled * scaled, axis=-1, keepdims=True)) + cot
    grad_zx = jnp.stack([owned_zo[:, :width], owned[:, :width]], axis=1)
    grad_dt = owned[:, width + states2 : width + states2 + heads]
    owned_out = owned_zo[:, width:].T
    owned_gain = _own(totals[:gain_rows].reshape(model), index, count)
    at = gain_rows + 4 * states2 // LANES
    owned_cbw = _own(totals[gain_rows:at].reshape(4, states2), index, count)
    owned_cbb = _own(totals[at : at + states2 // LANES].reshape(states2), index, count)
    gx_all = totals[both_rows : both_rows + 7 * width // LANES].reshape(7, width)
    gh_all = totals[both_rows + 7 * width // LANES :]
    skip = gx_all[5].reshape(heads, -1).sum(1)
    return (
        block_out[None], grad_resid[None], owned_gain, grad_zx, grad_dt, grad_bc, gx_all[:4], gx_all[4],
        owned_cbw, owned_cbb, gh_all[0, :heads], gh_all[1, :heads], skip, gx_all[6], owned_out,
    )


def solution(mesh):
    specs = (
        P("dp", "tensor", None), P(("dp", "tensor")), P("dp", None, "tensor"), P("dp", "tensor"),
        P(("dp", "tensor"), None), P(None, "tensor"), P("tensor"), P(None, ("dp", "tensor")),
        P(("dp", "tensor")), P("tensor"), P("tensor"), P("tensor"), P("tensor"), P("tensor", "dp"),
        P("dp", "tensor", None),
    )
    outs = (specs[0], specs[0]) + specs[1:14]
    return jax.shard_map(on_device, mesh=mesh, in_specs=specs, out_specs=outs, check_vma=False)
```
